32 devices in a mesh: gx: 4 (over z), gy: 4 (over y, core), gz: 2 (over x).
Axes of the slice: x: 2, y: 2, z: 4, core: 2. Of those that a mesh axis runs over, the one named last changes fastest.
Arguments:
- solution: float32 [64, 64, 256], P('gx', 'gy', 'gz'), may hold values from -6 to 6
- right_side: float32 [64, 64, 256], P('gx', 'gy', 'gz'), may hold values from -6 to 6
Outputs:
- improved: float32 [64, 64, 256], P('gx', 'gy', 'gz')
The draws below stay inside these ranges and needn't reach their ends.
All inputs are finite; a program needn't handle non-finite values.
Results may differ from the reference program's by a relative error of at most 0.00015.
Values sent between devices are 32-bit elements; how exact they have to be, the bound alone decides.
A program may use at most 64 MiB of HBM per device.

```python
import jax
import jax.numpy as jnp
from jax import lax

LEVELS = 3
DEGREE = 2
SWEEPS = 2
NX = 64
NY = 64
NZ = 256


def levels(stream_key, shape, shards, low, largest):
    loudness = 1.0
    for dim, parts in shards:
        draws = jax.random.uniform(jax.random.fold_in(jax.random.fold_in(stream_key, 6), dim), (parts,), jnp.float32, low / len(shards), largest / len(shards))
        loudness = loudness * jnp.repeat(jnp.exp(draws), shape[dim] // parts).reshape((-1,) + (1,) * (len(shape) - 1 - dim))
    return loudness


def normal_values(key, shape, scale, most, shards=(), kind=jnp.bfloat16):
    result = scale * jax.random.normal(key, shape, jnp.float32)
    if shards:
        result = result * levels(key, shape, shards, -0.22, 0.18)
    return jnp.clip(result, -most, most).astype(kind)


def setup_inputs(seed: int = 0) -> dict:
    key_list = jax.random.split(jax.random.key(seed), 3)
    solution = normal_values(key_list[0], (NX, NY, NZ), 1.0, 6.0, ((0, 4), (1, 4), (2, 2)), jnp.float32)
    right_side = normal_values(key_list[1], (NX, NY, NZ), 1.0, 6.0, ((0, 4), (1, 4), (2, 2)), jnp.float32)
    return {"solution": solution, "right_side": right_side}


stiff_matrix = ((7.0 / 3.0, -8.0 / 3.0, 1.0 / 3.0), (-8.0 / 3.0, 16.0 / 3.0, -8.0 / 3.0), (1.0 / 3.0, -8.0 / 3.0, 7.0 / 3.0))
mass_matrix = ((4.0 / 30.0, 2.0 / 30.0, -1.0 / 30.0), (2.0 / 30.0, 16.0 / 30.0, 2.0 / 30.0), (-1.0 / 30.0, 2.0 / 30.0, 4.0 / 30.0))
cheb_centre = 1.32
cheb_half = 1.1
cheb_sigma = 1.2


def along_axis(values, dim_index, matrix):
    inner_len = values.shape[dim_index] - 4
    parity = jnp.arange(inner_len) % 2 == 0
    vertex = (matrix[2][0], matrix[2][1], matrix[2][2] + matrix[0][0], matrix[0][1], matrix[0][2])
    middle = (0.0, matrix[1][0], matrix[1][1], matrix[1][2], 0.0)
    shape_list = [1, 1, 1]
    shape_list[dim_index] = inner_len
    summed = None
    for offset in range(5):
        weight = jnp.where(parity, vertex[offset], middle[offset]).astype(jnp.float32).reshape(shape_list)
        shifted = lax.slice_in_dim(values, offset, offset + inner_len, 1, dim_index)
        summed = weight * shifted if offset == 0 else summed + weight * shifted
    return summed


def apply_operator(padded, level_num):
    mass_z = along_axis(padded, 2, mass_matrix)
    stiff_z = along_axis(padded, 2, stiff_matrix)
    mass_yz = along_axis(mass_z, 1, mass_matrix)
    stiff_y = along_axis(mass_z, 1, stiff_matrix)
    stiff_only_z = along_axis(stiff_z, 1, mass_matrix)
    return (2.0 ** level_num) * (along_axis(mass_yz, 0, stiff_matrix) + along_axis(stiff_y + stiff_only_z, 0, mass_matrix))


def inverse_diagonal(new_shape, level_num):
    stiff_list = []
    mass_list = []
    for dim_index in range(3):
        even_node = jnp.arange(new_shape[dim_index]) % 2 == 0
        shape_list = [1, 1, 1]
        shape_list[dim_index] = new_shape[dim_index]
        stiff_list.append(jnp.where(even_node, 14.0 / 3.0, 16.0 / 3.0).astype(jnp.float32).reshape(shape_list))
        mass_list.append(jnp.where(even_node, 8.0 / 30.0, 16.0 / 30.0).astype(jnp.float32).reshape(shape_list))
    stiff_first, stiff_second, stiff_third = stiff_list
    mass_first, mass_second, mass_third = mass_list
    diagonal = (2.0 ** level_num) * (stiff_first * mass_second * mass_third + mass_first * stiff_second * mass_third + mass_first * mass_second * stiff_third)
    return 1.0 / diagonal


def along_dim_product(matrix, values, dim_index):
    einsum_forms = ("ap,pyz->ayz", "ap,xpz->xaz", "ap,xyp->xya")
    return jnp.einsum(einsum_forms[dim_index], matrix, values, precision=lax.Precision.HIGHEST)


def prolong_matrix(fine_count, coarse_len):
    row_index = jnp.arange(fine_count + 4)[:, None]
    col_index = jnp.arange(coarse_len)[None, :]
    half_index = row_index // 2
    offset = col_index - half_index
    even_row = row_index % 2 == 0
    even_half = half_index % 2 == 0
    odd_even = jnp.where(offset == 0, -0.125, jnp.where(offset == 1, 0.75, jnp.where(offset == 2, 0.375, 0.0)))
    odd_odd = jnp.where(offset == 1, 0.375, jnp.where(offset == 2, 0.75, jnp.where(offset == 3, -0.125, 0.0)))
    vertex = jnp.where(offset == 1, 1.0, 0.0)
    entries = jnp.where(even_row, vertex, jnp.where(even_half, odd_even, odd_odd))
    entries = jnp.where(row_index == fine_count + 3, 0.0, entries)
    return entries.astype(jnp.float32)


def restrict_matrix(coarse_count, length):
    row_index = jnp.arange(coarse_count)[:, None]
    col_index = jnp.arange(length)[None, :]
    offset = col_index - 2 * row_index
    even_row = row_index % 2 == 0
    outer = jnp.where(even_row, -0.125, 0.0)
    inner = jnp.where(even_row, 0.375, 0.75)
    entries = jnp.where(offset == 3, 1.0, jnp.where((offset == 0) | (offset == 6), outer, jnp.where((offset == 2) | (offset == 4), inner, 0.0)))
    return entries.astype(jnp.float32)


def prolongate(values, fine_shape):
    for dim_index in range(3):
        matrix = prolong_matrix(fine_shape[dim_index], values.shape[dim_index])
        values = along_dim_product(matrix, values, dim_index)
    return values


def restrict_residual(values, coarse_shape):
    for dim_index in range(3):
        matrix = restrict_matrix(coarse_shape[dim_index], values.shape[dim_index])
        values = along_dim_product(matrix, values, dim_index)
    return values


def operator_full(values, level_num):
    return apply_operator(jnp.pad(values, 2), level_num)


def chebyshev_full(level_num, solution, residual, sweep_count):
    inverse = inverse_diagonal(residual.shape, level_num)
    direction = (inverse * residual) * (1.0 / cheb_centre)
    solution = solution + direction
    ratio = 1.0 / cheb_sigma
    for sweep_step in range(1, sweep_count):
        residual = residual - operator_full(direction, level_num)
        ratio_next = 1.0 / (2.0 * cheb_sigma - ratio)
        direction = (ratio_next * ratio) * direction + (2.0 * ratio_next / cheb_half) * (inverse * residual)
        solution = solution + direction
        ratio = ratio_next
    return solution, residual, direction


def vcycle_full(level_num, solution, residual):
    if level_num == LEVELS - 1:
        solution, residual, direction = chebyshev_full(level_num, solution, residual, SWEEPS)
        return solution
    solution, residual, direction = chebyshev_full(level_num, solution, residual, DEGREE)
    residual = residual - operator_full(direction, level_num)
    coarse_shape = tuple(extent // 2 for extent in residual.shape)
    coarse_rhs = restrict_residual(jnp.pad(residual, 3), coarse_shape)
    coarse_sol = vcycle_full(level_num + 1, jnp.zeros(coarse_shape, jnp.float32), coarse_rhs)
    correction = prolongate(jnp.pad(coarse_sol, 2), residual.shape)[2:-2, 2:-2, 2:-2]
    solution = solution + correction
    residual = residual - operator_full(correction, level_num)
    solution, residual, direction = chebyshev_full(level_num, solution, residual, DEGREE)
    return solution


def reference(solution, right_side):
    residual = right_side - operator_full(solution, 0)
    return vcycle_full(0, solution, residual)
```

```python
import functools

import jax
import jax.numpy as jnp
import numpy as np
from jax import lax
from jax.experimental import pallas as pl
from jax.experimental.pallas import tpu as pltpu
from jax.sharding import PartitionSpec as P

F32 = jnp.float32
BF16 = jnp.bfloat16
MESH = pl.DeviceIdType.MESH
H = 8
ZR = 32
REACH = 3
LANES = 128

RHO0 = 1.0 / 1.2
RHO1 = 1.0 / (2.4 - RHO0)
FIRST = 1.0 / 1.32
KEEP = RHO1 * RHO0
STEP = 2.0 * RHO1 / 1.1
RATIO = STEP / FIRST
UNIT = 2700.0


def restrict_taps(g):
    if g % 2 == 0:
        return ((-3, -0.125), (-1, 0.375), (0, 1.0), (1, 0.375), (3, -0.125))
    return ((-1, 0.75), (0, 1.0), (1, 0.75))


def prolong_taps(f):
    if f % 2 == 0:
        return ((f // 2, 1.0),)
    q = f // 4
    if f % 4 == 1:
        return ((2 * q, 0.375), (2 * q + 1, 0.75), (2 * q + 2, -0.125))
    return ((2 * q, -0.125), (2 * q + 1, 0.75), (2 * q + 2, 0.375))


def stiff_taps(i):
    if i % 2 == 0:
        return {-2: 1, -1: -8, 0: 14, 1: -8, 2: 1}
    return {-1: -8, 0: 16, 1: -8}


def mass_taps(i):
    if i % 2 == 0:
        return {-2: -1, -1: 2, 0: 8, 1: 2, 2: -1}
    return {-1: 2, 0: 16, 1: 2}


class Level:
    def __init__(self, group, tiles, height, half, at, parts):
        self.group, self.tiles, self.height, self.half, self.at = group, tiles, height, half, at
        self.parts = parts
        self.rows = 2 * half
        self.paired = group >= 4


def operator_matrix(lv):
    k = 256 if lv.paired else 384
    m = np.zeros((k, 256), np.float64)
    for x in range(lv.group):
        for y in range(lv.height):
            for ox, mx in mass_taps(x).items():
                kx = stiff_taps(x)[ox]
                p = x + ox
                if lv.paired:
                    block = (p + lv.group // 2) // lv.group
                else:
                    block = p // lv.group + 1
                for oy, my in mass_taps(y).items():
                    ky = stiff_taps(y)[oy]
                    if not 0 <= y + oy < lv.height:
                        continue
                    row = block * LANES + lv.at(p % lv.group, y + oy)
                    both, mixed = mx * my, kx * my + mx * ky
                    m[row, lv.at(x, y)] = -8 * both + 2 * mixed
                    m[row, LANES + lv.at(x, y)] = both - mixed
    return m


def plane_matrix(n_in, n_out, pairs_x, pairs_y, at_in, at_out):
    m = np.zeros((n_in * LANES, n_out * LANES), np.float64)
    for (to, xo), ti, xi, wx in pairs_x:
        for yo, yi, wy in pairs_y:
            m[ti * LANES + at_in(xi, yi), to * LANES + at_out(xo, yo)] += wx * wy
    return m


def to_bf16(m):
    out = jnp.asarray(m, BF16)
    assert np.array_equal(np.asarray(m, jnp.bfloat16).astype(np.float64), m)
    return out


def split(v):
    hi = v.astype(BF16)
    return hi, (v - hi.astype(F32)).astype(BF16)


def loop(count, body, most=9):
    if count <= most:
        for i in range(count):
            body(i)
    else:

        def step(i, carry):
            body(i)
            return carry

        lax.fori_loop(0, count, step, 0)


def kernel(
    geo, lv0, lv1, lv2, offs, u_ref, b_ref, *refs,
):
    (wa0_h, wa1_h, wa2_h, wr0_h, wr1_h, wp1_h, wp0_h, out_ref,
     wa0, wa1, wa2, wr0, wr1, wp1, wp0,
     ue, be, tmp, strip_out, strip_in,
     d0, r0, acc0, hh0, hl0, ss0, iv0, mk0, zm0,
     d1, r1, acc1, hh1, hl1, ss1, iv1, mk1, zm1, c1,
     d2, r2, hh2, hl2, ss2, iv2, mk2, zm2,
     xs0, xs1, blk, line, land, up2, zp1, zp0, zh1, zl1, zh0, zl0,
     wsem, xysend, xyrecv, zsend, zrecv, gsend, grecv, psend, precv) = refs
    nx, ny, nz, bx, by, bz, wx, wy, wyp = geo
    ix, iy, iz = lax.axis_index("gx"), lax.axis_index("gy"), lax.axis_index("gz")
    place, counts = (ix, iy, iz), (nx, ny, nz)
    full_x, full_y = wx == nx, wy == ny
    cx, cy, cz = bx // 2, by // 2, bz // 2
    start_x = 0 if full_x else ix - REACH
    start_y = 0 if full_y else iy - REACH
    own_x = ix if full_x else REACH
    own_y = iy if full_y else REACH
    offs_xy, offs_z, offs_g, offs_p = offs

    def there(off, sign=1):
        ok = None
        for p, n, o in zip(place, counts, off):
            if o:
                q = p + sign * o
                c = (q >= 0) & (q < n)
                ok = c if ok is None else ok & c
        return ok

    def device(off):
        return tuple(p + o for p, o in zip(place, off))

    barrier = pltpu.get_barrier_semaphore()
    total = 0
    for off in sorted(set(offs_xy + offs_z + offs_g + offs_p)):
        ok = there(off)
        total = total + ok.astype(jnp.int32)

        @pl.when(ok)
        def _():
            pl.semaphore_signal(
                barrier, inc=1, device_id=device(off), device_id_type=MESH
            )

    loads = [
        pltpu.make_async_copy(s, d, wsem.at[n])
        for n, (s, d) in enumerate(
            ((wa0_h, wa0), (wr0_h, wr0), (wa1_h, wa1), (wr1_h, wr1), (wa2_h, wa2),
             (wp1_h, wp1), (wp0_h, wp0))
        )
    ]
    for c in loads:
        c.start()

    def remote(src, dst, ss, rs, off):
        return pltpu.make_async_remote_copy(
            src_ref=src, dst_ref=dst, send_sem=ss, recv_sem=rs,
            device_id=device(off), device_id_type=MESH,
        )

    def start_if(off, copies):
        @pl.when(there(off))
        def _():
            for c in copies:
                c.start()

    def recv_if(off, copies):
        @pl.when(there(off, -1))
        def _():
            for c in copies:
                c.wait_recv()

    def sent_if(off, copies):
        @pl.when(there(off))
        def _():
            for c in copies:
                c.wait_send()

    def cut(off, size, low, high):
        if off == 0:
            return slice(0, size), slice(H, H + size)
        if off > 0:
            return slice(size - low, size), slice(H - low, H)
        return slice(0, high), slice(H + size, H + size + high)

    fields = ((u_ref, ue, H, H - 1), (b_ref, be, H - 2, H - 3))

    def halo_cut(off, k):
        ref, ext, low, high = fields[k]
        sx, tx = cut(off[0], bx, low, high)
        sy, ty = cut(off[1], by, H, H)
        return ref, ext, sx, tx, sy, ty

    def zero(ref, *at):
        ref[at] = jnp.zeros_like(ref[at])

    def halo_copies(n, which=(0, 1)):
        off = offs_xy[n]
        res = []
        for k in which:
            ref, ext, sx, tx, sy, ty = halo_cut(off, k)
            res.append(
                remote(
                    ref.at[sx, sy], ext.at[tx, ty], xysend.at[n, k], xyrecv.at[n, k], off
                )
            )
        return res

    pl.semaphore_wait(barrier, total)
    for n, off in enumerate(offs_xy):
        start_if(off, halo_copies(n, (0,)))
    for n, off in enumerate(offs_xy):
        start_if(off, halo_copies(n, (1,)))

    ue[H : H + bx, H : H + by] = u_ref[...]
    be[H : H + bx, H : H + by] = b_ref[...]
    for _, ext, low, high in fields:
        for at in (slice(0, H - low), slice(H + bx + high, 2 * H + bx)):
            if at.stop > at.start:
                zero(ext, at)
    for off in [(a, c, 0) for a in (-1, 0, 1) for c in (-1, 0, 1) if a or c]:

        def clear():
            for k in range(2):
                _, ext, _, tx, _, ty = halo_cut(off, k)
                zero(ext, tx, ty)

        if off in offs_xy:
            pl.when(jnp.logical_not(there(off, -1)))(clear)
        else:
            clear()
    zq, half_c = ZR // 2, cz // 2
    for side, rows in ((-1, slice(zq + half_c, 2 * zq + half_c)), (1, slice(0, zq))):

        def clear():
            zero(strip_in, (side + 1) // 2)
            zero(land, slice(None), slice(None), rows)

        if nz > 1:
            pl.when(jnp.logical_not(there((0, 0, side), -1)))(clear)
        else:
            clear()
    if not full_x:
        for off in offs_g:

            @pl.when(jnp.logical_not(there(off, -1)))
            def _():
                zero(line, REACH - off[0])

    if not full_y:
        for off in offs_p:
            if off[2] == 0:

                @pl.when(jnp.logical_not(there(off, -1)))
                def _():
                    zero(land, REACH - off[1])


    def set_up(lv, level, iv, mk, zm, d, ss, x_first, y_first, z_first, x_at, y_at):
        lane = lax.broadcasted_iota(jnp.int32, (8, LANES), 1)
        row = lax.broadcasted_iota(jnp.int32, (lv.half, LANES), 0)
        xx, yy = x_at(lane), y_at(lane)
        x_even, y_even = xx % 2 == 0, yy % 2 == 0
        n_x, n_y, n_z = (nx * bx) >> level, (ny * by) >> level, (nz * bz) >> level
        gy = y_first + yy
        y_ok = (gy >= 0) & (gy < n_y) & (yy < lv.height)
        mass = lambda e: jnp.where(e, 8.0, 16.0) / 30.0
        stiff = lambda e: jnp.where(e, 14.0, 16.0) / 3.0
        my, ky, mx, kx = mass(y_even), stiff(y_even), mass(x_even), stiff(x_even)
        inv = []
        for kz, mz in ((14.0 / 3.0, 8.0 / 30.0), (16.0 / 3.0, 16.0 / 30.0)):
            inv.append((FIRST / UNIT) / (kx * my * mz + mx * ky * mz + mx * my * kz))

        def one(t):
            gx = x_first + t * lv.group + xx
            ok = jnp.where(y_ok & (gx >= 0) & (gx < n_x), 1.0, 0.0).astype(F32)
            mk[t] = ok
            iv[t, 0] = inv[0] * ok
            iv[t, 1] = inv[1] * ok

        loop(lv.tiles, one)
        for par in range(2):
            gz = z_first + 2 * row + par
            zm[par] = jnp.where((gz >= 0) & (gz < n_z), 1.0, 0.0).astype(F32)
        d[0] = jnp.zeros_like(d[0])
        d[lv.tiles + 1] = jnp.zeros_like(d[0])
        ss[:, :, 0:8] = jnp.zeros_like(ss[:, :, 0:8])
        ss[:, :, 8 + lv.half :] = jnp.zeros_like(ss[:, :, 8 + lv.half :])

    gs = LANES // wyp
    yh0 = by + 2 * H
    set_up(
        lv0, 0, iv0, mk0, zm0, d0, ss0, ix * bx - H, iy * by - H, iz * bz - H,
        lambda n: n // yh0, lambda n: n % yh0,
    )
    set_up(
        lv1, 1, iv1, mk1, zm1, d1, ss1, start_x * cx, start_y * cy, iz * cz - ZR,
        lambda n: (n % gs) // cy, lambda n: (n // gs) * cy + n % cy,
    )
    yh2 = LANES // lv2.group
    set_up(
        lv2, 2, iv2, mk2, zm2, d2, ss2, start_x * (cx // 2), start_y * (cy // 2),
        iz * (cz // 2) - ZR // 2, lambda n: n // yh2, lambda n: n % yh2,
    )
    c1[0:2] = jnp.zeros_like(c1[0:2])
    c1[lv1.tiles + 2 :] = jnp.zeros_like(c1[0:2])
    xs1[:, 0:8] = jnp.zeros_like(xs1[:, 0:8])
    xs1[:, 8 + lv1.half :] = jnp.zeros_like(xs1[:, 8 + lv1.half :])
    up2[...] = jnp.zeros_like(up2)

    zh = H // 2
    hb = bz // 2

    def turned(ext, t):
        tmp[...] = ext[lv0.group * t : lv0.group * t + lv0.group].reshape(LANES, bz).T
        return tmp[pl.ds(0, hb, stride=2)], tmp[pl.ds(1, hb, stride=2)]

    def strips(n, t, par, val):
        lo, hi = par * zh, par * zh + zh
        strip_out[0, n, t, lo:hi] = val[:zh]
        strip_out[1, n, t, lo:hi] = val[hb - zh :]

    def z_copies(n):
        off = offs_z[n]
        k = 1 if off[2] > 0 else 0
        return [remote(strip_out.at[k], strip_in.at[k], zsend.at[k], zrecv.at[k], off)]

    for k, ext in enumerate((ue, be)):
        for n, off in enumerate(offs_xy):
            recv_if(off, halo_copies(n, (k,)))
        for t in range(lv0.tiles):
            for par, val in enumerate(turned(ext, t)):
                lo = par * lv0.half + zh
                strips(k, t, par, val)
                if k == 0:
                    d0[t + 1, lo : lo + hb] = val
                else:
                    r0[t, lo : lo + hb] = UNIT * val
    for n, off in enumerate(offs_z):
        start_if(off, z_copies(n))
    for n, off in enumerate(offs_z):
        recv_if(off, z_copies(n))
    for t in range(lv0.tiles):
        for par in range(2):
            for side in range(2):
                lo = par * lv0.half + (0 if side else zh + hb)
                rows = slice(lo, lo + zh)
                d0[t + 1, rows] = strip_in[side, 0, t, par * zh : par * zh + zh]
                r0[t, rows] = UNIT * strip_in[side, 1, t, par * zh : par * zh + zh]

    def stage(lv, d, hh, hl, lo, count):
        step = 48 if lv.rows % 48 == 0 else min(lv.rows, 64)
        lane = lax.broadcasted_iota(jnp.int32, (step, LANES), 1)
        if lv is lv1:
            plane = (lane % gs) // cy
        else:
            plane = lane // (LANES // lv.group)
        low = plane < lv.group // 2

        def one(i):
            t = lo + i
            for s in range(0, lv.rows, step):
                rows = slice(s, s + step)
                if lv.paired:
                    v = jnp.where(low, d[t + 1, rows], d[t, rows])
                else:
                    v = d[t, rows]
                hh[t, rows], hl[t, rows] = split(v)

        loop(count + (1 if lv.paired else 2), one)

    def sweep(lv, hh, hl, w, ss, zm, lo, count, use):
        chunk = 24 if lv.half % 24 == 0 else 32
        n_cat = 2 if lv.paired else 3
        size = 2 if count % 2 == 0 else 1

        def group(i):
            t0 = lo + size * i

            def lhs(h):
                return jnp.concatenate(
                    [h[pl.ds(t0 + j, size)].reshape(size * lv.rows, LANES) for j in range(n_cat)],
                    axis=1,
                )

            s = jnp.dot(lhs(hh), w[...], preferred_element_type=F32) + jnp.dot(
                lhs(hl), w[...], preferred_element_type=F32
            )
            for k in range(size):
                slot = (i % 2) * 2 + k if isinstance(i, int) else k
                for par in range(2):
                    at = k * lv.rows + par * lv.half
                    for c in range(2):
                        ss[slot, 2 * c + par, 8 : 8 + lv.half] = s[
                            at : at + lv.half, LANES * c : LANES * c + LANES
                        ]
                t = t0 + k
                for at in range(0, lv.half, chunk):

                    def rows_of(n, shift=0):
                        return ss[slot, n, pl.ds(8 + at + shift, chunk)]

                    even = (
                        (-11.0 / 3.0) * rows_of(0) + (-46.0 / 3.0) * rows_of(2)
                    ) + ((rows_of(1) + rows_of(1, -1)) + (rows_of(2, -1) + rows_of(2, 1)))
                    odd = ((-16.0 / 3.0) * rows_of(1) + (-80.0 / 3.0) * rows_of(3)) + (
                        rows_of(0) + rows_of(0, 1)
                    )
                    for par, val in enumerate((even, odd)):
                        edge = None
                        if at < lv.parts or at + chunk > lv.half - lv.parts:
                            edge = zm[par, at : at + chunk]
                        use(t, par, slice(par * lv.half + at, par * lv.half + at + chunk), val, edge)

        loop(count // size, group, 4)

    def wide(v, n):
        return jnp.broadcast_to(v[0:1], (n, LANES))

    def masked(v, edge):
        return v if edge is None else v * edge

    def n_rows(rows):
        return rows.stop - rows.start

    own_lo = H // lv0.group
    own_n = bx // lv0.group

    def own(t):
        return own_lo <= t < own_lo + own_n

    def reach(below, above):
        lo = (H - below) // lv0.group
        hi = (H + bx - 1 + above) // lv0.group
        return lo, hi - lo + 1

    def use_residual(t, par, rows, av, edge):
        r = r0[t, rows] - av
        r0[t, rows] = r
        d = masked(wide(iv0[t, par], n_rows(rows)) * r, edge)
        if own(t):
            acc0[t - own_lo, rows] = d0[t + 1, rows] + d
        d0[t + 1, rows] = d

    def use_step(t, par, rows, av, edge):
        r = r0[t, rows] - av
        r0[t, rows] = r
        d = KEEP * d0[t + 1, rows] + masked(
            (RATIO * wide(iv0[t, par], n_rows(rows))) * r, edge
        )
        if own(t):
            acc0[t - own_lo, rows] += d
        d0[t + 1, rows] = d

    def use_down(t, par, rows, av, edge):
        r0[t, rows] = masked((r0[t, rows] - av) * wide(mk0[t], n_rows(rows)), edge)

    lo_a, n_a = reach(6, 5)
    lo_b, n_b = reach(4, 3)
    loads[0].wait()
    stage(lv0, d0, hh0, hl0, lo_a, n_a)
    sweep(lv0, hh0, hl0, wa0, ss0, zm0, lo_a, n_a, use_residual)
    stage(lv0, d0, hh0, hl0, lo_b, n_b)
    sweep(lv0, hh0, hl0, wa0, ss0, zm0, lo_b, n_b, use_step)
    stage(lv0, d0, hh0, hl0, lo_b, n_b)
    sweep(lv0, hh0, hl0, wa0, ss0, zm0, lo_b, n_b, use_down)

    def restricted(parts, w):
        hi, lo = zip(*[split(p) for p in parts])
        return jnp.dot(
            jnp.concatenate(hi, axis=1), w, preferred_element_type=F32
        ) + jnp.dot(jnp.concatenate(lo, axis=1), w, preferred_element_type=F32)

    loads[1].wait()
    x = restricted([r0[lo_b + i] for i in range(n_b)], wr0[...])
    xs0[0] = x[: lv0.half]
    xs0[1] = x[lv0.half :]
    def pick(ref, par, start, n):
        return ref[par, pl.ds(start, n, stride=2)]

    def z_restricted(ref, even0, odd0, n):
        even = (
            0.5 * pick(ref, 0, even0, n)
            + 0.1875 * (pick(ref, 1, odd0, n) + pick(ref, 1, odd0 + 1, n))
            - 0.0625 * (pick(ref, 1, odd0 - 1, n) + pick(ref, 1, odd0 + 2, n))
        )
        odd = 0.5 * pick(ref, 0, even0 + 1, n) + 0.375 * (
            pick(ref, 1, odd0 + 1, n) + pick(ref, 1, odd0 + 2, n)
        )
        return even, odd

    even, odd = z_restricted(xs0, zh, zh - 1, half_c)
    lane_c = lax.broadcasted_iota(jnp.int32, (half_c, LANES), 1)
    packed = jnp.where(lane_c < LANES // 2, even, odd)
    blk[...] = packed

    def slot(axis, off):
        if (full_x, full_y)[axis]:
            return (ix, iy)[axis]
        return REACH - off

    def g_copies(n):
        off = offs_g[n]
        return [remote(blk, line.at[slot(0, off[0])], gsend.at[n], grecv.at[n], off)]

    def p_copies(n):
        off = offs_p[n]
        if off[2] == 0:
            src, dst = slice(0, half_c), slice(zq, zq + half_c)
        elif off[2] > 0:
            src, dst = slice(half_c - zq, half_c), slice(0, zq)
        else:
            src, dst = slice(0, zq), slice(zq + half_c, 2 * zq + half_c)
        return [
            remote(
                line.at[:, src], land.at[slot(1, off[1]), :, dst], psend.at[n], precv.at[n], off
            )
        ]

    for n, off in enumerate(offs_g):
        start_if(off, g_copies(n))
    line[own_x] = packed
    for n, off in enumerate(offs_g):
        recv_if(off, g_copies(n))
    for n, off in enumerate(offs_p):
        start_if(off, p_copies(n))
    land[own_y, :, zq : zq + half_c] = line[...]
    for n, off in enumerate(offs_p):
        recv_if(off, p_copies(n))

    per = cx // lv1.group
    lane_h = lax.broadcasted_iota(jnp.int32, (lv1.half, LANES), 1) // gs

    def place_block(jx):
        blocks = [land[jy, jx] for jy in range(wy)]
        for s in range(per):
            t = jx * per + s
            for par in range(2):
                at = par * (LANES // 2) + s * gs
                val = None
                for jy in range(wy):
                    shift = (jy * gs - at) % LANES
                    v = pltpu.roll(blocks[jy], shift, 1) if shift else blocks[jy]
                    if val is None:
                        val = v if wy == wyp else jnp.where(lane_h == jy, v, 0.0)
                    else:
                        val = jnp.where(lane_h == jy, v, val)
                rows = slice(par * lv1.half, par * lv1.half + lv1.half)
                r1[t, rows] = val
                d = (wide(iv1[t, par], lv1.half) * zm1[par]) * val
                d1[t + 1, rows] = d
                acc1[t, rows] = d

    loop(wx, place_block, 4)

    def use_step1(t, par, rows, av, edge):
        r = r1[t, rows] - av
        r1[t, rows] = r
        d = KEEP * d1[t + 1, rows] + masked(
            (RATIO * wide(iv1[t, par], n_rows(rows))) * r, edge
        )
        d1[t + 1, rows] = d
        acc1[t, rows] += d

    def use_down1(t, par, rows, av, edge):
        r1[t, rows] = masked((r1[t, rows] - av) * wide(mk1[t], n_rows(rows)), edge)

    loads[2].wait()
    n1 = lv1.tiles
    stage(lv1, d1, hh1, hl1, 0, n1)
    sweep(lv1, hh1, hl1, wa1, ss1, zm1, 0, n1, use_step1)
    stage(lv1, d1, hh1, hl1, 0, n1)
    sweep(lv1, hh1, hl1, wa1, ss1, zm1, 0, n1, use_down1)

    ratio = 2 * lv2.group // lv1.group
    r_lo = (-3) // lv1.group
    r_hi = (2 * lv2.group + 1) // lv1.group
    loads[3].wait()
    for t in range(lv2.tiles):
        a, e = max(0, ratio * t + r_lo), min(n1 - 1, ratio * t + r_hi)
        skip = (a - (ratio * t + r_lo)) * LANES
        x = restricted(
            [r1[i] for i in range(a, e + 1)], wr1[skip : skip + (e + 1 - a) * LANES]
        )
        xs1[0, 8 : 8 + lv1.half] = x[: lv1.half]
        xs1[1, 8 : 8 + lv1.half] = x[lv1.half :]
        for par, val in enumerate(z_restricted(xs1, 8, 7, lv2.half)):
            rows = slice(par * lv2.half, par * lv2.half + lv2.half)
            r2[t, rows] = val
            d2[t + 1, rows] = (wide(iv2[t, par], lv2.half) * zm2[par]) * val

    def use_last(t, par, rows, av, edge):
        r = r2[t, rows] - av
        step = masked((RATIO * wide(iv2[t, par], n_rows(rows))) * r, edge)
        lo = rows.start - par * lv2.half
        up2[t, par, lo : lo + n_rows(rows)] = (1.0 + KEEP) * d2[t + 1, rows] + step

    loads[4].wait()
    stage(lv2, d2, hh2, hl2, 0, lv2.tiles)
    sweep(lv2, hh2, hl2, wa2, ss2, zm2, 0, lv2.tiles, use_last)

    loads[5].wait()
    n2 = lv2.half
    for t in range(lv2.tiles):
        e2, o2, e3 = up2[t, 0, 0:n2], up2[t, 1, 0:n2], up2[t, 0, 1 : n2 + 1]
        zp1[t, pl.ds(0, n2, stride=2)] = e2
        zp1[t, pl.ds(1, n2, stride=2)] = o2
        zp1[t, pl.ds(lv1.half, n2, stride=2)] = 0.375 * e2 + 0.75 * o2 - 0.125 * e3
        zp1[t, pl.ds(lv1.half + 1, n2, stride=2)] = 0.75 * o2 + 0.375 * e3 - 0.125 * e2
        zh1[t], zl1[t] = split(zp1[t])
    for t in range(lv2.tiles):
        n_in = min(2, lv2.tiles - t)
        w = wp1[: n_in * LANES]
        e = jnp.dot(
            jnp.concatenate([zh1[t + i] for i in range(n_in)], axis=1), w,
            preferred_element_type=F32,
        ) + jnp.dot(
            jnp.concatenate([zl1[t + i] for i in range(n_in)], axis=1), w,
            preferred_element_type=F32,
        )
        for k in range(ratio):
            to = ratio * t + k
            if to < n1:
                for par in range(2):
                    rows = slice(par * lv1.half, par * lv1.half + lv1.half)
                    v = e[rows, LANES * k : LANES * k + LANES] * (
                        wide(mk1[to], lv1.half) * zm1[par]
                    )
                    d1[to + 1, rows] = v
                    acc1[to, rows] += v

    def use_up1(t, par, rows, av, edge):
        r = r1[t, rows] - av
        r1[t, rows] = r
        d1[t + 1, rows] = masked(wide(iv1[t, par], n_rows(rows)) * r, edge)

    def use_final1(t, par, rows, av, edge):
        r = r1[t, rows] - av
        c1[t + 2, rows] = (acc1[t, rows] + (1.0 + KEEP) * d1[t + 1, rows]) + masked(
            (RATIO * wide(iv1[t, par], n_rows(rows))) * r, edge
        )

    stage(lv1, d1, hh1, hl1, 0, n1)
    sweep(lv1, hh1, hl1, wa1, ss1, zm1, 0, n1, use_up1)
    stage(lv1, d1, hh1, hl1, 0, n1)
    sweep(lv1, hh1, hl1, wa1, ss1, zm1, 0, n1, use_final1)

    up = 2 * lv1.group // lv0.group
    tau_lo = (lo_b - own_lo) // up
    tau_hi = (lo_b + n_b - 1 - own_lo) // up
    n_tau = tau_hi + 2 - tau_lo
    jn = (lv0.half // 2 + 7) // 8 * 8
    lane_j = lax.broadcasted_iota(jnp.int32, (jn, LANES), 1) // gs
    bad = ((lane_j == 0) & (own_y == 0)) | ((lane_j == 2) & (own_y == wy - 1))
    turn = lax.rem(1 - own_y + wyp, wyp) * gs
    first = ZR // 2 - zh // 2
    loads[6].wait()
    for i in range(n_tau):
        at = own_x * per + (tau_lo + i + 2)

        def rows_of(par, start):
            v = pltpu.roll(c1[at, pl.ds(par * lv1.half + start, jn)], turn, 1)
            return jnp.where(bad, 0.0, v)

        e2, o2, e3 = rows_of(0, first), rows_of(1, first), rows_of(0, first + 1)
        zp0[i, pl.ds(0, jn, stride=2)] = e2
        zp0[i, pl.ds(1, jn, stride=2)] = o2
        zp0[i, pl.ds(lv0.half, jn, stride=2)] = 0.375 * e2 + 0.75 * o2 - 0.125 * e3
        zp0[i, pl.ds(lv0.half + 1, jn, stride=2)] = 0.75 * o2 + 0.375 * e3 - 0.125 * e2
        zh0[i], zl0[i] = split(zp0[i, 0 : lv0.rows])
    for i in range(n_tau - 1):
        e = jnp.dot(
            jnp.concatenate([zh0[i], zh0[i + 1]], axis=1), wp0[...],
            preferred_element_type=F32,
        ) + jnp.dot(
            jnp.concatenate([zl0[i], zl0[i + 1]], axis=1), wp0[...],
            preferred_element_type=F32,
        )
        for k in range(up):
            t = own_lo + up * (tau_lo + i) + k
            if lo_b <= t < lo_b + n_b:
                for par in range(2):
                    rows = slice(par * lv0.half, par * lv0.half + lv0.half)
                    v = e[rows, LANES * k : LANES * k + LANES] * (
                        wide(mk0[t], lv0.half) * zm0[par]
                    )
                    d0[t + 1, rows] = v
                    if own(t):
                        acc0[t - own_lo, rows] += v

    def use_up(t, par, rows, av, edge):
        r = r0[t, rows] - av
        r0[t, rows] = r
        d0[t + 1, rows] = masked(wide(iv0[t, par], n_rows(rows)) * r, edge)

    def use_final(t, par, rows, av, edge):
        r = r0[t, rows] - av
        acc0[t - own_lo, rows] += (1.0 + KEEP) * d0[t + 1, rows] + (
            RATIO * wide(iv0[t, par], n_rows(rows))
        ) * r

    lo_c, n_c = reach(2, 1)
    stage(lv0, d0, hh0, hl0, lo_c, n_c)
    sweep(lv0, hh0, hl0, wa0, ss0, zm0, lo_c, n_c, use_up)
    stage(lv0, d0, hh0, hl0, own_lo, own_n)
    sweep(lv0, hh0, hl0, wa0, ss0, zm0, own_lo, own_n, use_final)

    for i in range(own_n):
        for par in range(2):
            lo = par * lv0.half + zh
            tmp[pl.ds(par, hb, stride=2)] = acc0[i, lo : lo + hb]
        v = tmp[...].T.reshape(lv0.group, yh0, bz)
        out_ref[lv0.group * i : lv0.group * i + lv0.group] = v[:, H : H + by]

    for n, off in enumerate(offs_xy):
        sent_if(off, halo_copies(n))
    for n, off in enumerate(offs_z):
        sent_if(off, z_copies(n))
    for n, off in enumerate(offs_g):
        sent_if(off, g_copies(n))
    for n, off in enumerate(offs_p):
        sent_if(off, p_copies(n))


def local(mesh_shape, u, b):
    nx, ny, nz = (mesh_shape[a] for a in ("gx", "gy", "gz"))
    bx, by, bz = u.shape
    cx, cy, cz = bx // 2, by // 2, bz // 2
    wx = nx if nx <= 2 * REACH + 1 else 2 * REACH + 1
    wy = ny if ny <= 2 * REACH + 1 else 2 * REACH + 1
    wyp = 4 if wy <= 4 else 8
    gs = LANES // wyp
    yh0 = by + 2 * H
    xg0 = LANES // yh0
    lv0 = Level(
        xg0, (bx + 2 * H) // xg0, yh0, (bz + 2 * H) // 2, lambda x, y: x * yh0 + y, H // 2
    )
    xg1 = gs // cy
    lv1 = Level(
        xg1, cx * wx // xg1, cy * wy, (cz + 2 * ZR) // 2,
        lambda x, y: (y // cy) * gs + x * cy + y % cy, ZR // 2,
    )
    y2 = cy * wy // 2
    yh2 = 16 if y2 <= 16 else 32
    xg2 = LANES // yh2
    lv2 = Level(
        xg2, -(-(cx * wx // 2) // xg2), y2, (cz + 2 * ZR) // 4, lambda x, y: x * yh2 + y,
        ZR // 4,
    )

    offs_xy = [(a, c, 0) for a in (-1, 0, 1) for c in (-1, 0, 1) if (a or c)]
    offs_xy = [o for o in offs_xy if (nx > 1 or not o[0]) and (ny > 1 or not o[1])]
    zs = (-1, 1) if nz > 1 else ()
    offs_z = [(0, 0, c) for c in zs]
    sx = wx - 1 if wx == nx else REACH
    sy = wy - 1 if wy == ny else REACH
    offs_g = [(a, 0, 0) for a in range(-sx, sx + 1) if a]
    offs_p = [(0, a, c) for a in range(-sy, sy + 1) for c in (0,) + zs if a or c]
    offs = (offs_xy, offs_z, offs_g, offs_p)

    own_lo = H // xg0
    lo_b = (H - 4) // xg0
    n_b = (H + bx - 1 + 3) // xg0 - lo_b + 1
    px = []
    for x in range(cx):
        for s, w in restrict_taps(x):
            f = H + 2 * x + s
            px.append(((0, x), f // xg0 - lo_b, f % xg0, w))
    py = [(y, H + 2 * y + s, w) for y in range(cy) for s, w in restrict_taps(y)]
    once = plane_matrix(n_b, 1, px, py, lv0.at, lambda x, y: x * cy + y)
    m_r0 = once + np.roll(once, LANES // 2, axis=1)

    r_lo, r_hi = (-3) // xg1, (2 * xg2 + 1) // xg1
    px = []
    for x in range(xg2):
        for s, w in restrict_taps(x):
            f = 2 * x + s
            px.append(((0, x), f // xg1 - r_lo, f % xg1, w))
    py = [
        (y, 2 * y + s, w) for y in range(y2) for s, w in restrict_taps(y)
        if 0 <= 2 * y + s < cy * wy
    ]
    m_r1 = plane_matrix(r_hi - r_lo + 1, 1, px, py, lv1.at, lv2.at)

    ratio = 2 * xg2 // xg1
    px = []
    for f in range(2 * xg2):
        for c, w in prolong_taps(f):
            px.append(((f // xg1, f % xg1), c // xg2, c % xg2, w))
    py = [
        (f, c, w) for f in range(cy * wy) for c, w in prolong_taps(f) if 0 <= c < y2
    ]
    m_p1 = plane_matrix(2, ratio, px, py, lv2.at, lv1.at)

    up = 2 * xg1 // xg0
    px = []
    for f in range(2 * xg1):
        for c, w in prolong_taps(f):
            px.append(((f // xg0, f % xg0), c // xg1, c % xg1, w))
    py = [
        (f + H, c + cy, w) for f in range(-H, by + H) for c, w in prolong_taps(f)
        if -cy <= c < 2 * cy
    ]
    m_p0 = plane_matrix(2, up, px, py, lv1.at, lv0.at)

    consts = tuple(
        to_bf16(m)
        for m in (
            operator_matrix(lv0), operator_matrix(lv1), operator_matrix(lv2),
            m_r0, m_r1, m_p1, m_p0,
        )
    )
    vm = lambda *s: pltpu.VMEM(s, F32)
    bm = lambda *s: pltpu.VMEM(s, BF16)
    dma = lambda *s: pltpu.SemaphoreType.DMA(s)

    def per_level(lv):
        t, n = lv.tiles, lv.rows
        return (
            vm(t + 2, n, LANES), vm(t, n, LANES), vm(t, n, LANES),
            bm(t + 2, n, LANES), bm(t + 2, n, LANES), vm(4, 4, lv.half + 16, LANES),
            vm(t, 2, 8, LANES), vm(t, 8, LANES), vm(2, lv.half, LANES),
        )

    p0, p1, p2 = per_level(lv0), per_level(lv1), per_level(lv2)
    tau_lo = (lo_b - own_lo) // up
    n_tau = (lo_b + n_b - 1 - own_lo) // up + 2 - tau_lo
    jn = (lv0.half // 2 + 7) // 8 * 8
    geo = (nx, ny, nz, bx, by, bz, wx, wy, wyp)
    return pl.pallas_call(
        functools.partial(kernel, geo, lv0, lv1, lv2, offs),
        out_shape=jax.ShapeDtypeStruct(u.shape, F32),
        in_specs=[pl.BlockSpec(memory_space=pltpu.VMEM)] * 2
        + [pl.BlockSpec(memory_space=pl.ANY)] * len(consts),
        out_specs=pl.BlockSpec(memory_space=pltpu.VMEM),
        scratch_shapes=[bm(*c.shape) for c in consts]
        + [
            vm(bx + 2 * H, yh0, bz), vm(bx + 2 * H, yh0, bz), vm(bz, LANES),
            vm(2, 2, lv0.tiles, H, LANES), vm(2, 2, lv0.tiles, H, LANES),
            *p0, *p1, vm(lv1.tiles + 4, lv1.rows, LANES), p2[0], p2[1], *p2[3:],
            vm(2, lv0.half, LANES), vm(2, lv1.half + 16, LANES), vm(cz // 2, LANES),
            vm(wx, cz // 2, LANES), vm(wy, wx, lv1.half, LANES),
            vm(lv2.tiles, 2, lv2.half + 8, LANES), vm(lv2.tiles, lv1.rows, LANES),
            vm(n_tau, lv0.half + 2 * jn, LANES),
            bm(lv2.tiles, lv1.rows, LANES), bm(lv2.tiles, lv1.rows, LANES),
            bm(n_tau, lv0.rows, LANES), bm(n_tau, lv0.rows, LANES),
            dma(len(consts)), dma(max(1, len(offs_xy)), 2), dma(max(1, len(offs_xy)), 2),
            dma(2), dma(2), dma(max(1, len(offs_g))), dma(max(1, len(offs_g))),
            dma(max(1, len(offs_p))), dma(max(1, len(offs_p))),
        ],
        compiler_params=pltpu.CompilerParams(
            collective_id=0, has_side_effects=True, vmem_limit_bytes=60 * 1024 * 1024
        ),
    )(u, b, *consts)


def solution(mesh):
    placed = P("gx", "gy", "gz")
    return jax.shard_map(
        functools.partial(local, dict(mesh.shape)), mesh=mesh,
        in_specs=(placed, placed), out_specs=placed, check_vma=False,
    )
```

```python
import functools

import jax
import jax.numpy as jnp
import numpy as np
from jax import lax
from jax.experimental import pallas as pl
from jax.experimental.pallas import tpu as pltpu
from jax.sharding import PartitionSpec as P

F32 = jnp.float32
BF16 = jnp.bfloat16
MESH = pl.DeviceIdType.MESH
H = 8
ZR = 32
REACH = 3
LANES = 128

RHO0 = 1.0 / 1.2
RHO1 = 1.0 / (2.4 - RHO0)
FIRST = 1.0 / 1.32
KEEP = RHO1 * RHO0
STEP = 2.0 * RHO1 / 1.1
RATIO = STEP / FIRST
UNIT = 2700.0


def restrict_taps(g):
    if g % 2 == 0:
        return ((-3, -0.125), (-1, 0.375), (0, 1.0), (1, 0.375), (3, -0.125))
    return ((-1, 0.75), (0, 1.0), (1, 0.75))


def prolong_taps(f):
    if f % 2 == 0:
        return ((f // 2, 1.0),)
    q = f // 4
    if f % 4 == 1:
        return ((2 * q, 0.375), (2 * q + 1, 0.75), (2 * q + 2, -0.125))
    return ((2 * q, -0.125), (2 * q + 1, 0.75), (2 * q + 2, 0.375))


def stiff_taps(i):
    if i % 2 == 0:
        return {-2: 1, -1: -8, 0: 14, 1: -8, 2: 1}
    return {-1: -8, 0: 16, 1: -8}


def mass_taps(i):
    if i % 2 == 0:
        return {-2: -1, -1: 2, 0: 8, 1: 2, 2: -1}
    return {-1: 2, 0: 16, 1: 2}


class Level:
    def __init__(self, group, tiles, height, half, at, parts):
        self.group, self.tiles, self.height, self.half, self.at = group, tiles, height, half, at
        self.parts = parts
        self.rows = 2 * half
        self.paired = group >= 4


def operator_matrix(lv):
    k = 256 if lv.paired else 384
    m = np.zeros((k, 256), np.float64)
    for x in range(lv.group):
        for y in range(lv.height):
            for ox, mx in mass_taps(x).items():
                kx = stiff_taps(x)[ox]
                p = x + ox
                if lv.paired:
                    block = (p + lv.group // 2) // lv.group
                else:
                    block = p // lv.group + 1
                for oy, my in mass_taps(y).items():
                    ky = stiff_taps(y)[oy]
                    if not 0 <= y + oy < lv.height:
                        continue
                    row = block * LANES + lv.at(p % lv.group, y + oy)
                    both, mixed = mx * my, kx * my + mx * ky
                    m[row, lv.at(x, y)] = -8 * both + 2 * mixed
                    m[row, LANES + lv.at(x, y)] = both - mixed
    return m


def plane_matrix(n_in, n_out, pairs_x, pairs_y, at_in, at_out):
    m = np.zeros((n_in * LANES, n_out * LANES), np.float64)
    for (to, xo), ti, xi, wx in pairs_x:
        for yo, yi, wy in pairs_y:
            m[ti * LANES + at_in(xi, yi), to * LANES + at_out(xo, yo)] += wx * wy
    return m


def to_bf16(m):
    out = jnp.asarray(m, BF16)
    assert np.array_equal(np.asarray(m, jnp.bfloat16).astype(np.float64), m)
    return out


def split(v):
    hi = v.astype(BF16)
    return hi, (v - hi.astype(F32)).astype(BF16)


def loop(count, body, most=9):
    if count <= most:
        for i in range(count):
            body(i)
    else:

        def step(i, carry):
            body(i)
            return carry

        lax.fori_loop(0, count, step, 0)


def kernel(
    geo, lv0, lv1, lv2, parts, u_hbm, b_hbm, w_hbm, out_ref, *refs,
):
    (wall, u_ref, b_ref, ue, be, tmp, pad, strip_out, strip_in,
     d0, r0, acc0, hh0, hl0, ss0, iv0, mk0, zm0,
     d1, r1, acc1, hh1, hl1, ss1, iv1, mk1, zm1, c1,
     d2, r2, hh2, hl2, ss2, iv2, mk2, zm2,
     xs0, xs1, blk, line, land, up2, zp1, zp0, zh1, zl1, zh0, zl0,
     wsem, xysend, xyrecv, zsend, zrecv, gsend, grecv, psend, precv) = refs
    nx, ny, nz, bx, by, bz, wx, wy, wyp = geo
    ix, iy, iz = lax.axis_index("gx"), lax.axis_index("gy"), lax.axis_index("gz")
    place, counts = (ix, iy, iz), (nx, ny, nz)
    full_x, full_y = wx == nx, wy == ny
    cx, cy, cz = bx // 2, by // 2, bz // 2
    start_x = 0 if full_x else ix - REACH
    start_y = 0 if full_y else iy - REACH
    own_x = ix if full_x else REACH
    own_y = iy if full_y else REACH

    def both(*oks):
        ok = None
        for o in oks:
            if o is not None:
                ok = o if ok is None else ok & o
        return ok

    def when(ok, act):
        if ok is None:
            act()
        else:
            pl.when(ok)(act)

    def unless(ok, act):
        if ok is not None:
            pl.when(jnp.logical_not(ok))(act)

    def inside(axis, p):
        return (p >= 0) & (p < counts[axis])

    def shifted(axis, off):
        if off == 0:
            return (place[axis], None, place[axis], None)
        to, source = place[axis] + off, place[axis] - off
        return (to, inside(axis, to), source, inside(axis, source))

    def line_steps(axis, full):
        p, n = place[axis], counts[axis]
        if full:
            steps = []
            for k in sorted(range(1, n), key=lambda k: min(k, n - k)):
                to, source = lax.rem(p + k, n), lax.rem(p + n - k, n)
                steps.append((to, None, source, None, p, source))
            return steps
        offs = sorted((o for o in range(-REACH, REACH + 1) if o), key=abs)
        return [shifted(axis, o) + (REACH - o, REACH - o) for o in offs]

    zq, half_c = ZR // 2, cz // 2
    x_steps = line_steps(0, full_x)
    y_steps = line_steps(1, full_y)
    if nz == 2:
        z_steps = [
            (1 - iz, None, 1 - iz, None, 1 - iz,
             pl.multiple_of((1 - iz) * (half_c - zq), 8),
             pl.multiple_of(iz * (zq + half_c), 8))
        ]
    elif nz > 2:
        z_steps = [
            shifted(2, 1) + (1, half_c - zq, 0), shifted(2, -1) + (0, 0, zq + half_c)
        ]
    else:
        z_steps = []
    plane_steps = [
        ((ix, ys[0], iz), ys[1], ys[3], ys[4], None) for ys in y_steps
    ] + [
        ((ix, iy, zs[0]), zs[1], zs[3], own_y, zs) for zs in z_steps
    ] + [
        ((ix, ys[0], zs[0]), both(ys[1], zs[1]), both(ys[3], zs[3]), ys[4], zs)
        for zs in z_steps for ys in y_steps
    ]
    near = [0] + ([-1, 1] if nx > 1 else [])
    side = [0] + ([-1, 1] if ny > 1 else [])
    xy_offs = [(a, c) for a in near for c in side if a or c]

    def xy_step(off):
        xs, ys = shifted(0, off[0]), shifted(1, off[1])
        return (xs[0], ys[0]), both(xs[1], ys[1]), both(xs[3], ys[3])

    greet = [((st[0], iy, iz), st[1], st[3]) for st in x_steps]
    greet += [(st[0], st[1], st[2]) for st in plane_steps]
    for off in xy_offs:
        if off[0]:
            to, ok, ok_from = xy_step(off)
            if off[1]:
                greet.append((to + (iz,), ok, ok_from))
            for zs in z_steps:
                greet.append((to + (zs[0],), both(ok, zs[1]), both(ok_from, zs[3])))

    barrier = pltpu.get_barrier_semaphore()
    total = 0
    for to, ok, ok_from in greet:
        total = total + (1 if ok_from is None else ok_from.astype(jnp.int32))

        def signal():
            pl.semaphore_signal(barrier, inc=1, device_id=to, device_id_type=MESH)

        when(ok, signal)

    load_u = pltpu.make_async_copy(u_hbm, u_ref, wsem.at[0])
    load_b = pltpu.make_async_copy(b_hbm, b_ref, wsem.at[1])
    load_w = pltpu.make_async_copy(w_hbm, wall, wsem.at[2])
    load_u.start()
    load_b.start()
    load_w.start()

    def remote(src, dst, ss, rs, to):
        return pltpu.make_async_remote_copy(
            src_ref=src, dst_ref=dst, send_sem=ss, recv_sem=rs,
            device_id=to, device_id_type=MESH,
        )

    def weights(name):
        blocks = []
        for row, lane, rows, lanes in parts[name]:
            blocks.append(wall[row : row + rows, lane : lane + lanes])
        if parts[name][0][3] == LANES:
            return jnp.concatenate(blocks, axis=0)
        return jnp.concatenate(blocks, axis=1)

    def cut(off, size, low, high):
        if off == 0:
            return slice(0, size), slice(H, H + size)
        if off > 0:
            return slice(size - low, size), slice(H - low, H)
        return slice(0, high), slice(H + size, H + size + high)

    fields = ((u_ref, ue, H, H - 1), (b_ref, be, H - 2, H - 3))

    def halo_cut(off, k):
        ref, ext, low, high = fields[k]
        sx, tx = cut(off[0], bx, low, high)
        sy, ty = cut(off[1], by, H, H)
        return ref, ext, sx, tx, sy, ty

    def zero(ref, *at):
        ref[at] = jnp.zeros_like(ref[at])

    def halo_copy(n, k):
        ref, ext, sx, tx, sy, ty = halo_cut(xy_offs[n], k)
        to = xy_step(xy_offs[n])[0] + (iz,)
        return remote(ref.at[sx, sy], ext.at[tx, ty], xysend.at[n, k], xyrecv.at[n, k], to)

    yh0 = by + 2 * H
    zh, hb = H // 2, bz // 2
    own_lo, own_n = H // lv0.group, bx // lv0.group
    edge_n = H // lv0.group
    spots = [(a, c) for a in near for c in side]

    def variant(c):
        return 0 if c == 0 else (1 if c > 0 else 2)

    def strip_cut(a):
        if a == 0:
            return slice(0, own_n), slice(own_lo, own_lo + own_n)
        if a > 0:
            return slice(own_n - edge_n, own_n), slice(0, edge_n)
        return slice(0, edge_n), slice(own_lo + own_n, own_lo + own_n + edge_n)

    def strip_copy(n, m):
        a, c = spots[n]
        zs = z_steps[m]
        src, dst = strip_cut(a)
        v, k = variant(c), zs[4]
        to = (shifted(0, a)[0], shifted(1, c)[0], zs[0])
        return remote(
            strip_out.at[k, v, :, src], strip_in.at[k, v, :, dst],
            zsend.at[n, m], zrecv.at[n, m], to,
        )

    def strip_ok(n, m, at):
        a, c = spots[n]
        return both(shifted(0, a)[at], shifted(1, c)[at], z_steps[m][at])

    zero(pad, slice(None), slice(0, H))
    zero(pad, slice(None), slice(H + by, yh0))
    lane_y = lax.broadcasted_iota(jnp.int32, (2 * zh, LANES), 1) % yh0
    load_u.wait()
    load_b.wait()
    for k, ref in enumerate((u_ref, b_ref)):
        for t in range(own_n):
            pad[:, H : H + by] = ref[lv0.group * t : lv0.group * t + lv0.group]
            tmp[...] = pad[...].reshape(LANES, bz).T
            for s, start in ((0, 0), (1, bz - H)):
                v = jnp.concatenate(
                    [tmp[pl.ds(start + par, zh, stride=2)] for par in range(2)], axis=0
                )
                strip_out[s, 0, k, t] = v
                if ny > 1:
                    strip_out[s, 1, k, t] = jnp.where(
                        lane_y < H, pltpu.roll(v, LANES - by, 1), 0.0
                    )
                    strip_out[s, 2, k, t] = jnp.where(
                        lane_y >= H + by, pltpu.roll(v, by, 1), 0.0
                    )

    pl.semaphore_wait(barrier, total)
    for n, off in enumerate(xy_offs):
        when(xy_step(off)[1], lambda: halo_copy(n, 0).start())
    for m in range(len(z_steps)):
        for n in range(len(spots)):
            when(strip_ok(n, m, 1), lambda: strip_copy(n, m).start())
    for n, off in enumerate(xy_offs):
        when(xy_step(off)[1], lambda: halo_copy(n, 1).start())

    ue[H : H + bx, H : H + by] = u_ref[...]
    be[H : H + bx, H : H + by] = b_ref[...]
    for _, ext, low, high in fields:
        for at in (slice(0, H - low), slice(H + bx + high, 2 * H + bx)):
            if at.stop > at.start:
                zero(ext, at)
    for off in [(a, c) for a in (-1, 0, 1) for c in (-1, 0, 1) if a or c]:

        def clear():
            for k in range(2):
                _, ext, _, tx, _, ty = halo_cut(off, k)
                zero(ext, tx, ty)

        if off in xy_offs:
            unless(xy_step(off)[2], clear)
        else:
            clear()
    for s, rows in ((0, slice(zq + half_c, 2 * zq + half_c)), (1, slice(0, zq))):
        z_ok = inside(2, iz + (1 - 2 * s)) if nz > 1 else None
        for a in (-1, 0, 1):
            for c in (-1, 0, 1):

                def clear():
                    zero(strip_in, s, variant(c), slice(None), strip_cut(a)[1])

                if (a, c) in spots and nz > 1:
                    unless(both(shifted(0, a)[3], shifted(1, c)[3], z_ok), clear)
                else:
                    clear()

        def clear():
            zero(land, slice(None), slice(None), rows)

        if nz > 1:
            unless(z_ok, clear)
        else:
            clear()
    for st in x_steps:
        unless(st[3], lambda: zero(land, slice(None), st[5]))
    for st in y_steps:
        unless(st[3], lambda: zero(land, st[5]))

    def set_up(lv, level, iv, mk, zm, d, ss, x_first, y_first, z_first, x_at, y_at):
        lane = lax.broadcasted_iota(jnp.int32, (8, LANES), 1)
        row = lax.broadcasted_iota(jnp.int32, (lv.half, LANES), 0)
        xx, yy = x_at(lane), y_at(lane)
        x_even, y_even = xx % 2 == 0, yy % 2 == 0
        n_x, n_y, n_z = (nx * bx) >> level, (ny * by) >> level, (nz * bz) >> level
        gy = y_first + yy
        y_ok = (gy >= 0) & (gy < n_y) & (yy < lv.height)
        mass = lambda e: jnp.where(e, 8.0, 16.0) / 30.0
        stiff = lambda e: jnp.where(e, 14.0, 16.0) / 3.0
        my, ky, mx, kx = mass(y_even), stiff(y_even), mass(x_even), stiff(x_even)
        inv = []
        for kz, mz in ((14.0 / 3.0, 8.0 / 30.0), (16.0 / 3.0, 16.0 / 30.0)):
            inv.append((FIRST / UNIT) / (kx * my * mz + mx * ky * mz + mx * my * kz))

        def one(t):
            gx = x_first + t * lv.group + xx
            ok = jnp.where(y_ok & (gx >= 0) & (gx < n_x), 1.0, 0.0).astype(F32)
            mk[t] = ok
            iv[t, 0] = inv[0] * ok
            iv[t, 1] = inv[1] * ok

        loop(lv.tiles, one)
        for par in range(2):
            gz = z_first + 2 * row + par
            zm[par] = jnp.where((gz >= 0) & (gz < n_z), 1.0, 0.0).astype(F32)
        d[0] = jnp.zeros_like(d[0])
        d[lv.tiles + 1] = jnp.zeros_like(d[0])
        ss[:, :, 0:8] = jnp.zeros_like(ss[:, :, 0:8])
        ss[:, :, 8 + lv.half :] = jnp.zeros_like(ss[:, :, 8 + lv.half :])

    gs = LANES // wyp
    set_up(
        lv0, 0, iv0, mk0, zm0, d0, ss0, ix * bx - H, iy * by - H, iz * bz - H,
        lambda n: n // yh0, lambda n: n % yh0,
    )
    set_up(
        lv1, 1, iv1, mk1, zm1, d1, ss1, start_x * cx, start_y * cy, iz * cz - ZR,
        lambda n: (n % gs) // cy, lambda n: (n // gs) * cy + n % cy,
    )
    yh2 = LANES // lv2.group
    set_up(
        lv2, 2, iv2, mk2, zm2, d2, ss2, start_x * (cx // 2), start_y * (cy // 2),
        iz * (cz // 2) - ZR // 2, lambda n: n // yh2, lambda n: n % yh2,
    )
    c1[0:2] = jnp.zeros_like(c1[0:2])
    c1[lv1.tiles + 2 :] = jnp.zeros_like(c1[0:2])
    xs1[:, 0:8] = jnp.zeros_like(xs1[:, 0:8])
    xs1[:, 8 + lv1.half :] = jnp.zeros_like(xs1[:, 8 + lv1.half :])
    up2[...] = jnp.zeros_like(up2)

    def turn_field(k):
        ext = (ue, be)[k]
        for n, off in enumerate(xy_offs):
            when(xy_step(off)[2], lambda: halo_copy(n, k).wait_recv())
        for t in range(lv0.tiles):
            tmp[...] = ext[lv0.group * t : lv0.group * t + lv0.group].reshape(LANES, bz).T
            for par in range(2):
                val = tmp[pl.ds(par, hb, stride=2)]
                lo = par * lv0.half + zh
                if k == 0:
                    d0[t + 1, lo : lo + hb] = val
                else:
                    r0[t, lo : lo + hb] = UNIT * val

    def fill_strips():
        for t in range(lv0.tiles):
            for s in range(2):
                for k in range(2):
                    v = (strip_in[s, 0, k, t] + strip_in[s, 1, k, t]) + strip_in[s, 2, k, t]
                    for par in range(2):
                        lo = par * lv0.half + (0 if s else zh + hb)
                        rows, part = slice(lo, lo + zh), v[par * zh : par * zh + zh]
                        if k == 0:
                            d0[t + 1, rows] = part
                        else:
                            r0[t, rows] = UNIT * part

    turn_field(0)
    for m in range(len(z_steps)):
        for n in range(len(spots)):
            when(strip_ok(n, m, 3), lambda: strip_copy(n, m).wait_recv())
    fill_strips()
    turn_field(1)

    def stage(lv, d, hh, hl, lo, count):
        step = 48 if lv.rows % 48 == 0 else min(lv.rows, 64)
        lane = lax.broadcasted_iota(jnp.int32, (step, LANES), 1)
        if lv is lv1:
            plane = (lane % gs) // cy
        else:
            plane = lane // (LANES // lv.group)
        low = plane < lv.group // 2

        def one(i):
            t = lo + i
            for s in range(0, lv.rows, step):
                rows = slice(s, s + step)
                if lv.paired:
                    v = jnp.where(low, d[t + 1, rows], d[t, rows])
                else:
                    v = d[t, rows]
                hh[t, rows], hl[t, rows] = split(v)

        loop(count + (1 if lv.paired else 2), one)

    def sweep(lv, hh, hl, w, ss, zm, lo, count, use):
        chunk = 24 if lv.half % 24 == 0 else 32
        n_cat = 2 if lv.paired else 3
        size = 2 if count % 2 == 0 else 1

        def group(i):
            t0 = lo + size * i

            def lhs(h):
                return jnp.concatenate(
                    [h[pl.ds(t0 + j, size)].reshape(size * lv.rows, LANES) for j in range(n_cat)],
                    axis=1,
                )

            s = jnp.dot(lhs(hh), w, preferred_element_type=F32) + jnp.dot(
                lhs(hl), w, preferred_element_type=F32
            )
            for k in range(size):
                slot = (i % 2) * 2 + k if isinstance(i, int) else k
                for par in range(2):
                    at = k * lv.rows + par * lv.half
                    for c in range(2):
                        ss[slot, 2 * c + par, 8 : 8 + lv.half] = s[
                            at : at + lv.half, LANES * c : LANES * c + LANES
                        ]
                t = t0 + k
                for at in range(0, lv.half, chunk):

                    def rows_of(n, shift=0):
                        return ss[slot, n, pl.ds(8 + at + shift, chunk)]

                    even = (
                        (-11.0 / 3.0) * rows_of(0) + (-46.0 / 3.0) * rows_of(2)
                    ) + ((rows_of(1) + rows_of(1, -1)) + (rows_of(2, -1) + rows_of(2, 1)))
                    odd = ((-16.0 / 3.0) * rows_of(1) + (-80.0 / 3.0) * rows_of(3)) + (
                        rows_of(0) + rows_of(0, 1)
                    )
                    for par, val in enumerate((even, odd)):
                        edge = None
                        if at < lv.parts or at + chunk > lv.half - lv.parts:
                            edge = zm[par, at : at + chunk]
                        use(t, par, slice(par * lv.half + at, par * lv.half + at + chunk), val, edge)

        loop(count // size, group, 4)

    def wide(v, n):
        return jnp.broadcast_to(v[0:1], (n, LANES))

    def masked(v, edge):
        return v if edge is None else v * edge

    def n_rows(rows):
        return rows.stop - rows.start

    def own(t):
        return own_lo <= t < own_lo + own_n

    def reach(below, above):
        lo = (H - below) // lv0.group
        hi = (H + bx - 1 + above) // lv0.group
        return lo, hi - lo + 1

    def use_residual(t, par, rows, av, edge):
        r = r0[t, rows] - av
        r0[t, rows] = r
        d = masked(wide(iv0[t, par], n_rows(rows)) * r, edge)
        if own(t):
            acc0[t - own_lo, rows] = d0[t + 1, rows] + d
        d0[t + 1, rows] = d

    def use_step(t, par, rows, av, edge):
        r = r0[t, rows] - av
        r0[t, rows] = r
        d = KEEP * d0[t + 1, rows] + masked(
            (RATIO * wide(iv0[t, par], n_rows(rows))) * r, edge
        )
        if own(t):
            acc0[t - own_lo, rows] += d
        d0[t + 1, rows] = d

    def use_down(t, par, rows, av, edge):
        r0[t, rows] = masked((r0[t, rows] - av) * wide(mk0[t], n_rows(rows)), edge)

    lo_a, n_a = reach(6, 5)
    lo_b, n_b = reach(4, 3)
    load_w.wait()
    stage(lv0, d0, hh0, hl0, lo_a, n_a)
    sweep(lv0, hh0, hl0, weights('wa0'), ss0, zm0, lo_a, n_a, use_residual)
    stage(lv0, d0, hh0, hl0, lo_b, n_b)
    sweep(lv0, hh0, hl0, weights('wa0'), ss0, zm0, lo_b, n_b, use_step)
    stage(lv0, d0, hh0, hl0, lo_b, n_b)
    sweep(lv0, hh0, hl0, weights('wa0'), ss0, zm0, lo_b, n_b, use_down)

    def restricted(parts, w):
        hi, lo = zip(*[split(p) for p in parts])
        return jnp.dot(
            jnp.concatenate(hi, axis=1), w, preferred_element_type=F32
        ) + jnp.dot(jnp.concatenate(lo, axis=1), w, preferred_element_type=F32)

    x = restricted([r0[lo_b + i] for i in range(n_b)], weights('wr0'))
    xs0[0] = x[: lv0.half]
    xs0[1] = x[lv0.half :]
    def pick(ref, par, start, n):
        return ref[par, pl.ds(start, n, stride=2)]

    def z_restricted(ref, even0, odd0, n):
        even = (
            0.5 * pick(ref, 0, even0, n)
            + 0.1875 * (pick(ref, 1, odd0, n) + pick(ref, 1, odd0 + 1, n))
            - 0.0625 * (pick(ref, 1, odd0 - 1, n) + pick(ref, 1, odd0 + 2, n))
        )
        odd = 0.5 * pick(ref, 0, even0 + 1, n) + 0.375 * (
            pick(ref, 1, odd0 + 1, n) + pick(ref, 1, odd0 + 2, n)
        )
        return even, odd

    even, odd = z_restricted(xs0, zh, zh - 1, half_c)
    lane_c = lax.broadcasted_iota(jnp.int32, (half_c, LANES), 1)
    packed = jnp.where(lane_c < LANES // 2, even, odd)
    blk[...] = packed

    def g_copy(n):
        st = x_steps[n]
        return remote(blk, line.at[st[4]], gsend.at[n], grecv.at[n], (st[0], iy, iz))

    def p_copy(n, m, jx):
        to, _, _, jy, zs = plane_steps[n]
        if zs is None:
            src, dst = pl.ds(0, half_c), pl.ds(zq, half_c)
        else:
            src, dst = pl.ds(zs[5], zq), pl.ds(zs[6], zq)
        from_ref = blk if m == 0 else line.at[jx]
        return remote(
            from_ref.at[src], land.at[jy, jx, dst], psend.at[n, m], precv.at[n, m], to
        )

    sources = [(None, own_x)] + [(st[3], st[5]) for st in x_steps]
    for n, st in enumerate(x_steps):
        when(st[1], lambda: g_copy(n).start())
    for m, (ok, jx) in enumerate(sources):

        def act():
            if m:
                g_copy(m - 1).wait_recv()
            for n, st in enumerate(plane_steps):
                when(st[1], lambda: p_copy(n, m, jx).start())
            land[own_y, jx, zq : zq + half_c] = packed if m == 0 else line[jx]

        when(ok, act)
    for m, (ok, jx) in enumerate(sources):

        def act():
            for n, st in enumerate(plane_steps):
                when(st[2], lambda: p_copy(n, m, jx).wait_recv())

        when(ok, act)

    per = cx // lv1.group
    lane_h = lax.broadcasted_iota(jnp.int32, (lv1.half, LANES), 1) // gs

    def place_block(jx):
        blocks = [land[jy, jx] for jy in range(wy)]
        for s in range(per):
            t = jx * per + s
            for par in range(2):
                at = par * (LANES // 2) + s * gs
                val = None
                for jy in range(wy):
                    shift = (jy * gs - at) % LANES
                    v = pltpu.roll(blocks[jy], shift, 1) if shift else blocks[jy]
                    if val is None:
                        val = v if wy == wyp else jnp.where(lane_h == jy, v, 0.0)
                    else:
                        val = jnp.where(lane_h == jy, v, val)
                rows = slice(par * lv1.half, par * lv1.half + lv1.half)
                r1[t, rows] = val
                d = (wide(iv1[t, par], lv1.half) * zm1[par]) * val
                d1[t + 1, rows] = d
                acc1[t, rows] = d

    loop(wx, place_block, 4)

    def use_step1(t, par, rows, av, edge):
        r = r1[t, rows] - av
        r1[t, rows] = r
        d = KEEP * d1[t + 1, rows] + masked(
            (RATIO * wide(iv1[t, par], n_rows(rows))) * r, edge
        )
        d1[t + 1, rows] = d
        acc1[t, rows] += d

    def use_down1(t, par, rows, av, edge):
        r1[t, rows] = masked((r1[t, rows] - av) * wide(mk1[t], n_rows(rows)), edge)

    n1 = lv1.tiles
    stage(lv1, d1, hh1, hl1, 0, n1)
    sweep(lv1, hh1, hl1, weights('wa1'), ss1, zm1, 0, n1, use_step1)
    stage(lv1, d1, hh1, hl1, 0, n1)
    sweep(lv1, hh1, hl1, weights('wa1'), ss1, zm1, 0, n1, use_down1)

    ratio = 2 * lv2.group // lv1.group
    r_lo = (-3) // lv1.group
    r_hi = (2 * lv2.group + 1) // lv1.group
    wr1 = weights('wr1')
    for t in range(lv2.tiles):
        a, e = max(0, ratio * t + r_lo), min(n1 - 1, ratio * t + r_hi)
        skip = (a - (ratio * t + r_lo)) * LANES
        x = restricted(
            [r1[i] for i in range(a, e + 1)], wr1[skip : skip + (e + 1 - a) * LANES]
        )
        xs1[0, 8 : 8 + lv1.half] = x[: lv1.half]
        xs1[1, 8 : 8 + lv1.half] = x[lv1.half :]
        for par, val in enumerate(z_restricted(xs1, 8, 7, lv2.half)):
            rows = slice(par * lv2.half, par * lv2.half + lv2.half)
            r2[t, rows] = val
            d2[t + 1, rows] = (wide(iv2[t, par], lv2.half) * zm2[par]) * val

    def use_last(t, par, rows, av, edge):
        r = r2[t, rows] - av
        step = masked((RATIO * wide(iv2[t, par], n_rows(rows))) * r, edge)
        lo = rows.start - par * lv2.half
        up2[t, par, lo : lo + n_rows(rows)] = (1.0 + KEEP) * d2[t + 1, rows] + step

    stage(lv2, d2, hh2, hl2, 0, lv2.tiles)
    sweep(lv2, hh2, hl2, weights('wa2'), ss2, zm2, 0, lv2.tiles, use_last)

    n2 = lv2.half
    wp1 = weights('wp1')
    for t in range(lv2.tiles):
        e2, o2, e3 = up2[t, 0, 0:n2], up2[t, 1, 0:n2], up2[t, 0, 1 : n2 + 1]
        zp1[t, pl.ds(0, n2, stride=2)] = e2
        zp1[t, pl.ds(1, n2, stride=2)] = o2
        zp1[t, pl.ds(lv1.half, n2, stride=2)] = 0.375 * e2 + 0.75 * o2 - 0.125 * e3
        zp1[t, pl.ds(lv1.half + 1, n2, stride=2)] = 0.75 * o2 + 0.375 * e3 - 0.125 * e2
        zh1[t], zl1[t] = split(zp1[t])
    for t in range(lv2.tiles):
        n_in = min(2, lv2.tiles - t)
        w = wp1[: n_in * LANES]
        e = jnp.dot(
            jnp.concatenate([zh1[t + i] for i in range(n_in)], axis=1), w,
            preferred_element_type=F32,
        ) + jnp.dot(
            jnp.concatenate([zl1[t + i] for i in range(n_in)], axis=1), w,
            preferred_element_type=F32,
        )
        for k in range(ratio):
            to = ratio * t + k
            if to < n1:
                for par in range(2):
                    rows = slice(par * lv1.half, par * lv1.half + lv1.half)
                    v = e[rows, LANES * k : LANES * k + LANES] * (
                        wide(mk1[to], lv1.half) * zm1[par]
                    )
                    d1[to + 1, rows] = v
                    acc1[to, rows] += v

    def use_up1(t, par, rows, av, edge):
        r = r1[t, rows] - av
        r1[t, rows] = r
        d1[t + 1, rows] = masked(wide(iv1[t, par], n_rows(rows)) * r, edge)

    def use_final1(t, par, rows, av, edge):
        r = r1[t, rows] - av
        c1[t + 2, rows] = (acc1[t, rows] + (1.0 + KEEP) * d1[t + 1, rows]) + masked(
            (RATIO * wide(iv1[t, par], n_rows(rows))) * r, edge
        )

    stage(lv1, d1, hh1, hl1, 0, n1)
    sweep(lv1, hh1, hl1, weights('wa1'), ss1, zm1, 0, n1, use_up1)
    stage(lv1, d1, hh1, hl1, 0, n1)
    sweep(lv1, hh1, hl1, weights('wa1'), ss1, zm1, 0, n1, use_final1)

    up = 2 * lv1.group // lv0.group
    tau_lo = (lo_b - own_lo) // up
    tau_hi = (lo_b + n_b - 1 - own_lo) // up
    n_tau = tau_hi + 2 - tau_lo
    jn = (lv0.half // 2 + 7) // 8 * 8
    lane_j = lax.broadcasted_iota(jnp.int32, (jn, LANES), 1) // gs
    bad = ((lane_j == 0) & (own_y == 0)) | ((lane_j == 2) & (own_y == wy - 1))
    turn = lax.rem(1 - own_y + wyp, wyp) * gs
    first = ZR // 2 - zh // 2
    wp0 = weights('wp0')
    for i in range(n_tau):
        at = own_x * per + (tau_lo + i + 2)

        def rows_of(par, start):
            v = pltpu.roll(c1[at, pl.ds(par * lv1.half + start, jn)], turn, 1)
            return jnp.where(bad, 0.0, v)

        e2, o2, e3 = rows_of(0, first), rows_of(1, first), rows_of(0, first + 1)
        zp0[i, pl.ds(0, jn, stride=2)] = e2
        zp0[i, pl.ds(1, jn, stride=2)] = o2
        zp0[i, pl.ds(lv0.half, jn, stride=2)] = 0.375 * e2 + 0.75 * o2 - 0.125 * e3
        zp0[i, pl.ds(lv0.half + 1, jn, stride=2)] = 0.75 * o2 + 0.375 * e3 - 0.125 * e2
        zh0[i], zl0[i] = split(zp0[i, 0 : lv0.rows])
    for i in range(n_tau - 1):
        e = jnp.dot(
            jnp.concatenate([zh0[i], zh0[i + 1]], axis=1), wp0,
            preferred_element_type=F32,
        ) + jnp.dot(
            jnp.concatenate([zl0[i], zl0[i + 1]], axis=1), wp0,
            preferred_element_type=F32,
        )
        for k in range(up):
            t = own_lo + up * (tau_lo + i) + k
            if lo_b <= t < lo_b + n_b:
                for par in range(2):
                    rows = slice(par * lv0.half, par * lv0.half + lv0.half)
                    v = e[rows, LANES * k : LANES * k + LANES] * (
                        wide(mk0[t], lv0.half) * zm0[par]
                    )
                    d0[t + 1, rows] = v
                    if own(t):
                        acc0[t - own_lo, rows] += v

    def use_up(t, par, rows, av, edge):
        r = r0[t, rows] - av
        r0[t, rows] = r
        d0[t + 1, rows] = masked(wide(iv0[t, par], n_rows(rows)) * r, edge)

    def use_final(t, par, rows, av, edge):
        r = r0[t, rows] - av
        acc0[t - own_lo, rows] += (1.0 + KEEP) * d0[t + 1, rows] + (
            RATIO * wide(iv0[t, par], n_rows(rows))
        ) * r

    lo_c, n_c = reach(2, 1)
    stage(lv0, d0, hh0, hl0, lo_c, n_c)
    sweep(lv0, hh0, hl0, weights('wa0'), ss0, zm0, lo_c, n_c, use_up)
    stage(lv0, d0, hh0, hl0, own_lo, own_n)
    sweep(lv0, hh0, hl0, weights('wa0'), ss0, zm0, own_lo, own_n, use_final)

    for i in range(own_n):
        for par in range(2):
            lo = par * lv0.half + zh
            tmp[pl.ds(par, hb, stride=2)] = acc0[i, lo : lo + hb]
        v = tmp[...].T.reshape(lv0.group, yh0, bz)
        out_ref[lv0.group * i : lv0.group * i + lv0.group] = v[:, H : H + by]

    for n, off in enumerate(xy_offs):
        for k in range(2):
            when(xy_step(off)[1], lambda: halo_copy(n, k).wait_send())
    for m in range(len(z_steps)):
        for n in range(len(spots)):
            when(strip_ok(n, m, 1), lambda: strip_copy(n, m).wait_send())
    for n, st in enumerate(x_steps):
        when(st[1], lambda: g_copy(n).wait_send())
    for m, (ok, jx) in enumerate(sources):

        def act():
            for n, st in enumerate(plane_steps):
                when(st[1], lambda: p_copy(n, m, jx).wait_send())

        when(ok, act)


def local(mesh_shape, u, b):
    nx, ny, nz = (mesh_shape[a] for a in ("gx", "gy", "gz"))
    bx, by, bz = u.shape
    cx, cy, cz = bx // 2, by // 2, bz // 2
    wx = nx if nx <= 2 * REACH + 1 else 2 * REACH + 1
    wy = ny if ny <= 2 * REACH + 1 else 2 * REACH + 1
    wyp = 4 if wy <= 4 else 8
    gs = LANES // wyp
    yh0 = by + 2 * H
    xg0 = LANES // yh0
    lv0 = Level(
        xg0, (bx + 2 * H) // xg0, yh0, (bz + 2 * H) // 2, lambda x, y: x * yh0 + y, H // 2
    )
    xg1 = gs // cy
    lv1 = Level(
        xg1, cx * wx // xg1, cy * wy, (cz + 2 * ZR) // 2,
        lambda x, y: (y // cy) * gs + x * cy + y % cy, ZR // 2,
    )
    y2 = cy * wy // 2
    yh2 = 16 if y2 <= 16 else 32
    xg2 = LANES // yh2
    lv2 = Level(
        xg2, -(-(cx * wx // 2) // xg2), y2, (cz + 2 * ZR) // 4, lambda x, y: x * yh2 + y,
        ZR // 4,
    )

    own_lo = H // xg0
    lo_b = (H - 4) // xg0
    n_b = (H + bx - 1 + 3) // xg0 - lo_b + 1
    px = []
    for x in range(cx):
        for s, w in restrict_taps(x):
            f = H + 2 * x + s
            px.append(((0, x), f // xg0 - lo_b, f % xg0, w))
    py = [(y, H + 2 * y + s, w) for y in range(cy) for s, w in restrict_taps(y)]
    once = plane_matrix(n_b, 1, px, py, lv0.at, lambda x, y: x * cy + y)
    m_r0 = once + np.roll(once, LANES // 2, axis=1)

    r_lo, r_hi = (-3) // xg1, (2 * xg2 + 1) // xg1
    px = []
    for x in range(xg2):
        for s, w in restrict_taps(x):
            f = 2 * x + s
            px.append(((0, x), f // xg1 - r_lo, f % xg1, w))
    py = [
        (y, 2 * y + s, w) for y in range(y2) for s, w in restrict_taps(y)
        if 0 <= 2 * y + s < cy * wy
    ]
    m_r1 = plane_matrix(r_hi - r_lo + 1, 1, px, py, lv1.at, lv2.at)

    ratio = 2 * xg2 // xg1
    px = []
    for f in range(2 * xg2):
        for c, w in prolong_taps(f):
            px.append(((f // xg1, f % xg1), c // xg2, c % xg2, w))
    py = [
        (f, c, w) for f in range(cy * wy) for c, w in prolong_taps(f) if 0 <= c < y2
    ]
    m_p1 = plane_matrix(2, ratio, px, py, lv2.at, lv1.at)

    up = 2 * xg1 // xg0
    px = []
    for f in range(2 * xg1):
        for c, w in prolong_taps(f):
            px.append(((f // xg0, f % xg0), c // xg1, c % xg1, w))
    py = [
        (f + H, c + cy, w) for f in range(-H, by + H) for c, w in prolong_taps(f)
        if -cy <= c < 2 * cy
    ]
    m_p0 = plane_matrix(2, up, px, py, lv1.at, lv0.at)

    parts, stack, row = {}, [], 0
    for name, m in (
        ("wa0", operator_matrix(lv0)), ("wa1", operator_matrix(lv1)),
        ("wa2", operator_matrix(lv2)), ("wr0", m_r0), ("wr1", m_r1), ("wp1", m_p1),
        ("wp0", m_p0),
    ):
        if m.shape[1] == LANES:
            m = np.pad(m, ((0, m.shape[0] % 2), (0, 0)))
            half = m.shape[0] // 2
            assert half % 16 == 0
            parts[name] = [(row, 0, half, LANES), (row, LANES, half, LANES)]
            stack.append(np.concatenate([m[:half], m[half:]], axis=1))
            row += half
        else:
            parts[name] = []
            for c in range(0, m.shape[1], 256):
                parts[name].append((row, 0, m.shape[0], min(256, m.shape[1] - c)))
                piece = m[:, c : c + 256]
                stack.append(np.pad(piece, ((0, 0), (0, 256 - piece.shape[1]))))
                row += m.shape[0]
    consts = to_bf16(np.concatenate(stack, axis=0))
    vm = lambda *s: pltpu.VMEM(s, F32)
    bm = lambda *s: pltpu.VMEM(s, BF16)
    dma = lambda *s: pltpu.SemaphoreType.DMA(s)

    def per_level(lv):
        t, n = lv.tiles, lv.rows
        return (
            vm(t + 2, n, LANES), vm(t, n, LANES), vm(t, n, LANES),
            bm(t + 2, n, LANES), bm(t + 2, n, LANES), vm(4, 4, lv.half + 16, LANES),
            vm(t, 2, 8, LANES), vm(t, 8, LANES), vm(2, lv.half, LANES),
        )

    p0, p1, p2 = per_level(lv0), per_level(lv1), per_level(lv2)
    tau_lo = (lo_b - own_lo) // up
    n_tau = (lo_b + n_b - 1 - own_lo) // up + 2 - tau_lo
    jn = (lv0.half // 2 + 7) // 8 * 8
    geo = (nx, ny, nz, bx, by, bz, wx, wy, wyp)
    near, side = (3 if nx > 1 else 1), (3 if ny > 1 else 1)
    n_z = 0 if nz == 1 else 1 if nz == 2 else 2
    n_x = max(1, nx - 1 if wx == nx else 2 * REACH)
    n_y = ny - 1 if wy == ny else 2 * REACH
    n_p = max(1, (n_y + 1) * (n_z + 1) - 1)
    n_xy, n_s = max(1, near * side - 1), near * side
    return pl.pallas_call(
        functools.partial(kernel, geo, lv0, lv1, lv2, parts),
        out_shape=jax.ShapeDtypeStruct(u.shape, F32),
        in_specs=[pl.BlockSpec(memory_space=pl.ANY)] * 3,
        out_specs=pl.BlockSpec(memory_space=pltpu.VMEM),
        scratch_shapes=[
            bm(*consts.shape), vm(bx, by, bz), vm(bx, by, bz),
            vm(bx + 2 * H, yh0, bz), vm(bx + 2 * H, yh0, bz), vm(bz, LANES),
            vm(xg0, yh0, bz), vm(2, 3, 2, bx // xg0, H, LANES),
            vm(2, 3, 2, lv0.tiles, H, LANES),
            *p0, *p1, vm(lv1.tiles + 4, lv1.rows, LANES), p2[0], p2[1], *p2[3:],
            vm(2, lv0.half, LANES), vm(2, lv1.half + 16, LANES), vm(cz // 2, LANES),
            vm(wx, cz // 2, LANES), vm(wy, wx, lv1.half, LANES),
            vm(lv2.tiles, 2, lv2.half + 8, LANES), vm(lv2.tiles, lv1.rows, LANES),
            vm(n_tau, lv0.half + 2 * jn, LANES),
            bm(lv2.tiles, lv1.rows, LANES), bm(lv2.tiles, lv1.rows, LANES),
            bm(n_tau, lv0.rows, LANES), bm(n_tau, lv0.rows, LANES),
            dma(3), dma(n_xy, 2), dma(n_xy, 2), dma(n_s, max(1, n_z)), dma(n_s, max(1, n_z)),
            dma(n_x), dma(n_x), dma(n_p, n_x + 1), dma(n_p, n_x + 1),
        ],
        compiler_params=pltpu.CompilerParams(
            collective_id=0, has_side_effects=True, vmem_limit_bytes=60 * 1024 * 1024
        ),
    )(u, b, consts)


def solution(mesh):
    placed = P("gx", "gy", "gz")
    return jax.shard_map(
        functools.partial(local, dict(mesh.shape)), mesh=mesh,
        in_specs=(placed, placed), out_specs=placed, check_vma=False,
    )
```

```python
import functools

import jax
import jax.numpy as jnp
import numpy as np
from jax import lax
from jax.experimental import pallas as pl
from jax.experimental.pallas import tpu as pltpu
from jax.sharding import PartitionSpec as P

F32 = jnp.float32
BF16 = jnp.bfloat16
MESH = pl.DeviceIdType.MESH
H = 8
ZR = 32
REACH = 3
LANES = 128

RHO0 = 1.0 / 1.2
RHO1 = 1.0 / (2.4 - RHO0)
FIRST = 1.0 / 1.32
KEEP = RHO1 * RHO0
STEP = 2.0 * RHO1 / 1.1
RATIO = STEP / FIRST
UNIT = 2700.0


def restrict_taps(g):
    if g % 2 == 0:
        return ((-3, -0.125), (-1, 0.375), (0, 1.0), (1, 0.375), (3, -0.125))
    return ((-1, 0.75), (0, 1.0), (1, 0.75))


def prolong_taps(f):
    if f % 2 == 0:
        return ((f // 2, 1.0),)
    q = f // 4
    if f % 4 == 1:
        return ((2 * q, 0.375), (2 * q + 1, 0.75), (2 * q + 2, -0.125))
    return ((2 * q, -0.125), (2 * q + 1, 0.75), (2 * q + 2, 0.375))


def stiff_taps(i):
    if i % 2 == 0:
        return {-2: 1, -1: -8, 0: 14, 1: -8, 2: 1}
    return {-1: -8, 0: 16, 1: -8}


def mass_taps(i):
    if i % 2 == 0:
        return {-2: -1, -1: 2, 0: 8, 1: 2, 2: -1}
    return {-1: 2, 0: 16, 1: 2}


class Level:
    def __init__(self, group, tiles, height, half, at, parts):
        self.group, self.tiles, self.height, self.half, self.at = group, tiles, height, half, at
        self.parts = parts
        self.rows = 2 * half
        self.paired = group >= 4


def operator_matrix(lv):
    k = 256 if lv.paired else 384
    m = np.zeros((k, 256), np.float64)
    for x in range(lv.group):
        for y in range(lv.height):
            for ox, mx in mass_taps(x).items():
                kx = stiff_taps(x)[ox]
                p = x + ox
                if lv.paired:
                    block = (p + lv.group // 2) // lv.group
                else:
                    block = p // lv.group + 1
                for oy, my in mass_taps(y).items():
                    ky = stiff_taps(y)[oy]
                    if not 0 <= y + oy < lv.height:
                        continue
                    row = block * LANES + lv.at(p % lv.group, y + oy)
                    both, mixed = mx * my, kx * my + mx * ky
                    m[row, lv.at(x, y)] = -8 * both + 2 * mixed
                    m[row, LANES + lv.at(x, y)] = both - mixed
    return m


def plane_matrix(n_in, n_out, pairs_x, pairs_y, at_in, at_out):
    m = np.zeros((n_in * LANES, n_out * LANES), np.float64)
    for (to, xo), ti, xi, wx in pairs_x:
        for yo, yi, wy in pairs_y:
            m[ti * LANES + at_in(xi, yi), to * LANES + at_out(xo, yo)] += wx * wy
    return m


def to_bf16(m):
    out = jnp.asarray(m, BF16)
    assert np.array_equal(np.asarray(m, jnp.bfloat16).astype(np.float64), m)
    return out


def split(v):
    hi = v.astype(BF16)
    return hi, (v - hi.astype(F32)).astype(BF16)


def loop(count, body, most=9):
    if count <= most:
        for i in range(count):
            body(i)
    else:

        def step(i, carry):
            body(i)
            return carry

        lax.fori_loop(0, count, step, 0)


def kernel(
    geo, lv0, lv1, lv2, parts, u_hbm, b_hbm, w_hbm, out_ref, *refs,
):
    (wall, u_ref, b_ref, ue, be, tmp, pad, strip_out, strip_in,
     d0, r0, acc0, hh0, hl0, ss0, iv0, mk0, zm0,
     d1, r1, acc1, hh1, hl1, ss1, iv1, mk1, zm1, c1,
     d2, r2, hh2, hl2, ss2, iv2, mk2, zm2,
     xs0, xs1, blk, line, land, up2, zp1, zp0, zh1, zl1, zh0, zl0,
     wsem, xysend, xyrecv, zsend, zrecv, gsend, grecv, psend, precv) = refs
    nx, ny, nz, bx, by, bz, wx, wy, wyp = geo
    ix, iy, iz = lax.axis_index("gx"), lax.axis_index("gy"), lax.axis_index("gz")
    place, counts = (ix, iy, iz), (nx, ny, nz)
    full_x, full_y = wx == nx, wy == ny
    cx, cy, cz = bx // 2, by // 2, bz // 2
    start_x = 0 if full_x else ix - REACH
    start_y = 0 if full_y else iy - REACH
    own_x = ix if full_x else REACH
    own_y = iy if full_y else REACH

    def both(*oks):
        ok = None
        for o in oks:
            if o is not None:
                ok = o if ok is None else ok & o
        return ok

    def when(ok, act):
        if ok is None:
            act()
        else:
            pl.when(ok)(act)

    def unless(ok, act):
        if ok is not None:
            pl.when(jnp.logical_not(ok))(act)

    def inside(axis, p):
        return (p >= 0) & (p < counts[axis])

    def shifted(axis, off):
        if off == 0:
            return (place[axis], None, place[axis], None)
        to, source = place[axis] + off, place[axis] - off
        return (to, inside(axis, to), source, inside(axis, source))

    def line_steps(axis, full):
        p, n = place[axis], counts[axis]
        if full:
            steps = []
            for k in sorted(range(1, n), key=lambda k: min(k, n - k)):
                to, source = lax.rem(p + k, n), lax.rem(p + n - k, n)
                steps.append((to, None, source, None, p, source))
            return steps
        offs = sorted((o for o in range(-REACH, REACH + 1) if o), key=abs)
        return [shifted(axis, o) + (REACH - o, REACH - o) for o in offs]

    zq, half_c = ZR // 2, cz // 2
    x_steps = line_steps(0, full_x)
    y_steps = line_steps(1, full_y)
    if nz == 2:
        z_steps = [
            (1 - iz, None, 1 - iz, None, 1 - iz,
             pl.multiple_of((1 - iz) * (half_c - zq), 8),
             pl.multiple_of(iz * (zq + half_c), 8))
        ]
    elif nz > 2:
        z_steps = [
            shifted(2, 1) + (1, half_c - zq, 0), shifted(2, -1) + (0, 0, zq + half_c)
        ]
    else:
        z_steps = []
    plane_steps = [
        ((ix, ys[0], iz), ys[1], ys[3], ys[4], None) for ys in y_steps
    ] + [
        ((ix, iy, zs[0]), zs[1], zs[3], own_y, zs) for zs in z_steps
    ] + [
        ((ix, ys[0], zs[0]), both(ys[1], zs[1]), both(ys[3], zs[3]), ys[4], zs)
        for zs in z_steps for ys in y_steps
    ]
    near = [0] + ([-1, 1] if nx > 1 else [])
    side = [0] + ([-1, 1] if ny > 1 else [])
    xy_offs = [(a, c) for a in near for c in side if a or c]

    def xy_step(off):
        xs, ys = shifted(0, off[0]), shifted(1, off[1])
        return (xs[0], ys[0]), both(xs[1], ys[1]), both(xs[3], ys[3])

    greet = [((st[0], iy, iz), st[1], st[3]) for st in x_steps]
    greet += [(st[0], st[1], st[2]) for st in plane_steps]
    for off in xy_offs:
        if off[0]:
            to, ok, ok_from = xy_step(off)
            if off[1]:
                greet.append((to + (iz,), ok, ok_from))
            for zs in z_steps:
                greet.append((to + (zs[0],), both(ok, zs[1]), both(ok_from, zs[3])))

    barrier = pltpu.get_barrier_semaphore()
    total = 0
    for to, ok, ok_from in greet:
        total = total + (1 if ok_from is None else ok_from.astype(jnp.int32))

        def signal():
            pl.semaphore_signal(barrier, inc=1, device_id=to, device_id_type=MESH)

        when(ok, signal)

    load_u = pltpu.make_async_copy(u_hbm, u_ref, wsem.at[0])
    load_b = pltpu.make_async_copy(b_hbm, b_ref, wsem.at[1])
    load_w = pltpu.make_async_copy(w_hbm, wall, wsem.at[2])
    load_u.start()
    load_b.start()
    load_w.start()

    def remote(src, dst, ss, rs, to):
        return pltpu.make_async_remote_copy(
            src_ref=src, dst_ref=dst, send_sem=ss, recv_sem=rs,
            device_id=to, device_id_type=MESH,
        )

    def weights(name):
        blocks = []
        for row, lane, rows, lanes in parts[name]:
            blocks.append(wall[row : row + rows, lane : lane + lanes])
        if parts[name][0][3] == LANES:
            return jnp.concatenate(blocks, axis=0)
        return jnp.concatenate(blocks, axis=1)

    def cut(off, size, low, high):
        if off == 0:
            return slice(0, size), slice(H, H + size)
        if off > 0:
            return slice(size - low, size), slice(H - low, H)
        return slice(0, high), slice(H + size, H + size + high)

    fields = ((u_ref, ue, H, H - 1), (b_ref, be, H - 2, H - 3))

    def halo_cut(off, k):
        ref, ext, low, high = fields[k]
        sx, tx = cut(off[0], bx, low, high)
        sy, ty = cut(off[1], by, H, H)
        return ref, ext, sx, tx, sy, ty

    def zero(ref, *at):
        ref[at] = jnp.zeros_like(ref[at])

    def halo_copy(n, k):
        ref, ext, sx, tx, sy, ty = halo_cut(xy_offs[n], k)
        to = xy_step(xy_offs[n])[0] + (iz,)
        return remote(ref.at[sx, sy], ext.at[tx, ty], xysend.at[n, k], xyrecv.at[n, k], to)

    yh0 = by + 2 * H
    zh, hb = H // 2, bz // 2
    own_lo, own_n = H // lv0.group, bx // lv0.group
    edge_n = H // lv0.group
    spots = [(a, c) for a in near for c in side]

    def variant(c):
        return 0 if c == 0 else (1 if c > 0 else 2)

    def strip_cut(a):
        if a == 0:
            return slice(0, own_n), slice(own_lo, own_lo + own_n)
        if a > 0:
            return slice(own_n - edge_n, own_n), slice(0, edge_n)
        return slice(0, edge_n), slice(own_lo + own_n, own_lo + own_n + edge_n)

    def strip_copy(n, m):
        a, c = spots[n]
        zs = z_steps[m]
        src, dst = strip_cut(a)
        v, k = variant(c), zs[4]
        to = (shifted(0, a)[0], shifted(1, c)[0], zs[0])
        return remote(
            strip_out.at[k, v, :, src], strip_in.at[k, v, :, dst],
            zsend.at[n, m], zrecv.at[n, m], to,
        )

    def strip_ok(n, m, at):
        a, c = spots[n]
        return both(shifted(0, a)[at], shifted(1, c)[at], z_steps[m][at])

    zero(pad, slice(None), slice(0, H))
    zero(pad, slice(None), slice(H + by, yh0))
    lane_y = lax.broadcasted_iota(jnp.int32, (2 * zh, LANES), 1) % yh0
    load_u.wait()
    load_b.wait()
    for k, ref in enumerate((u_ref, b_ref)):
        for t in range(own_n):
            pad[:, H : H + by] = ref[lv0.group * t : lv0.group * t + lv0.group]
            tmp[...] = pad[...].reshape(LANES, bz).T
            for s, start in ((0, 0), (1, bz - H)):
                v = jnp.concatenate(
                    [tmp[pl.ds(start + par, zh, stride=2)] for par in range(2)], axis=0
                )
                strip_out[s, 0, k, t] = v
                if ny > 1:
                    strip_out[s, 1, k, t] = jnp.where(
                        lane_y < H, pltpu.roll(v, LANES - by, 1), 0.0
                    )
                    strip_out[s, 2, k, t] = jnp.where(
                        lane_y >= H + by, pltpu.roll(v, by, 1), 0.0
                    )

    pl.semaphore_wait(barrier, total)
    for m in range(len(z_steps)):
        for n in sorted(range(len(spots)), key=lambda n: -abs(spots[n][0]) - abs(spots[n][1])):
            when(strip_ok(n, m, 1), lambda: strip_copy(n, m).start())
    far_first = sorted(range(len(xy_offs)), key=lambda n: -abs(xy_offs[n][0] * xy_offs[n][1]))
    for n in far_first:
        when(xy_step(xy_offs[n])[1], lambda: halo_copy(n, 0).start())
    for n in far_first:
        when(xy_step(xy_offs[n])[1], lambda: halo_copy(n, 1).start())

    ue[H : H + bx, H : H + by] = u_ref[...]
    be[H : H + bx, H : H + by] = b_ref[...]
    for _, ext, low, high in fields:
        for at in (slice(0, H - low), slice(H + bx + high, 2 * H + bx)):
            if at.stop > at.start:
                zero(ext, at)
    for off in [(a, c) for a in (-1, 0, 1) for c in (-1, 0, 1) if a or c]:

        def clear():
            for k in range(2):
                _, ext, _, tx, _, ty = halo_cut(off, k)
                zero(ext, tx, ty)

        if off in xy_offs:
            unless(xy_step(off)[2], clear)
        else:
            clear()
    for s, rows in ((0, slice(zq + half_c, 2 * zq + half_c)), (1, slice(0, zq))):
        z_ok = inside(2, iz + (1 - 2 * s)) if nz > 1 else None
        for a in (-1, 0, 1):
            for c in (-1, 0, 1):

                def clear():
                    zero(strip_in, s, variant(c), slice(None), strip_cut(a)[1])

                if (a, c) in spots and nz > 1:
                    unless(both(shifted(0, a)[3], shifted(1, c)[3], z_ok), clear)
                else:
                    clear()

        def clear():
            zero(land, slice(None), slice(None), rows)

        if nz > 1:
            unless(z_ok, clear)
        else:
            clear()
    for st in x_steps:
        unless(st[3], lambda: zero(land, slice(None), st[5]))
    for st in y_steps:
        unless(st[3], lambda: zero(land, st[5]))

    def set_up(lv, level, iv, mk, zm, d, ss, x_first, y_first, z_first, x_at, y_at):
        lane = lax.broadcasted_iota(jnp.int32, (8, LANES), 1)
        row = lax.broadcasted_iota(jnp.int32, (lv.half, LANES), 0)
        xx, yy = x_at(lane), y_at(lane)
        x_even, y_even = xx % 2 == 0, yy % 2 == 0
        n_x, n_y, n_z = (nx * bx) >> level, (ny * by) >> level, (nz * bz) >> level
        gy = y_first + yy
        y_ok = (gy >= 0) & (gy < n_y) & (yy < lv.height)
        mass = lambda e: jnp.where(e, 8.0, 16.0) / 30.0
        stiff = lambda e: jnp.where(e, 14.0, 16.0) / 3.0
        my, ky, mx, kx = mass(y_even), stiff(y_even), mass(x_even), stiff(x_even)
        inv = []
        for kz, mz in ((14.0 / 3.0, 8.0 / 30.0), (16.0 / 3.0, 16.0 / 30.0)):
            inv.append((FIRST / UNIT) / (kx * my * mz + mx * ky * mz + mx * my * kz))

        def one(t):
            gx = x_first + t * lv.group + xx
            ok = jnp.where(y_ok & (gx >= 0) & (gx < n_x), 1.0, 0.0).astype(F32)
            mk[t] = ok
            iv[t, 0] = inv[0] * ok
            iv[t, 1] = inv[1] * ok

        loop(lv.tiles, one)
        for par in range(2):
            gz = z_first + 2 * row + par
            zm[par] = jnp.where((gz >= 0) & (gz < n_z), 1.0, 0.0).astype(F32)
        d[0] = jnp.zeros_like(d[0])
        d[lv.tiles + 1] = jnp.zeros_like(d[0])
        ss[:, :, 0:8] = jnp.zeros_like(ss[:, :, 0:8])
        ss[:, :, 8 + lv.half :] = jnp.zeros_like(ss[:, :, 8 + lv.half :])

    gs = LANES // wyp
    set_up(
        lv0, 0, iv0, mk0, zm0, d0, ss0, ix * bx - H, iy * by - H, iz * bz - H,
        lambda n: n // yh0, lambda n: n % yh0,
    )
    set_up(
        lv1, 1, iv1, mk1, zm1, d1, ss1, start_x * cx, start_y * cy, iz * cz - ZR,
        lambda n: (n % gs) // cy, lambda n: (n // gs) * cy + n % cy,
    )
    yh2 = LANES // lv2.group
    set_up(
        lv2, 2, iv2, mk2, zm2, d2, ss2, start_x * (cx // 2), start_y * (cy // 2),
        iz * (cz // 2) - ZR // 2, lambda n: n // yh2, lambda n: n % yh2,
    )
    c1[0:2] = jnp.zeros_like(c1[0:2])
    c1[lv1.tiles + 2 :] = jnp.zeros_like(c1[0:2])
    xs1[:, 0:8] = jnp.zeros_like(xs1[:, 0:8])
    xs1[:, 8 + lv1.half :] = jnp.zeros_like(xs1[:, 8 + lv1.half :])
    up2[...] = jnp.zeros_like(up2)

    def turn_field(k):
        ext = (ue, be)[k]
        for n, off in enumerate(xy_offs):
            when(xy_step(off)[2], lambda: halo_copy(n, k).wait_recv())
        for t in range(lv0.tiles):
            tmp[...] = ext[lv0.group * t : lv0.group * t + lv0.group].reshape(LANES, bz).T
            for par in range(2):
                val = tmp[pl.ds(par, hb, stride=2)]
                lo = par * lv0.half + zh
                if k == 0:
                    d0[t + 1, lo : lo + hb] = val
                else:
                    r0[t, lo : lo + hb] = UNIT * val - r0[t, lo : lo + hb]

    def fill_strips(k):
        for t in range(lv0.tiles):
            for s in range(2):
                v = (strip_in[s, 0, k, t] + strip_in[s, 1, k, t]) + strip_in[s, 2, k, t]
                for par in range(2):
                    lo = par * lv0.half + (0 if s else zh + hb)
                    rows, part = slice(lo, lo + zh), v[par * zh : par * zh + zh]
                    if k == 0:
                        d0[t + 1, rows] = part
                    else:
                        r0[t, rows] = UNIT * part - r0[t, rows]

    turn_field(0)
    for m in range(len(z_steps)):
        for n in range(len(spots)):
            when(strip_ok(n, m, 3), lambda: strip_copy(n, m).wait_recv())
    fill_strips(0)

    def stage(lv, d, hh, hl, lo, count):
        step = 48 if lv.rows % 48 == 0 else min(lv.rows, 64)
        lane = lax.broadcasted_iota(jnp.int32, (step, LANES), 1)
        if lv is lv1:
            plane = (lane % gs) // cy
        else:
            plane = lane // (LANES // lv.group)
        low = plane < lv.group // 2

        def one(i):
            t = lo + i
            for s in range(0, lv.rows, step):
                rows = slice(s, s + step)
                if lv.paired:
                    v = jnp.where(low, d[t + 1, rows], d[t, rows])
                else:
                    v = d[t, rows]
                hh[t, rows], hl[t, rows] = split(v)

        loop(count + (1 if lv.paired else 2), one)

    def sweep(lv, hh, hl, w, ss, zm, lo, count, use):
        chunk = 24 if lv.half % 24 == 0 else 32
        n_cat = 2 if lv.paired else 3
        size = 2 if count % 2 == 0 else 1

        def group(i):
            t0 = lo + size * i

            def lhs(h):
                return jnp.concatenate(
                    [h[pl.ds(t0 + j, size)].reshape(size * lv.rows, LANES) for j in range(n_cat)],
                    axis=1,
                )

            s = jnp.dot(lhs(hh), w, preferred_element_type=F32) + jnp.dot(
                lhs(hl), w, preferred_element_type=F32
            )
            for k in range(size):
                slot = (i % 2) * 2 + k if isinstance(i, int) else k
                for par in range(2):
                    at = k * lv.rows + par * lv.half
                    for c in range(2):
                        ss[slot, 2 * c + par, 8 : 8 + lv.half] = s[
                            at : at + lv.half, LANES * c : LANES * c + LANES
                        ]
                t = t0 + k
                for at in range(0, lv.half, chunk):

                    def rows_of(n, shift=0):
                        return ss[slot, n, pl.ds(8 + at + shift, chunk)]

                    even = (
                        (-11.0 / 3.0) * rows_of(0) + (-46.0 / 3.0) * rows_of(2)
                    ) + ((rows_of(1) + rows_of(1, -1)) + (rows_of(2, -1) + rows_of(2, 1)))
                    odd = ((-16.0 / 3.0) * rows_of(1) + (-80.0 / 3.0) * rows_of(3)) + (
                        rows_of(0) + rows_of(0, 1)
                    )
                    for par, val in enumerate((even, odd)):
                        edge = None
                        if at < lv.parts or at + chunk > lv.half - lv.parts:
                            edge = zm[par, at : at + chunk]
                        use(t, par, slice(par * lv.half + at, par * lv.half + at + chunk), val, edge)

        loop(count // size, group, 4)

    def wide(v, n):
        return jnp.broadcast_to(v[0:1], (n, LANES))

    def masked(v, edge):
        return v if edge is None else v * edge

    def n_rows(rows):
        return rows.stop - rows.start

    def own(t):
        return own_lo <= t < own_lo + own_n

    def reach(below, above):
        lo = (H - below) // lv0.group
        hi = (H + bx - 1 + above) // lv0.group
        return lo, hi - lo + 1

    def use_product(t, par, rows, av, edge):
        r0[t, rows] = av

    def first_step(t):
        size = 24 if lv0.half % 24 == 0 else 8
        for par in range(2):
            for at in range(0, lv0.half, size):
                rows = slice(par * lv0.half + at, par * lv0.half + at + size)
                d = wide(iv0[t, par], size) * r0[t, rows] * zm0[par, at : at + size]
                if own(t):
                    acc0[t - own_lo, rows] = d0[t + 1, rows] + d
                d0[t + 1, rows] = d

    def use_step(t, par, rows, av, edge):
        r = r0[t, rows] - av
        r0[t, rows] = r
        d = KEEP * d0[t + 1, rows] + masked(
            (RATIO * wide(iv0[t, par], n_rows(rows))) * r, edge
        )
        if own(t):
            acc0[t - own_lo, rows] += d
        d0[t + 1, rows] = d

    def use_down(t, par, rows, av, edge):
        r0[t, rows] = masked((r0[t, rows] - av) * wide(mk0[t], n_rows(rows)), edge)

    lo_a, n_a = reach(6, 5)
    lo_b, n_b = reach(4, 3)
    load_w.wait()
    stage(lv0, d0, hh0, hl0, lo_a, n_a)
    sweep(lv0, hh0, hl0, weights('wa0'), ss0, zm0, lo_a, n_a, use_product)
    turn_field(1)
    fill_strips(1)
    for t in range(lo_a, lo_a + n_a):
        first_step(t)
    stage(lv0, d0, hh0, hl0, lo_b, n_b)
    sweep(lv0, hh0, hl0, weights('wa0'), ss0, zm0, lo_b, n_b, use_step)
    stage(lv0, d0, hh0, hl0, lo_b, n_b)
    sweep(lv0, hh0, hl0, weights('wa0'), ss0, zm0, lo_b, n_b, use_down)

    def restricted(parts, w):
        hi, lo = zip(*[split(p) for p in parts])
        return jnp.dot(
            jnp.concatenate(hi, axis=1), w, preferred_element_type=F32
        ) + jnp.dot(jnp.concatenate(lo, axis=1), w, preferred_element_type=F32)

    x = restricted([r0[lo_b + i] for i in range(n_b)], weights('wr0'))
    xs0[0] = x[: lv0.half]
    xs0[1] = x[lv0.half :]
    def pick(ref, par, start, n):
        return ref[par, pl.ds(start, n, stride=2)]

    def z_restricted(ref, even0, odd0, n):
        even = (
            0.5 * pick(ref, 0, even0, n)
            + 0.1875 * (pick(ref, 1, odd0, n) + pick(ref, 1, odd0 + 1, n))
            - 0.0625 * (pick(ref, 1, odd0 - 1, n) + pick(ref, 1, odd0 + 2, n))
        )
        odd = 0.5 * pick(ref, 0, even0 + 1, n) + 0.375 * (
            pick(ref, 1, odd0 + 1, n) + pick(ref, 1, odd0 + 2, n)
        )
        return even, odd

    even, odd = z_restricted(xs0, zh, zh - 1, half_c)
    lane_c = lax.broadcasted_iota(jnp.int32, (half_c, LANES), 1)
    packed = jnp.where(lane_c < LANES // 2, even, odd)
    blk[...] = packed

    def g_copy(n):
        st = x_steps[n]
        return remote(blk, line.at[st[4]], gsend.at[n], grecv.at[n], (st[0], iy, iz))

    def p_copy(n, m, jx):
        to, _, _, jy, zs = plane_steps[n]
        if zs is None:
            src, dst = pl.ds(0, half_c), pl.ds(zq, half_c)
        else:
            src, dst = pl.ds(zs[5], zq), pl.ds(zs[6], zq)
        from_ref = blk if m == 0 else line.at[jx]
        return remote(
            from_ref.at[src], land.at[jy, jx, dst], psend.at[n, m], precv.at[n, m], to
        )

    sources = [(None, own_x)] + [(st[3], st[5]) for st in x_steps]
    for n, st in enumerate(x_steps):
        when(st[1], lambda: g_copy(n).start())
    for m, (ok, jx) in enumerate(sources):

        def act():
            if m:
                g_copy(m - 1).wait_recv()
            for n, st in enumerate(plane_steps):
                when(st[1], lambda: p_copy(n, m, jx).start())
            land[own_y, jx, zq : zq + half_c] = packed if m == 0 else line[jx]

        when(ok, act)
    per = cx // lv1.group
    lane_h = lax.broadcasted_iota(jnp.int32, (lv1.half, LANES), 1) // gs

    def place_block(jx):
        blocks = [land[jy, jx] for jy in range(wy)]
        for s in range(per):
            t = jx * per + s
            for par in range(2):
                at = par * (LANES // 2) + s * gs
                val = None
                for jy in range(wy):
                    shift = (jy * gs - at) % LANES
                    v = pltpu.roll(blocks[jy], shift, 1) if shift else blocks[jy]
                    if val is None:
                        val = v if wy == wyp else jnp.where(lane_h == jy, v, 0.0)
                    else:
                        val = jnp.where(lane_h == jy, v, val)
                rows = slice(par * lv1.half, par * lv1.half + lv1.half)
                r1[t, rows] = val
                d = (wide(iv1[t, par], lv1.half) * zm1[par]) * val
                d1[t + 1, rows] = d
                acc1[t, rows] = d

    for m, (ok, jx) in enumerate(sources):

        def act():
            for n, st in enumerate(plane_steps):
                when(st[2], lambda: p_copy(n, m, jx).wait_recv())

        when(ok, act)
        place_block(jx)

    def use_step1(t, par, rows, av, edge):
        r = r1[t, rows] - av
        r1[t, rows] = r
        d = KEEP * d1[t + 1, rows] + masked(
            (RATIO * wide(iv1[t, par], n_rows(rows))) * r, edge
        )
        d1[t + 1, rows] = d
        acc1[t, rows] += d

    def use_down1(t, par, rows, av, edge):
        r1[t, rows] = masked((r1[t, rows] - av) * wide(mk1[t], n_rows(rows)), edge)

    n1 = lv1.tiles
    stage(lv1, d1, hh1, hl1, 0, n1)
    sweep(lv1, hh1, hl1, weights('wa1'), ss1, zm1, 0, n1, use_step1)
    stage(lv1, d1, hh1, hl1, 0, n1)
    sweep(lv1, hh1, hl1, weights('wa1'), ss1, zm1, 0, n1, use_down1)

    ratio = 2 * lv2.group // lv1.group
    r_lo = (-3) // lv1.group
    r_hi = (2 * lv2.group + 1) // lv1.group
    wr1 = weights('wr1')
    for t in range(lv2.tiles):
        a, e = max(0, ratio * t + r_lo), min(n1 - 1, ratio * t + r_hi)
        skip = (a - (ratio * t + r_lo)) * LANES
        x = restricted(
            [r1[i] for i in range(a, e + 1)], wr1[skip : skip + (e + 1 - a) * LANES]
        )
        xs1[0, 8 : 8 + lv1.half] = x[: lv1.half]
        xs1[1, 8 : 8 + lv1.half] = x[lv1.half :]
        for par, val in enumerate(z_restricted(xs1, 8, 7, lv2.half)):
            rows = slice(par * lv2.half, par * lv2.half + lv2.half)
            r2[t, rows] = val
            d2[t + 1, rows] = (wide(iv2[t, par], lv2.half) * zm2[par]) * val

    def use_last(t, par, rows, av, edge):
        r = r2[t, rows] - av
        step = masked((RATIO * wide(iv2[t, par], n_rows(rows))) * r, edge)
        lo = rows.start - par * lv2.half
        up2[t, par, lo : lo + n_rows(rows)] = (1.0 + KEEP) * d2[t + 1, rows] + step

    stage(lv2, d2, hh2, hl2, 0, lv2.tiles)
    sweep(lv2, hh2, hl2, weights('wa2'), ss2, zm2, 0, lv2.tiles, use_last)

    n2 = lv2.half
    wp1 = weights('wp1')
    for t in range(lv2.tiles):
        e2, o2, e3 = up2[t, 0, 0:n2], up2[t, 1, 0:n2], up2[t, 0, 1 : n2 + 1]
        zp1[t, pl.ds(0, n2, stride=2)] = e2
        zp1[t, pl.ds(1, n2, stride=2)] = o2
        zp1[t, pl.ds(lv1.half, n2, stride=2)] = 0.375 * e2 + 0.75 * o2 - 0.125 * e3
        zp1[t, pl.ds(lv1.half + 1, n2, stride=2)] = 0.75 * o2 + 0.375 * e3 - 0.125 * e2
        zh1[t], zl1[t] = split(zp1[t])
    for t in range(lv2.tiles):
        n_in = min(2, lv2.tiles - t)
        w = wp1[: n_in * LANES]
        e = jnp.dot(
            jnp.concatenate([zh1[t + i] for i in range(n_in)], axis=1), w,
            preferred_element_type=F32,
        ) + jnp.dot(
            jnp.concatenate([zl1[t + i] for i in range(n_in)], axis=1), w,
            preferred_element_type=F32,
        )
        for k in range(ratio):
            to = ratio * t + k
            if to < n1:
                for par in range(2):
                    rows = slice(par * lv1.half, par * lv1.half + lv1.half)
                    v = e[rows, LANES * k : LANES * k + LANES] * (
                        wide(mk1[to], lv1.half) * zm1[par]
                    )
                    d1[to + 1, rows] = v
                    acc1[to, rows] += v

    def use_up1(t, par, rows, av, edge):
        r = r1[t, rows] - av
        r1[t, rows] = r
        d1[t + 1, rows] = masked(wide(iv1[t, par], n_rows(rows)) * r, edge)

    def use_final1(t, par, rows, av, edge):
        r = r1[t, rows] - av
        c1[t + 2, rows] = (acc1[t, rows] + (1.0 + KEEP) * d1[t + 1, rows]) + masked(
            (RATIO * wide(iv1[t, par], n_rows(rows))) * r, edge
        )

    stage(lv1, d1, hh1, hl1, 0, n1)
    sweep(lv1, hh1, hl1, weights('wa1'), ss1, zm1, 0, n1, use_up1)
    stage(lv1, d1, hh1, hl1, 0, n1)
    sweep(lv1, hh1, hl1, weights('wa1'), ss1, zm1, 0, n1, use_final1)

    up = 2 * lv1.group // lv0.group
    tau_lo = (lo_b - own_lo) // up
    tau_hi = (lo_b + n_b - 1 - own_lo) // up
    n_tau = tau_hi + 2 - tau_lo
    jn = (lv0.half // 2 + 7) // 8 * 8
    lane_j = lax.broadcasted_iota(jnp.int32, (jn, LANES), 1) // gs
    bad = ((lane_j == 0) & (own_y == 0)) | ((lane_j == 2) & (own_y == wy - 1))
    turn = lax.rem(1 - own_y + wyp, wyp) * gs
    first = ZR // 2 - zh // 2
    wp0 = weights('wp0')
    for i in range(n_tau):
        at = own_x * per + (tau_lo + i + 2)

        def rows_of(par, start):
            v = pltpu.roll(c1[at, pl.ds(par * lv1.half + start, jn)], turn, 1)
            return jnp.where(bad, 0.0, v)

        e2, o2, e3 = rows_of(0, first), rows_of(1, first), rows_of(0, first + 1)
        zp0[i, pl.ds(0, jn, stride=2)] = e2
        zp0[i, pl.ds(1, jn, stride=2)] = o2
        zp0[i, pl.ds(lv0.half, jn, stride=2)] = 0.375 * e2 + 0.75 * o2 - 0.125 * e3
        zp0[i, pl.ds(lv0.half + 1, jn, stride=2)] = 0.75 * o2 + 0.375 * e3 - 0.125 * e2
        zh0[i], zl0[i] = split(zp0[i, 0 : lv0.rows])
    for i in range(n_tau - 1):
        e = jnp.dot(
            jnp.concatenate([zh0[i], zh0[i + 1]], axis=1), wp0,
            preferred_element_type=F32,
        ) + jnp.dot(
            jnp.concatenate([zl0[i], zl0[i + 1]], axis=1), wp0,
            preferred_element_type=F32,
        )
        for k in range(up):
            t = own_lo + up * (tau_lo + i) + k
            if lo_b <= t < lo_b + n_b:
                for par in range(2):
                    rows = slice(par * lv0.half, par * lv0.half + lv0.half)
                    v = e[rows, LANES * k : LANES * k + LANES] * (
                        wide(mk0[t], lv0.half) * zm0[par]
                    )
                    d0[t + 1, rows] = v
                    if own(t):
                        acc0[t - own_lo, rows] += v

    def use_up(t, par, rows, av, edge):
        r = r0[t, rows] - av
        r0[t, rows] = r
        d0[t + 1, rows] = masked(wide(iv0[t, par], n_rows(rows)) * r, edge)

    def use_final(t, par, rows, av, edge):
        r = r0[t, rows] - av
        acc0[t - own_lo, rows] += (1.0 + KEEP) * d0[t + 1, rows] + (
            RATIO * wide(iv0[t, par], n_rows(rows))
        ) * r

    lo_c, n_c = reach(2, 1)
    stage(lv0, d0, hh0, hl0, lo_c, n_c)
    sweep(lv0, hh0, hl0, weights('wa0'), ss0, zm0, lo_c, n_c, use_up)
    stage(lv0, d0, hh0, hl0, own_lo, own_n)
    sweep(lv0, hh0, hl0, weights('wa0'), ss0, zm0, own_lo, own_n, use_final)

    for i in range(own_n):
        for par in range(2):
            lo = par * lv0.half + zh
            tmp[pl.ds(par, hb, stride=2)] = acc0[i, lo : lo + hb]
        v = tmp[...].T.reshape(lv0.group, yh0, bz)
        out_ref[lv0.group * i : lv0.group * i + lv0.group] = v[:, H : H + by]

    for n, off in enumerate(xy_offs):
        for k in range(2):
            when(xy_step(off)[1], lambda: halo_copy(n, k).wait_send())
    for m in range(len(z_steps)):
        for n in range(len(spots)):
            when(strip_ok(n, m, 1), lambda: strip_copy(n, m).wait_send())
    for n, st in enumerate(x_steps):
        when(st[1], lambda: g_copy(n).wait_send())
    for m, (ok, jx) in enumerate(sources):

        def act():
            for n, st in enumerate(plane_steps):
                when(st[1], lambda: p_copy(n, m, jx).wait_send())

        when(ok, act)


def local(mesh_shape, u, b):
    nx, ny, nz = (mesh_shape[a] for a in ("gx", "gy", "gz"))
    bx, by, bz = u.shape
    cx, cy, cz = bx // 2, by // 2, bz // 2
    wx = nx if nx <= 2 * REACH + 1 else 2 * REACH + 1
    wy = ny if ny <= 2 * REACH + 1 else 2 * REACH + 1
    wyp = 4 if wy <= 4 else 8
    gs = LANES // wyp
    yh0 = by + 2 * H
    xg0 = LANES // yh0
    lv0 = Level(
        xg0, (bx + 2 * H) // xg0, yh0, (bz + 2 * H) // 2, lambda x, y: x * yh0 + y, H // 2
    )
    xg1 = gs // cy
    lv1 = Level(
        xg1, cx * wx // xg1, cy * wy, (cz + 2 * ZR) // 2,
        lambda x, y: (y // cy) * gs + x * cy + y % cy, ZR // 2,
    )
    y2 = cy * wy // 2
    yh2 = 16 if y2 <= 16 else 32
    xg2 = LANES // yh2
    lv2 = Level(
        xg2, -(-(cx * wx // 2) // xg2), y2, (cz + 2 * ZR) // 4, lambda x, y: x * yh2 + y,
        ZR // 4,
    )

    own_lo = H // xg0
    lo_b = (H - 4) // xg0
    n_b = (H + bx - 1 + 3) // xg0 - lo_b + 1
    px = []
    for x in range(cx):
        for s, w in restrict_taps(x):
            f = H + 2 * x + s
            px.append(((0, x), f // xg0 - lo_b, f % xg0, w))
    py = [(y, H + 2 * y + s, w) for y in range(cy) for s, w in restrict_taps(y)]
    once = plane_matrix(n_b, 1, px, py, lv0.at, lambda x, y: x * cy + y)
    m_r0 = once + np.roll(once, LANES // 2, axis=1)

    r_lo, r_hi = (-3) // xg1, (2 * xg2 + 1) // xg1
    px = []
    for x in range(xg2):
        for s, w in restrict_taps(x):
            f = 2 * x + s
            px.append(((0, x), f // xg1 - r_lo, f % xg1, w))
    py = [
        (y, 2 * y + s, w) for y in range(y2) for s, w in restrict_taps(y)
        if 0 <= 2 * y + s < cy * wy
    ]
    m_r1 = plane_matrix(r_hi - r_lo + 1, 1, px, py, lv1.at, lv2.at)

    ratio = 2 * xg2 // xg1
    px = []
    for f in range(2 * xg2):
        for c, w in prolong_taps(f):
            px.append(((f // xg1, f % xg1), c // xg2, c % xg2, w))
    py = [
        (f, c, w) for f in range(cy * wy) for c, w in prolong_taps(f) if 0 <= c < y2
    ]
    m_p1 = plane_matrix(2, ratio, px, py, lv2.at, lv1.at)

    up = 2 * xg1 // xg0
    px = []
    for f in range(2 * xg1):
        for c, w in prolong_taps(f):
            px.append(((f // xg0, f % xg0), c // xg1, c % xg1, w))
    py = [
        (f + H, c + cy, w) for f in range(-H, by + H) for c, w in prolong_taps(f)
        if -cy <= c < 2 * cy
    ]
    m_p0 = plane_matrix(2, up, px, py, lv1.at, lv0.at)

    parts, stack, row = {}, [], 0
    for name, m in (
        ("wa0", operator_matrix(lv0)), ("wa1", operator_matrix(lv1)),
        ("wa2", operator_matrix(lv2)), ("wr0", m_r0), ("wr1", m_r1), ("wp1", m_p1),
        ("wp0", m_p0),
    ):
        if m.shape[1] == LANES:
            m = np.pad(m, ((0, m.shape[0] % 2), (0, 0)))
            half = m.shape[0] // 2
            assert half % 16 == 0
            parts[name] = [(row, 0, half, LANES), (row, LANES, half, LANES)]
            stack.append(np.concatenate([m[:half], m[half:]], axis=1))
            row += half
        else:
            parts[name] = []
            for c in range(0, m.shape[1], 256):
                parts[name].append((row, 0, m.shape[0], min(256, m.shape[1] - c)))
                piece = m[:, c : c + 256]
                stack.append(np.pad(piece, ((0, 0), (0, 256 - piece.shape[1]))))
                row += m.shape[0]
    consts = to_bf16(np.concatenate(stack, axis=0))
    vm = lambda *s: pltpu.VMEM(s, F32)
    bm = lambda *s: pltpu.VMEM(s, BF16)
    dma = lambda *s: pltpu.SemaphoreType.DMA(s)

    def per_level(lv):
        t, n = lv.tiles, lv.rows
        return (
            vm(t + 2, n, LANES), vm(t, n, LANES), vm(t, n, LANES),
            bm(t + 2, n, LANES), bm(t + 2, n, LANES), vm(4, 4, lv.half + 16, LANES),
            vm(t, 2, 8, LANES), vm(t, 8, LANES), vm(2, lv.half, LANES),
        )

    p0, p1, p2 = per_level(lv0), per_level(lv1), per_level(lv2)
    tau_lo = (lo_b - own_lo) // up
    n_tau = (lo_b + n_b - 1 - own_lo) // up + 2 - tau_lo
    jn = (lv0.half // 2 + 7) // 8 * 8
    geo = (nx, ny, nz, bx, by, bz, wx, wy, wyp)
    near, side = (3 if nx > 1 else 1), (3 if ny > 1 else 1)
    n_z = 0 if nz == 1 else 1 if nz == 2 else 2
    n_x = max(1, nx - 1 if wx == nx else 2 * REACH)
    n_y = ny - 1 if wy == ny else 2 * REACH
    n_p = max(1, (n_y + 1) * (n_z + 1) - 1)
    n_xy, n_s = max(1, near * side - 1), near * side
    return pl.pallas_call(
        functools.partial(kernel, geo, lv0, lv1, lv2, parts),
        out_shape=pltpu.VMEM(u.shape, F32),
        in_specs=[pl.BlockSpec(memory_space=pl.ANY)] * 3,
        out_specs=pl.BlockSpec(memory_space=pltpu.VMEM),
        scratch_shapes=[
            bm(*consts.shape), vm(bx, by, bz), vm(bx, by, bz),
            vm(bx + 2 * H, yh0, bz), vm(bx + 2 * H, yh0, bz), vm(bz, LANES),
            vm(xg0, yh0, bz), vm(2, 3, 2, bx // xg0, H, LANES),
            vm(2, 3, 2, lv0.tiles, H, LANES),
            *p0, *p1, vm(lv1.tiles + 4, lv1.rows, LANES), p2[0], p2[1], *p2[3:],
            vm(2, lv0.half, LANES), vm(2, lv1.half + 16, LANES), vm(cz // 2, LANES),
            vm(wx, cz // 2, LANES), vm(wy, wx, lv1.half, LANES),
            vm(lv2.tiles, 2, lv2.half + 8, LANES), vm(lv2.tiles, lv1.rows, LANES),
            vm(n_tau, lv0.half + 2 * jn, LANES),
            bm(lv2.tiles, lv1.rows, LANES), bm(lv2.tiles, lv1.rows, LANES),
            bm(n_tau, lv0.rows, LANES), bm(n_tau, lv0.rows, LANES),
            dma(3), dma(n_xy, 2), dma(n_xy, 2), dma(n_s, max(1, n_z)), dma(n_s, max(1, n_z)),
            dma(n_x), dma(n_x), dma(n_p, n_x + 1), dma(n_p, n_x + 1),
        ],
        compiler_params=pltpu.CompilerParams(
            collective_id=0, has_side_effects=True, vmem_limit_bytes=60 * 1024 * 1024
        ),
    )(u, b, consts)


def solution(mesh):
    placed = P("gx", "gy", "gz")
    return jax.shard_map(
        functools.partial(local, dict(mesh.shape)), mesh=mesh,
        in_specs=(placed, placed), out_specs=placed, check_vma=False,
    )
```

```python
import functools

import jax
import jax.numpy as jnp
import numpy as np
from jax import lax
from jax.experimental import pallas as pl
from jax.experimental.pallas import tpu as pltpu
from jax.sharding import PartitionSpec as P

F32 = jnp.float32
BF16 = jnp.bfloat16
MESH = pl.DeviceIdType.MESH
H = 8
ZR = 32
REACH = 3
LANES = 128

RHO0 = 1.0 / 1.2
RHO1 = 1.0 / (2.4 - RHO0)
FIRST = 1.0 / 1.32
KEEP = RHO1 * RHO0
STEP = 2.0 * RHO1 / 1.1
RATIO = STEP / FIRST
UNIT = 2700.0


def restrict_taps(g):
    if g % 2 == 0:
        return ((-3, -0.125), (-1, 0.375), (0, 1.0), (1, 0.375), (3, -0.125))
    return ((-1, 0.75), (0, 1.0), (1, 0.75))


def prolong_taps(f):
    if f % 2 == 0:
        return ((f // 2, 1.0),)
    q = f // 4
    if f % 4 == 1:
        return ((2 * q, 0.375), (2 * q + 1, 0.75), (2 * q + 2, -0.125))
    return ((2 * q, -0.125), (2 * q + 1, 0.75), (2 * q + 2, 0.375))


def stiff_taps(i):
    if i % 2 == 0:
        return {-2: 1, -1: -8, 0: 14, 1: -8, 2: 1}
    return {-1: -8, 0: 16, 1: -8}


def mass_taps(i):
    if i % 2 == 0:
        return {-2: -1, -1: 2, 0: 8, 1: 2, 2: -1}
    return {-1: 2, 0: 16, 1: 2}


class Level:
    def __init__(self, group, tiles, height, half, at, parts, pad):
        self.group, self.tiles, self.height, self.half, self.at = group, tiles, height, half, at
        self.parts, self.pad = parts, pad
        self.rows = 2 * half
        self.paired = group >= 4


def operator_matrix(lv):
    k = 256 if lv.paired else 384
    m = np.zeros((k, 256), np.float64)
    for x in range(lv.group):
        for y in range(lv.height):
            for ox, mx in mass_taps(x).items():
                kx = stiff_taps(x)[ox]
                p = x + ox
                if lv.paired:
                    block = (p + lv.group // 2) // lv.group
                else:
                    block = p // lv.group + 1
                for oy, my in mass_taps(y).items():
                    ky = stiff_taps(y)[oy]
                    if not 0 <= y + oy < lv.height:
                        continue
                    row = block * LANES + lv.at(p % lv.group, y + oy)
                    both, mixed = mx * my, kx * my + mx * ky
                    m[row, lv.at(x, y)] = -8 * both + 2 * mixed
                    m[row, LANES + lv.at(x, y)] = both - mixed
    return m


def plane_matrix(n_in, n_out, pairs_x, pairs_y, at_in, at_out):
    m = np.zeros((n_in * LANES, n_out * LANES), np.float64)
    for (to, xo), ti, xi, wx in pairs_x:
        for yo, yi, wy in pairs_y:
            m[ti * LANES + at_in(xi, yi), to * LANES + at_out(xo, yo)] += wx * wy
    return m


def to_bf16(m):
    out = jnp.asarray(m, BF16)
    assert np.array_equal(np.asarray(m, jnp.bfloat16).astype(np.float64), m)
    return out


def split(v):
    hi = v.astype(BF16)
    return hi, (v - hi.astype(F32)).astype(BF16)


def loop(count, body, most=9):
    if count <= most:
        for i in range(count):
            body(i)
    else:

        def step(i, carry):
            body(i)
            return carry

        lax.fori_loop(0, count, step, 0)


def kernel(
    geo, lv0, lv1, lv2, parts, u_hbm, b_hbm, w_hbm, out_ref, *refs,
):
    (wall, u_ref, b_ref, ue, be, tmp, pad, strip_out, strip_in,
     d0, r0, acc0, hh0, hl0, ss0, iv0, mk0, zm0,
     d1, r1, acc1, hh1, hl1, ss1, iv1, mk1, zm1, c1,
     d2, r2, hh2, hl2, ss2, iv2, mk2, zm2,
     xs0, xs1, blk, line, land, up2, zp1, zp0, zh1, zl1, zh0, zl0,
     wsem, xysend, xyrecv, zsend, zrecv, gsend, grecv, psend, precv) = refs
    nx, ny, nz, bx, by, bz, wx, wy, wyp = geo
    ix, iy, iz = lax.axis_index("gx"), lax.axis_index("gy"), lax.axis_index("gz")
    place, counts = (ix, iy, iz), (nx, ny, nz)
    full_x, full_y = wx == nx, wy == ny
    cx, cy, cz = bx // 2, by // 2, bz // 2
    start_x = 0 if full_x else ix - REACH
    start_y = 0 if full_y else iy - REACH
    own_x = ix if full_x else REACH
    own_y = iy if full_y else REACH

    def both(*oks):
        ok = None
        for o in oks:
            if o is not None:
                ok = o if ok is None else ok & o
        return ok

    def when(ok, act):
        if ok is None:
            act()
        else:
            pl.when(ok)(act)

    def unless(ok, act):
        if ok is not None:
            pl.when(jnp.logical_not(ok))(act)

    def inside(axis, p):
        return (p >= 0) & (p < counts[axis])

    def shifted(axis, off):
        if off == 0:
            return (place[axis], None, place[axis], None)
        to, source = place[axis] + off, place[axis] - off
        return (to, inside(axis, to), source, inside(axis, source))

    def line_steps(axis, full):
        p, n = place[axis], counts[axis]
        if full:
            steps = []
            for k in sorted(range(1, n), key=lambda k: -k):
                to, source = lax.rem(p + k, n), lax.rem(p + n - k, n)
                steps.append((to, None, source, None, p, source))
            return steps
        offs = sorted((o for o in range(-REACH, REACH + 1) if o), key=abs)
        return [shifted(axis, o) + (REACH - o, REACH - o) for o in offs]

    zq, half_c = ZR // 2, cz // 2
    x_steps = line_steps(0, full_x)
    y_steps = line_steps(1, full_y)
    if nz == 2:
        z_steps = [
            (1 - iz, None, 1 - iz, None, 1 - iz,
             pl.multiple_of((1 - iz) * (half_c - zq), 8),
             pl.multiple_of(iz * (zq + half_c), 8))
        ]
    elif nz > 2:
        z_steps = [
            shifted(2, 1) + (1, half_c - zq, 0), shifted(2, -1) + (0, 0, zq + half_c)
        ]
    else:
        z_steps = []
    plane_steps = [
        ((ix, ys[0], iz), ys[1], ys[3], ys[4], None) for ys in y_steps
    ] + [
        ((ix, iy, zs[0]), zs[1], zs[3], own_y, zs) for zs in z_steps
    ] + [
        ((ix, ys[0], zs[0]), both(ys[1], zs[1]), both(ys[3], zs[3]), ys[4], zs)
        for zs in z_steps for ys in y_steps
    ]
    near = [0] + ([-1, 1] if nx > 1 else [])
    side = [0] + ([-1, 1] if ny > 1 else [])
    xy_offs = [(a, c) for a in near for c in side if a or c]

    def xy_step(off):
        xs, ys = shifted(0, off[0]), shifted(1, off[1])
        return (xs[0], ys[0]), both(xs[1], ys[1]), both(xs[3], ys[3])

    greet = [((st[0], iy, iz), st[1], st[3]) for st in x_steps]
    greet += [(st[0], st[1], st[2]) for st in plane_steps]
    for off in xy_offs:
        if off[0]:
            to, ok, ok_from = xy_step(off)
            if off[1]:
                greet.append((to + (iz,), ok, ok_from))
            for zs in z_steps:
                greet.append((to + (zs[0],), both(ok, zs[1]), both(ok_from, zs[3])))

    barrier = pltpu.get_barrier_semaphore()
    total = 0
    for to, ok, ok_from in greet:
        total = total + (1 if ok_from is None else ok_from.astype(jnp.int32))

        def signal():
            pl.semaphore_signal(barrier, inc=1, device_id=to, device_id_type=MESH)

        when(ok, signal)

    load_u = pltpu.make_async_copy(u_hbm, u_ref, wsem.at[0])
    load_b = pltpu.make_async_copy(b_hbm, b_ref, wsem.at[1])
    load_w = pltpu.make_async_copy(w_hbm, wall, wsem.at[2])
    load_u.start()
    load_b.start()
    load_w.start()

    def remote(src, dst, ss, rs, to):
        return pltpu.make_async_remote_copy(
            src_ref=src, dst_ref=dst, send_sem=ss, recv_sem=rs,
            device_id=to, device_id_type=MESH,
        )

    def weights(name):
        blocks = []
        for row, lane, rows, lanes in parts[name]:
            blocks.append(wall[row : row + rows, lane : lane + lanes])
        if parts[name][0][3] == LANES:
            return jnp.concatenate(blocks, axis=0)
        return jnp.concatenate(blocks, axis=1)

    def cut(off, size, low, high):
        if off == 0:
            return slice(0, size), slice(H, H + size)
        if off > 0:
            return slice(size - low, size), slice(H - low, H)
        return slice(0, high), slice(H + size, H + size + high)

    fields = ((u_ref, ue, H, H - 1), (b_ref, be, H - 2, H - 3))

    def halo_cut(off, k):
        ref, ext, low, high = fields[k]
        sx, tx = cut(off[0], bx, low, high)
        sy, ty = cut(off[1], by, H, H)
        return ref, ext, sx, tx, sy, ty

    def zero(ref, *at):
        ref[at] = jnp.zeros_like(ref[at])

    def halo_copy(n, k):
        ref, ext, sx, tx, sy, ty = halo_cut(xy_offs[n], k)
        to = xy_step(xy_offs[n])[0] + (iz,)
        return remote(ref.at[sx, sy], ext.at[tx, ty], xysend.at[n, k], xyrecv.at[n, k], to)

    yh0 = by + 2 * H
    zh, hb = H // 2, bz // 2
    own_lo, own_n = H // lv0.group, bx // lv0.group
    edge_n = H // lv0.group
    spots = [(a, c) for a in near for c in side]

    def variant(c):
        return 0 if c == 0 else (1 if c > 0 else 2)

    def strip_cut(a):
        if a == 0:
            return slice(0, own_n), slice(own_lo, own_lo + own_n)
        if a > 0:
            return slice(own_n - edge_n, own_n), slice(0, edge_n)
        return slice(0, edge_n), slice(own_lo + own_n, own_lo + own_n + edge_n)

    def strip_copy(n, m):
        a, c = spots[n]
        zs = z_steps[m]
        src, dst = strip_cut(a)
        v, k = variant(c), zs[4]
        to = (shifted(0, a)[0], shifted(1, c)[0], zs[0])
        return remote(
            strip_out.at[k, v, :, src], strip_in.at[k, v, :, dst],
            zsend.at[n, m], zrecv.at[n, m], to,
        )

    def strip_ok(n, m, at):
        a, c = spots[n]
        return both(shifted(0, a)[at], shifted(1, c)[at], z_steps[m][at])

    zero(pad, slice(None), slice(0, H))
    zero(pad, slice(None), slice(H + by, yh0))
    lane_y = lax.broadcasted_iota(jnp.int32, (2 * zh, LANES), 1) % yh0
    load_u.wait()
    load_b.wait()
    for k, ref in enumerate((u_ref, b_ref)):
        for t in range(own_n):
            pad[:, H : H + by] = ref[lv0.group * t : lv0.group * t + lv0.group]
            tmp[...] = pad[...].reshape(LANES, bz).T
            for s, start in ((0, 0), (1, bz - H)):
                v = jnp.concatenate(
                    [tmp[pl.ds(start + par, zh, stride=2)] for par in range(2)], axis=0
                )
                strip_out[s, 0, k, t] = v
                if ny > 1:
                    strip_out[s, 1, k, t] = jnp.where(
                        lane_y < H, pltpu.roll(v, LANES - by, 1), 0.0
                    )
                    strip_out[s, 2, k, t] = jnp.where(
                        lane_y >= H + by, pltpu.roll(v, by, 1), 0.0
                    )

    pl.semaphore_wait(barrier, total)
    for m in range(len(z_steps)):
        for n in sorted(range(len(spots)), key=lambda n: -abs(spots[n][0]) - abs(spots[n][1])):
            when(strip_ok(n, m, 1), lambda: strip_copy(n, m).start())
    far_first = sorted(range(len(xy_offs)), key=lambda n: -abs(xy_offs[n][0] * xy_offs[n][1]))
    for n in far_first:
        when(xy_step(xy_offs[n])[1], lambda: halo_copy(n, 0).start())
    for n in far_first:
        when(xy_step(xy_offs[n])[1], lambda: halo_copy(n, 1).start())

    ue[H : H + bx, H : H + by] = u_ref[...]
    be[H : H + bx, H : H + by] = b_ref[...]
    for _, ext, low, high in fields:
        for at in (slice(0, H - low), slice(H + bx + high, 2 * H + bx)):
            if at.stop > at.start:
                zero(ext, at)
    for off in [(a, c) for a in (-1, 0, 1) for c in (-1, 0, 1) if a or c]:

        def clear():
            for k in range(2):
                _, ext, _, tx, _, ty = halo_cut(off, k)
                zero(ext, tx, ty)

        if off in xy_offs:
            unless(xy_step(off)[2], clear)
        else:
            clear()
    for s, rows in ((0, slice(zq + half_c, 2 * zq + half_c)), (1, slice(0, zq))):
        z_ok = inside(2, iz + (1 - 2 * s)) if nz > 1 else None
        for a in (-1, 0, 1):
            for c in (-1, 0, 1):

                def clear():
                    zero(strip_in, s, variant(c), slice(None), strip_cut(a)[1])

                if (a, c) in spots and nz > 1:
                    unless(both(shifted(0, a)[3], shifted(1, c)[3], z_ok), clear)
                else:
                    clear()

        def clear():
            zero(land, slice(None), slice(None), rows)

        if nz > 1:
            unless(z_ok, clear)
        else:
            clear()
    for st in x_steps:
        unless(st[3], lambda: zero(land, slice(None), st[5]))
    for st in y_steps:
        unless(st[3], lambda: zero(land, st[5]))

    def set_up(lv, level, iv, mk, zm, d, ss, x_first, y_first, z_first, x_at, y_at):
        lane = lax.broadcasted_iota(jnp.int32, (8, LANES), 1)
        row = lax.broadcasted_iota(jnp.int32, (lv.half, LANES), 0)
        xx, yy = x_at(lane), y_at(lane)
        x_even, y_even = xx % 2 == 0, yy % 2 == 0
        n_x, n_y, n_z = (nx * bx) >> level, (ny * by) >> level, (nz * bz) >> level
        gy = y_first + yy
        y_ok = (gy >= 0) & (gy < n_y) & (yy < lv.height)
        mass = lambda e: jnp.where(e, 8.0, 16.0) / 30.0
        stiff = lambda e: jnp.where(e, 14.0, 16.0) / 3.0
        my, ky, mx, kx = mass(y_even), stiff(y_even), mass(x_even), stiff(x_even)
        inv = []
        for kz, mz in ((14.0 / 3.0, 8.0 / 30.0), (16.0 / 3.0, 16.0 / 30.0)):
            inv.append((FIRST / UNIT) / (kx * my * mz + mx * ky * mz + mx * my * kz))

        def one(i):
            gx = x_first + (i - lv.pad) * lv.group + xx
            ok = jnp.where(y_ok & (gx >= 0) & (gx < n_x), 1.0, 0.0).astype(F32)
            mk[i] = ok
            iv[i, 0] = inv[0] * ok
            iv[i, 1] = inv[1] * ok

        loop(lv.tiles + 2 * lv.pad, one, 16)
        for par in range(2):
            gz = z_first + 2 * row + par
            zm[par] = jnp.where((gz >= 0) & (gz < n_z), 1.0, 0.0).astype(F32)
        zero(d, slice(0, lv.pad))
        zero(d, slice(lv.tiles + lv.pad, lv.tiles + 2 * lv.pad))
        ss[:, :, 0:8] = jnp.zeros_like(ss[:, :, 0:8])
        ss[:, :, 8 + lv.half :] = jnp.zeros_like(ss[:, :, 8 + lv.half :])

    gs = LANES // wyp
    set_up(
        lv0, 0, iv0, mk0, zm0, d0, ss0, ix * bx - H, iy * by - H, iz * bz - H,
        lambda n: n // yh0, lambda n: n % yh0,
    )
    set_up(
        lv1, 1, iv1, mk1, zm1, d1, ss1, start_x * cx, start_y * cy, iz * cz - ZR,
        lambda n: (n % gs) // cy, lambda n: (n // gs) * cy + n % cy,
    )
    yh2 = LANES // lv2.group
    set_up(
        lv2, 2, iv2, mk2, zm2, d2, ss2, start_x * (cx // 2), start_y * (cy // 2),
        iz * (cz // 2) - ZR // 2, lambda n: n // yh2, lambda n: n % yh2,
    )
    for ref in (r1, acc1):
        zero(ref, slice(0, lv1.pad))
        zero(ref, slice(lv1.tiles + lv1.pad, lv1.tiles + 2 * lv1.pad))
    xs1[:, 0:8] = jnp.zeros_like(xs1[:, 0:8])
    xs1[:, 8 + lv1.half :] = jnp.zeros_like(xs1[:, 8 + lv1.half :])
    up2[...] = jnp.zeros_like(up2)

    def turn_field(k):
        ext = (ue, be)[k]
        for n, off in enumerate(xy_offs):
            when(xy_step(off)[2], lambda: halo_copy(n, k).wait_recv())
        for t in range(lv0.tiles):
            tmp[...] = ext[lv0.group * t : lv0.group * t + lv0.group].reshape(LANES, bz).T
            for par in range(2):
                val = tmp[pl.ds(par, hb, stride=2)]
                lo = par * lv0.half + zh
                if k == 0:
                    d0[t + 1, lo : lo + hb] = val
                else:
                    r0[t, lo : lo + hb] = UNIT * val - r0[t, lo : lo + hb]

    def fill_strips(k):
        for t in range(lv0.tiles):
            for s in range(2):
                v = (strip_in[s, 0, k, t] + strip_in[s, 1, k, t]) + strip_in[s, 2, k, t]
                for par in range(2):
                    lo = par * lv0.half + (0 if s else zh + hb)
                    rows, part = slice(lo, lo + zh), v[par * zh : par * zh + zh]
                    if k == 0:
                        d0[t + 1, rows] = part
                    else:
                        r0[t, rows] = UNIT * part - r0[t, rows]

    turn_field(0)
    for m in range(len(z_steps)):
        for n in range(len(spots)):
            when(strip_ok(n, m, 3), lambda: strip_copy(n, m).wait_recv())
    fill_strips(0)

    def stage(lv, d, hh, hl, lo, count):
        step = 48 if lv.rows % 48 == 0 else min(lv.rows, 64)
        lane = lax.broadcasted_iota(jnp.int32, (step, LANES), 1)
        if lv is lv1:
            plane = (lane % gs) // cy
        else:
            plane = lane // (LANES // lv.group)
        low = plane < lv.group // 2

        def one(i):
            t = lo + i
            for s in range(0, lv.rows, step):
                rows = slice(s, s + step)
                if lv.paired:
                    v = jnp.where(low, d[t + lv.pad, rows], d[t + lv.pad - 1, rows])
                else:
                    v = d[t + lv.pad - 1, rows]
                hh[t + lv.pad, rows], hl[t + lv.pad, rows] = split(v)

        loop(count + (1 if lv.paired else 2), one)

    def sweep(lv, hh, hl, w, ss, zm, lo, count, use, r_lo=0, r_hi=None):
        r_hi = lv.half if r_hi is None else r_hi
        chunk = next(c for c in (32, 24, 28, 8) if (r_hi - r_lo) % c == 0)
        n_cat = 2 if lv.paired else 3
        size = 2 if count % 2 == 0 else 1

        def group(i):
            t0 = lo + size * i

            def lhs(h):
                return jnp.concatenate(
                    [h[pl.ds(t0 + j + lv.pad, size)].reshape(size * lv.rows, LANES) for j in range(n_cat)],
                    axis=1,
                )

            s = jnp.dot(lhs(hh), w, preferred_element_type=F32) + jnp.dot(
                lhs(hl), w, preferred_element_type=F32
            )
            for k in range(size):
                slot = (i % 2) * 2 + k if isinstance(i, int) else k
                for par in range(2):
                    at = k * lv.rows + par * lv.half
                    for c in range(2):
                        ss[slot, 2 * c + par, 8 : 8 + lv.half] = s[
                            at : at + lv.half, LANES * c : LANES * c + LANES
                        ]
                t = t0 + k
                for at in range(r_lo, r_hi, chunk):

                    def rows_of(n, shift=0):
                        return ss[slot, n, pl.ds(8 + at + shift, chunk)]

                    even = (
                        (-11.0 / 3.0) * rows_of(0) + (-46.0 / 3.0) * rows_of(2)
                    ) + ((rows_of(1) + rows_of(1, -1)) + (rows_of(2, -1) + rows_of(2, 1)))
                    odd = ((-16.0 / 3.0) * rows_of(1) + (-80.0 / 3.0) * rows_of(3)) + (
                        rows_of(0) + rows_of(0, 1)
                    )
                    for par, val in enumerate((even, odd)):
                        edge = None
                        if at < lv.parts or at + chunk > lv.half - lv.parts:
                            edge = zm[par, at : at + chunk]
                        use(t, par, slice(par * lv.half + at, par * lv.half + at + chunk), val, edge)

        loop(count // size, group, 4)

    def wide(v, n):
        return jnp.broadcast_to(v[0:1], (n, LANES))

    def masked(v, edge):
        return v if edge is None else v * edge

    def n_rows(rows):
        return rows.stop - rows.start

    def own(t):
        return own_lo <= t < own_lo + own_n

    def reach(below, above):
        lo = (H - below) // lv0.group
        hi = (H + bx - 1 + above) // lv0.group
        return lo, hi - lo + 1

    def use_product(t, par, rows, av, edge):
        r0[t, rows] = av

    def first_step(t):
        size = 24 if lv0.half % 24 == 0 else 8
        for par in range(2):
            for at in range(0, lv0.half, size):
                rows = slice(par * lv0.half + at, par * lv0.half + at + size)
                d = wide(iv0[t + 1, par], size) * r0[t, rows] * zm0[par, at : at + size]
                if own(t):
                    acc0[t - own_lo, rows] = d0[t + 1, rows] + d
                d0[t + 1, rows] = d

    def use_step(t, par, rows, av, edge):
        r = r0[t, rows] - av
        r0[t, rows] = r
        d = KEEP * d0[t + 1, rows] + masked(
            (RATIO * wide(iv0[t + 1, par], n_rows(rows))) * r, edge
        )
        if own(t):
            acc0[t - own_lo, rows] += d
        d0[t + 1, rows] = d

    def use_down(t, par, rows, av, edge):
        r0[t, rows] = masked((r0[t, rows] - av) * wide(mk0[t + 1], n_rows(rows)), edge)

    lo_a, n_a = reach(6, 5)
    lo_b, n_b = reach(4, 3)
    load_w.wait()
    stage(lv0, d0, hh0, hl0, lo_a, n_a)
    sweep(lv0, hh0, hl0, weights('wa0'), ss0, zm0, lo_a, n_a, use_product)
    turn_field(1)
    fill_strips(1)
    for t in range(lo_a, lo_a + n_a):
        first_step(t)
    stage(lv0, d0, hh0, hl0, lo_b, n_b)
    sweep(lv0, hh0, hl0, weights('wa0'), ss0, zm0, lo_b, n_b, use_step)
    stage(lv0, d0, hh0, hl0, lo_b, n_b)
    sweep(lv0, hh0, hl0, weights('wa0'), ss0, zm0, lo_b, n_b, use_down)

    def restricted(parts, w):
        hi, lo = zip(*[split(p) for p in parts])
        return jnp.dot(
            jnp.concatenate(hi, axis=1), w, preferred_element_type=F32
        ) + jnp.dot(jnp.concatenate(lo, axis=1), w, preferred_element_type=F32)

    x = restricted([r0[lo_b + i] for i in range(n_b)], weights('wr0'))
    xs0[0] = x[: lv0.half]
    xs0[1] = x[lv0.half :]
    def pick(ref, par, start, n):
        return ref[par, pl.ds(start, n, stride=2)]

    def z_restricted(ref, even0, odd0, n):
        even = (
            0.5 * pick(ref, 0, even0, n)
            + 0.1875 * (pick(ref, 1, odd0, n) + pick(ref, 1, odd0 + 1, n))
            - 0.0625 * (pick(ref, 1, odd0 - 1, n) + pick(ref, 1, odd0 + 2, n))
        )
        odd = 0.5 * pick(ref, 0, even0 + 1, n) + 0.375 * (
            pick(ref, 1, odd0 + 1, n) + pick(ref, 1, odd0 + 2, n)
        )
        return even, odd

    even, odd = z_restricted(xs0, zh, zh - 1, half_c)
    lane_c = lax.broadcasted_iota(jnp.int32, (half_c, LANES), 1)
    packed = jnp.where(lane_c < LANES // 2, even, odd)
    blk[...] = packed

    def g_copy(n):
        st = x_steps[n]
        return remote(blk, line.at[st[4]], gsend.at[n], grecv.at[n], (st[0], iy, iz))

    def p_copy(n, m, jx):
        to, _, _, jy, zs = plane_steps[n]
        if zs is None:
            src, dst = pl.ds(0, half_c), pl.ds(zq, half_c)
        else:
            src, dst = pl.ds(zs[5], zq), pl.ds(zs[6], zq)
        from_ref = blk if m == 0 else line.at[jx]
        return remote(
            from_ref.at[src], land.at[jy, jx, dst], psend.at[n, m], precv.at[n, m], to
        )

    sources = [(None, own_x)] + [(st[3], st[5]) for st in x_steps]
    for n in reversed(range(len(x_steps))):
        when(x_steps[n][1], lambda: g_copy(n).start())
    for m, (ok, jx) in enumerate(sources):

        def act():
            if m:
                g_copy(m - 1).wait_recv()
            for n in reversed(range(len(plane_steps))):
                when(plane_steps[n][1], lambda: p_copy(n, m, jx).start())
            land[own_y, jx, zq : zq + half_c] = packed if m == 0 else line[jx]

        when(ok, act)
    per = cx // lv1.group
    lane_h = lax.broadcasted_iota(jnp.int32, (lv1.half, LANES), 1) // gs

    def place_block(jx):
        blocks = [land[jy, jx] for jy in range(wy)]
        for s in range(per):
            t = jx * per + s
            for par in range(2):
                at = par * (LANES // 2) + s * gs
                val = None
                for jy in range(wy):
                    shift = (jy * gs - at) % LANES
                    v = pltpu.roll(blocks[jy], shift, 1) if shift else blocks[jy]
                    if val is None:
                        val = v if wy == wyp else jnp.where(lane_h == jy, v, 0.0)
                    else:
                        val = jnp.where(lane_h == jy, v, val)
                rows = slice(par * lv1.half, par * lv1.half + lv1.half)
                r1[t + lv1.pad, rows] = val
                d = (wide(iv1[t + lv1.pad, par], lv1.half) * zm1[par]) * val
                d1[t + lv1.pad, rows] = d
                acc1[t + lv1.pad, rows] = d

    for m, (ok, jx) in enumerate(sources):

        def act():
            for n, st in enumerate(plane_steps):
                when(st[2], lambda: p_copy(n, m, jx).wait_recv())

        when(ok, act)
        place_block(jx)

    def use_step1(t, par, rows, av, edge):
        r = r1[t + lv1.pad, rows] - av
        r1[t + lv1.pad, rows] = r
        d = KEEP * d1[t + lv1.pad, rows] + masked(
            (RATIO * wide(iv1[t + lv1.pad, par], n_rows(rows))) * r, edge
        )
        d1[t + lv1.pad, rows] = d
        acc1[t + lv1.pad, rows] += d

    def use_down1(t, par, rows, av, edge):
        r1[t + lv1.pad, rows] = masked((r1[t + lv1.pad, rows] - av) * wide(mk1[t + lv1.pad], n_rows(rows)), edge)

    n1 = lv1.tiles
    stage(lv1, d1, hh1, hl1, 0, n1)
    z_cut = ZR // 4
    sweep(lv1, hh1, hl1, weights('wa1'), ss1, zm1, 0, n1, use_step1, z_cut)
    stage(lv1, d1, hh1, hl1, 0, n1)
    sweep(
        lv1, hh1, hl1, weights('wa1'), ss1, zm1, 0, n1, use_down1, z_cut, lv1.half - z_cut
    )

    ratio = 2 * lv2.group // lv1.group
    r_lo = (-3) // lv1.group
    r_hi = (2 * lv2.group + 1) // lv1.group
    wr1 = weights('wr1')
    for t in range(lv2.tiles):
        a, e = max(0, ratio * t + r_lo), min(n1 - 1, ratio * t + r_hi)
        skip = (a - (ratio * t + r_lo)) * LANES
        x = restricted(
            [r1[i + lv1.pad] for i in range(a, e + 1)], wr1[skip : skip + (e + 1 - a) * LANES]
        )
        xs1[0, 8 : 8 + lv1.half] = x[: lv1.half]
        xs1[1, 8 : 8 + lv1.half] = x[lv1.half :]
        for par, val in enumerate(z_restricted(xs1, 8, 7, lv2.half)):
            rows = slice(par * lv2.half, par * lv2.half + lv2.half)
            r2[t, rows] = val
            d2[t + 1, rows] = (wide(iv2[t + 1, par], lv2.half) * zm2[par]) * val

    def use_last(t, par, rows, av, edge):
        r = r2[t, rows] - av
        step = masked((RATIO * wide(iv2[t + 1, par], n_rows(rows))) * r, edge)
        lo = rows.start - par * lv2.half
        up2[t, par, lo : lo + n_rows(rows)] = (1.0 + KEEP) * d2[t + 1, rows] + step

    stage(lv2, d2, hh2, hl2, 0, lv2.tiles)
    sweep(lv2, hh2, hl2, weights('wa2'), ss2, zm2, 0, lv2.tiles, use_last)

    n2 = lv2.half
    wp1 = weights('wp1')
    for t in range(lv2.tiles):
        e2, o2, e3 = up2[t, 0, 0:n2], up2[t, 1, 0:n2], up2[t, 0, 1 : n2 + 1]
        zp1[t, pl.ds(0, n2, stride=2)] = e2
        zp1[t, pl.ds(1, n2, stride=2)] = o2
        zp1[t, pl.ds(lv1.half, n2, stride=2)] = 0.375 * e2 + 0.75 * o2 - 0.125 * e3
        zp1[t, pl.ds(lv1.half + 1, n2, stride=2)] = 0.75 * o2 + 0.375 * e3 - 0.125 * e2
        zh1[t], zl1[t] = split(zp1[t])
    for t in range(lv2.tiles):
        n_in = min(2, lv2.tiles - t)
        w = wp1[: n_in * LANES]
        e = jnp.dot(
            jnp.concatenate([zh1[t + i] for i in range(n_in)], axis=1), w,
            preferred_element_type=F32,
        ) + jnp.dot(
            jnp.concatenate([zl1[t + i] for i in range(n_in)], axis=1), w,
            preferred_element_type=F32,
        )
        for k in range(ratio):
            to = ratio * t + k
            if to < n1:
                for par in range(2):
                    rows = slice(par * lv1.half, par * lv1.half + lv1.half)
                    v = e[rows, LANES * k : LANES * k + LANES] * (
                        wide(mk1[to + lv1.pad], lv1.half) * zm1[par]
                    )
                    d1[to + lv1.pad, rows] = v
                    acc1[to + lv1.pad, rows] += v

    def use_up1(t, par, rows, av, edge):
        r = r1[t + lv1.pad, rows] - av
        r1[t + lv1.pad, rows] = r
        d1[t + lv1.pad, rows] = masked(wide(iv1[t + lv1.pad, par], n_rows(rows)) * r, edge)

    def use_final1(t, par, rows, av, edge):
        r = r1[t + lv1.pad, rows] - av
        c1[t + lv1.pad, rows] = (acc1[t + lv1.pad, rows] + (1.0 + KEEP) * d1[t + lv1.pad, rows]) + masked(
            (RATIO * wide(iv1[t + lv1.pad, par], n_rows(rows))) * r, edge
        )

    base1 = own_x * per

    def around(reach):
        lo, hi = (-reach) // lv1.group, (cx + reach) // lv1.group
        return lo, hi + 1 - lo

    up_lo, up_n = around(4)
    if up_n % 2:
        up_lo, up_n = up_lo - 1, up_n + 1
    fin_lo, fin_n = around(2)
    for lo, n, use in ((up_lo, up_n, use_up1), (fin_lo, fin_n, use_final1)):
        stage(lv1, d1, hh1, hl1, base1 + lo, n)
        sweep(
            lv1, hh1, hl1, weights('wa1'), ss1, zm1, base1 + lo, n, use, z_cut,
            lv1.half - z_cut,
        )

    up = 2 * lv1.group // lv0.group
    tau_lo = (lo_b - own_lo) // up
    tau_hi = (lo_b + n_b - 1 - own_lo) // up
    n_tau = fin_lo + fin_n - tau_lo
    jn = (lv0.half // 2 + 7) // 8 * 8
    lane_j = lax.broadcasted_iota(jnp.int32, (jn, LANES), 1) // gs
    bad = ((lane_j == 0) & (own_y == 0)) | ((lane_j == 2) & (own_y == wy - 1))
    turn = lax.rem(1 - own_y + wyp, wyp) * gs
    first = ZR // 2 - zh // 2
    wp0 = weights('wp0')
    for i in range(n_tau):
        at = base1 + (tau_lo + i + lv1.pad)

        def rows_of(par, start):
            v = pltpu.roll(c1[at, pl.ds(par * lv1.half + start, jn)], turn, 1)
            return jnp.where(bad, 0.0, v)

        e2, o2, e3 = rows_of(0, first), rows_of(1, first), rows_of(0, first + 1)
        zp0[i, pl.ds(0, jn, stride=2)] = e2
        zp0[i, pl.ds(1, jn, stride=2)] = o2
        zp0[i, pl.ds(lv0.half, jn, stride=2)] = 0.375 * e2 + 0.75 * o2 - 0.125 * e3
        zp0[i, pl.ds(lv0.half + 1, jn, stride=2)] = 0.75 * o2 + 0.375 * e3 - 0.125 * e2
        zh0[i], zl0[i] = split(zp0[i, 0 : lv0.rows])
    for i in range(tau_hi + 1 - tau_lo):
        n_in = min(2, n_tau - i)
        w = wp0[: n_in * LANES]
        e = jnp.dot(
            jnp.concatenate([zh0[i + j] for j in range(n_in)], axis=1), w,
            preferred_element_type=F32,
        ) + jnp.dot(
            jnp.concatenate([zl0[i + j] for j in range(n_in)], axis=1), w,
            preferred_element_type=F32,
        )
        for k in range(up):
            t = own_lo + up * (tau_lo + i) + k
            if lo_b <= t < lo_b + n_b:
                for par in range(2):
                    rows = slice(par * lv0.half, par * lv0.half + lv0.half)
                    v = e[rows, LANES * k : LANES * k + LANES] * (
                        wide(mk0[t + 1], lv0.half) * zm0[par]
                    )
                    d0[t + 1, rows] = v
                    if own(t):
                        acc0[t - own_lo, rows] += v

    def use_up(t, par, rows, av, edge):
        r = r0[t, rows] - av
        r0[t, rows] = r
        d0[t + 1, rows] = masked(wide(iv0[t + 1, par], n_rows(rows)) * r, edge)

    def use_final(t, par, rows, av, edge):
        r = r0[t, rows] - av
        acc0[t - own_lo, rows] += (1.0 + KEEP) * d0[t + 1, rows] + (
            RATIO * wide(iv0[t + 1, par], n_rows(rows))
        ) * r

    lo_c, n_c = reach(2, 1)
    stage(lv0, d0, hh0, hl0, lo_c, n_c)
    sweep(lv0, hh0, hl0, weights('wa0'), ss0, zm0, lo_c, n_c, use_up)
    stage(lv0, d0, hh0, hl0, own_lo, own_n)
    sweep(
        lv0, hh0, hl0, weights('wa0'), ss0, zm0, own_lo, own_n, use_final, zh, zh + hb
    )

    for i in range(own_n):
        for par in range(2):
            lo = par * lv0.half + zh
            tmp[pl.ds(par, hb, stride=2)] = acc0[i, lo : lo + hb]
        v = tmp[...].T.reshape(lv0.group, yh0, bz)
        out_ref[lv0.group * i : lv0.group * i + lv0.group] = v[:, H : H + by]

    for n, off in enumerate(xy_offs):
        for k in range(2):
            when(xy_step(off)[1], lambda: halo_copy(n, k).wait_send())
    for m in range(len(z_steps)):
        for n in range(len(spots)):
            when(strip_ok(n, m, 1), lambda: strip_copy(n, m).wait_send())
    for n, st in enumerate(x_steps):
        when(st[1], lambda: g_copy(n).wait_send())
    for m, (ok, jx) in enumerate(sources):

        def act():
            for n, st in enumerate(plane_steps):
                when(st[1], lambda: p_copy(n, m, jx).wait_send())

        when(ok, act)


def local(mesh_shape, u, b):
    nx, ny, nz = (mesh_shape[a] for a in ("gx", "gy", "gz"))
    bx, by, bz = u.shape
    cx, cy, cz = bx // 2, by // 2, bz // 2
    wx = nx if nx <= 2 * REACH + 1 else 2 * REACH + 1
    wy = ny if ny <= 2 * REACH + 1 else 2 * REACH + 1
    wyp = 4 if wy <= 4 else 8
    gs = LANES // wyp
    yh0 = by + 2 * H
    xg0 = LANES // yh0
    lv0 = Level(
        xg0, (bx + 2 * H) // xg0, yh0, (bz + 2 * H) // 2, lambda x, y: x * yh0 + y, H // 2, 1
    )
    xg1 = gs // cy
    lv1 = Level(
        xg1, cx * wx // xg1, cy * wy, (cz + 2 * ZR) // 2,
        lambda x, y: (y // cy) * gs + x * cy + y % cy, ZR // 2, 4,
    )
    y2 = cy * wy // 2
    yh2 = 16 if y2 <= 16 else 32
    xg2 = LANES // yh2
    lv2 = Level(
        xg2, -(-(cx * wx // 2) // xg2), y2, (cz + 2 * ZR) // 4, lambda x, y: x * yh2 + y,
        ZR // 4, 1,
    )

    own_lo = H // xg0
    lo_b = (H - 4) // xg0
    n_b = (H + bx - 1 + 3) // xg0 - lo_b + 1
    px = []
    for x in range(cx):
        for s, w in restrict_taps(x):
            f = H + 2 * x + s
            px.append(((0, x), f // xg0 - lo_b, f % xg0, w))
    py = [(y, H + 2 * y + s, w) for y in range(cy) for s, w in restrict_taps(y)]
    once = plane_matrix(n_b, 1, px, py, lv0.at, lambda x, y: x * cy + y)
    m_r0 = once + np.roll(once, LANES // 2, axis=1)

    r_lo, r_hi = (-3) // xg1, (2 * xg2 + 1) // xg1
    px = []
    for x in range(xg2):
        for s, w in restrict_taps(x):
            f = 2 * x + s
            px.append(((0, x), f // xg1 - r_lo, f % xg1, w))
    py = [
        (y, 2 * y + s, w) for y in range(y2) for s, w in restrict_taps(y)
        if 0 <= 2 * y + s < cy * wy
    ]
    m_r1 = plane_matrix(r_hi - r_lo + 1, 1, px, py, lv1.at, lv2.at)

    ratio = 2 * xg2 // xg1
    px = []
    for f in range(2 * xg2):
        for c, w in prolong_taps(f):
            px.append(((f // xg1, f % xg1), c // xg2, c % xg2, w))
    py = [
        (f, c, w) for f in range(cy * wy) for c, w in prolong_taps(f) if 0 <= c < y2
    ]
    m_p1 = plane_matrix(2, ratio, px, py, lv2.at, lv1.at)

    up = 2 * xg1 // xg0
    px = []
    for f in range(2 * xg1):
        for c, w in prolong_taps(f):
            px.append(((f // xg0, f % xg0), c // xg1, c % xg1, w))
    py = [
        (f + H, c + cy, w) for f in range(-H, by + H) for c, w in prolong_taps(f)
        if -cy <= c < 2 * cy
    ]
    m_p0 = plane_matrix(2, up, px, py, lv1.at, lv0.at)

    parts, stack, row = {}, [], 0
    for name, m in (
        ("wa0", operator_matrix(lv0)), ("wa1", operator_matrix(lv1)),
        ("wa2", operator_matrix(lv2)), ("wr0", m_r0), ("wr1", m_r1), ("wp1", m_p1),
        ("wp0", m_p0),
    ):
        if m.shape[1] == LANES:
            m = np.pad(m, ((0, m.shape[0] % 2), (0, 0)))
            half = m.shape[0] // 2
            assert half % 16 == 0
            parts[name] = [(row, 0, half, LANES), (row, LANES, half, LANES)]
            stack.append(np.concatenate([m[:half], m[half:]], axis=1))
            row += half
        else:
            parts[name] = []
            for c in range(0, m.shape[1], 256):
                parts[name].append((row, 0, m.shape[0], min(256, m.shape[1] - c)))
                piece = m[:, c : c + 256]
                stack.append(np.pad(piece, ((0, 0), (0, 256 - piece.shape[1]))))
                row += m.shape[0]
    consts = to_bf16(np.concatenate(stack, axis=0))
    vm = lambda *s: pltpu.VMEM(s, F32)
    bm = lambda *s: pltpu.VMEM(s, BF16)
    dma = lambda *s: pltpu.SemaphoreType.DMA(s)

    def per_level(lv):
        t, n, p = lv.tiles, lv.rows, lv.pad
        return (
            vm(t + 2 * p, n, LANES), vm(t + 2 * p, n, LANES), vm(t + 2 * p, n, LANES),
            bm(t + 2 * p + 2, n, LANES), bm(t + 2 * p + 2, n, LANES),
            vm(4, 4, lv.half + 16, LANES), vm(t + 2 * p, 2, 8, LANES),
            vm(t + 2 * p, 8, LANES), vm(2, lv.half, LANES),
        )

    p0, p1, p2 = per_level(lv0), per_level(lv1), per_level(lv2)
    tau_lo = (lo_b - own_lo) // up
    n_tau = (lo_b + n_b - 1 - own_lo) // up + 2 - tau_lo
    jn = (lv0.half // 2 + 7) // 8 * 8
    geo = (nx, ny, nz, bx, by, bz, wx, wy, wyp)
    near, side = (3 if nx > 1 else 1), (3 if ny > 1 else 1)
    n_z = 0 if nz == 1 else 1 if nz == 2 else 2
    n_x = max(1, nx - 1 if wx == nx else 2 * REACH)
    n_y = ny - 1 if wy == ny else 2 * REACH
    n_p = max(1, (n_y + 1) * (n_z + 1) - 1)
    n_xy, n_s = max(1, near * side - 1), near * side
    return pl.pallas_call(
        functools.partial(kernel, geo, lv0, lv1, lv2, parts),
        out_shape=pltpu.VMEM(u.shape, F32),
        in_specs=[pl.BlockSpec(memory_space=pl.ANY)] * 3,
        out_specs=pl.BlockSpec(memory_space=pltpu.VMEM),
        scratch_shapes=[
            bm(*consts.shape), vm(bx, by, bz), vm(bx, by, bz),
            vm(bx + 2 * H, yh0, bz), vm(bx + 2 * H, yh0, bz), vm(bz, LANES),
            vm(xg0, yh0, bz), vm(2, 3, 2, bx // xg0, H, LANES),
            vm(2, 3, 2, lv0.tiles, H, LANES),
            *p0, *p1, vm(lv1.tiles + 8, lv1.rows, LANES), p2[0], p2[1], *p2[3:],
            vm(2, lv0.half, LANES), vm(2, lv1.half + 16, LANES), vm(cz // 2, LANES),
            vm(wx, cz // 2, LANES), vm(wy, wx, lv1.half, LANES),
            vm(lv2.tiles, 2, lv2.half + 8, LANES), vm(lv2.tiles, lv1.rows, LANES),
            vm(n_tau, lv0.half + 2 * jn, LANES),
            bm(lv2.tiles, lv1.rows, LANES), bm(lv2.tiles, lv1.rows, LANES),
            bm(n_tau, lv0.rows, LANES), bm(n_tau, lv0.rows, LANES),
            dma(3), dma(n_xy, 2), dma(n_xy, 2), dma(n_s, max(1, n_z)), dma(n_s, max(1, n_z)),
            dma(n_x), dma(n_x), dma(n_p, n_x + 1), dma(n_p, n_x + 1),
        ],
        compiler_params=pltpu.CompilerParams(
            collective_id=0, has_side_effects=True, vmem_limit_bytes=60 * 1024 * 1024
        ),
    )(u, b, consts)


def solution(mesh):
    placed = P("gx", "gy", "gz")
    return jax.shard_map(
        functools.partial(local, dict(mesh.shape)), mesh=mesh,
        in_specs=(placed, placed), out_specs=placed, check_vma=False,
    )
```

```python
import functools

import jax
import jax.numpy as jnp
import numpy as np
from jax import lax
from jax.experimental import pallas as pl
from jax.experimental.pallas import tpu as pltpu
from jax.sharding import PartitionSpec as P

F32 = jnp.float32
BF16 = jnp.bfloat16
MESH = pl.DeviceIdType.MESH
H = 8
ZR = 32
REACH = 3
LANES = 128

RHO0 = 1.0 / 1.2
RHO1 = 1.0 / (2.4 - RHO0)
FIRST = 1.0 / 1.32
KEEP = RHO1 * RHO0
STEP = 2.0 * RHO1 / 1.1
RATIO = STEP / FIRST
UNIT = 2700.0


def restrict_taps(g):
    if g % 2 == 0:
        return ((-3, -0.125), (-1, 0.375), (0, 1.0), (1, 0.375), (3, -0.125))
    return ((-1, 0.75), (0, 1.0), (1, 0.75))


def prolong_taps(f):
    if f % 2 == 0:
        return ((f // 2, 1.0),)
    q = f // 4
    if f % 4 == 1:
        return ((2 * q, 0.375), (2 * q + 1, 0.75), (2 * q + 2, -0.125))
    return ((2 * q, -0.125), (2 * q + 1, 0.75), (2 * q + 2, 0.375))


def stiff_taps(i):
    if i % 2 == 0:
        return {-2: 1, -1: -8, 0: 14, 1: -8, 2: 1}
    return {-1: -8, 0: 16, 1: -8}


def mass_taps(i):
    if i % 2 == 0:
        return {-2: -1, -1: 2, 0: 8, 1: 2, 2: -1}
    return {-1: 2, 0: 16, 1: 2}


class Level:
    def __init__(self, group, tiles, height, half, at, parts, pad):
        self.group, self.tiles, self.height, self.half, self.at = group, tiles, height, half, at
        self.parts, self.pad = parts, pad
        self.rows = 2 * half
        self.paired = group >= 4


def operator_matrix(lv):
    k = 256 if lv.paired else 384
    m = np.zeros((k, 256), np.float64)
    for x in range(lv.group):
        for y in range(lv.height):
            for ox, mx in mass_taps(x).items():
                kx = stiff_taps(x)[ox]
                p = x + ox
                if lv.paired:
                    block = (p + lv.group // 2) // lv.group
                else:
                    block = p // lv.group + 1
                for oy, my in mass_taps(y).items():
                    ky = stiff_taps(y)[oy]
                    if not 0 <= y + oy < lv.height:
                        continue
                    row = block * LANES + lv.at(p % lv.group, y + oy)
                    both, mixed = mx * my, kx * my + mx * ky
                    m[row, lv.at(x, y)] = -8 * both + 2 * mixed
                    m[row, LANES + lv.at(x, y)] = both - mixed
    return m


def plane_matrix(n_in, n_out, pairs_x, pairs_y, at_in, at_out):
    m = np.zeros((n_in * LANES, n_out * LANES), np.float64)
    for (to, xo), ti, xi, wx in pairs_x:
        for yo, yi, wy in pairs_y:
            m[ti * LANES + at_in(xi, yi), to * LANES + at_out(xo, yo)] += wx * wy
    return m


def to_bf16(m):
    out = jnp.asarray(m, BF16)
    assert np.array_equal(np.asarray(m, jnp.bfloat16).astype(np.float64), m)
    return out


def split(v):
    hi = v.astype(BF16)
    return hi, (v - hi.astype(F32)).astype(BF16)


def loop(count, body, most=9):
    if count <= most:
        for i in range(count):
            body(i)
    else:

        def step(i, carry):
            body(i)
            return carry

        lax.fori_loop(0, count, step, 0)


def kernel(
    geo, lv0, lv1, lv2, parts, u_hbm, b_hbm, w_hbm, out_ref, *refs,
):
    (wall, u_ref, b_ref, ue, be, tmp, pad, strip_out, strip_in,
     d0, r0, acc0, hh0, hl0, ss0, iv0, mk0, zm0,
     d1, r1, acc1, hh1, hl1, ss1, iv1, mk1, zm1, c1,
     d2, r2, hh2, hl2, ss2, iv2, mk2, zm2,
     xs0, xs1, blk, line, land, up2, zp1, zp0, zh1, zl1, zh0, zl0,
     wsem, xysend, xyrecv, zsend, zrecv, gsend, grecv, psend, precv) = refs
    nx, ny, nz, bx, by, bz, wx, wy, wyp = geo
    ix, iy, iz = lax.axis_index("gx"), lax.axis_index("gy"), lax.axis_index("gz")
    place, counts = (ix, iy, iz), (nx, ny, nz)
    full_x, full_y = wx == nx, wy == ny
    cx, cy, cz = bx // 2, by // 2, bz // 2
    start_x = 0 if full_x else ix - REACH
    start_y = 0 if full_y else iy - REACH
    own_x = ix if full_x else REACH
    own_y = iy if full_y else REACH

    def both(*oks):
        ok = None
        for o in oks:
            if o is not None:
                ok = o if ok is None else ok & o
        return ok

    def when(ok, act):
        if ok is None:
            act()
        else:
            pl.when(ok)(act)

    def unless(ok, act):
        if ok is not None:
            pl.when(jnp.logical_not(ok))(act)

    def inside(axis, p):
        return (p >= 0) & (p < counts[axis])

    def shifted(axis, off):
        if off == 0:
            return (place[axis], None, place[axis], None)
        to, source = place[axis] + off, place[axis] - off
        return (to, inside(axis, to), source, inside(axis, source))

    def line_steps(axis, full):
        p, n = place[axis], counts[axis]
        if full:
            steps = []
            for k in sorted(range(1, n), key=lambda k: -k):
                to, source = lax.rem(p + k, n), lax.rem(p + n - k, n)
                steps.append((to, None, source, None, p, source))
            return steps
        offs = sorted((o for o in range(-REACH, REACH + 1) if o), key=abs)
        return [shifted(axis, o) + (REACH - o, REACH - o) for o in offs]

    zq, half_c = ZR // 2, cz // 2
    x_steps = line_steps(0, full_x)
    y_steps = line_steps(1, full_y)
    if nz == 2:
        z_steps = [
            (1 - iz, None, 1 - iz, None, 1 - iz,
             pl.multiple_of((1 - iz) * (half_c - zq), 8),
             pl.multiple_of(iz * (zq + half_c), 8))
        ]
    elif nz > 2:
        z_steps = [
            shifted(2, 1) + (1, half_c - zq, 0), shifted(2, -1) + (0, 0, zq + half_c)
        ]
    else:
        z_steps = []
    plane_steps = [
        ((ix, ys[0], iz), ys[1], ys[3], ys[4], None) for ys in y_steps
    ] + [
        ((ix, iy, zs[0]), zs[1], zs[3], own_y, zs) for zs in z_steps
    ] + [
        ((ix, ys[0], zs[0]), both(ys[1], zs[1]), both(ys[3], zs[3]), ys[4], zs)
        for zs in z_steps for ys in y_steps
    ]
    near = [0] + ([-1, 1] if nx > 1 else [])
    side = [0] + ([-1, 1] if ny > 1 else [])
    xy_offs = [(a, c) for a in near for c in side if a or c]

    def xy_step(off):
        xs, ys = shifted(0, off[0]), shifted(1, off[1])
        return (xs[0], ys[0]), both(xs[1], ys[1]), both(xs[3], ys[3])

    greet = [((st[0], iy, iz), st[1], st[3]) for st in x_steps]
    greet += [(st[0], st[1], st[2]) for st in plane_steps]
    for off in xy_offs:
        if off[0]:
            to, ok, ok_from = xy_step(off)
            if off[1]:
                greet.append((to + (iz,), ok, ok_from))
            for zs in z_steps:
                greet.append((to + (zs[0],), both(ok, zs[1]), both(ok_from, zs[3])))

    barrier = pltpu.get_barrier_semaphore()
    total = 0
    for to, ok, ok_from in greet:
        total = total + (1 if ok_from is None else ok_from.astype(jnp.int32))

        def signal():
            pl.semaphore_signal(barrier, inc=1, device_id=to, device_id_type=MESH)

        when(ok, signal)

    load_u = pltpu.make_async_copy(u_hbm, u_ref, wsem.at[0])
    load_b = pltpu.make_async_copy(b_hbm, b_ref, wsem.at[1])
    load_w = pltpu.make_async_copy(w_hbm, wall, wsem.at[2])
    load_u.start()
    load_b.start()
    load_w.start()

    def remote(src, dst, ss, rs, to):
        return pltpu.make_async_remote_copy(
            src_ref=src, dst_ref=dst, send_sem=ss, recv_sem=rs,
            device_id=to, device_id_type=MESH,
        )

    def weights(name):
        blocks = []
        for row, lane, rows, lanes in parts[name]:
            blocks.append(wall[row : row + rows, lane : lane + lanes])
        if parts[name][0][3] == LANES:
            return jnp.concatenate(blocks, axis=0)
        return jnp.concatenate(blocks, axis=1)

    def cut(off, size, low, high):
        if off == 0:
            return slice(0, size), slice(H, H + size)
        if off > 0:
            return slice(size - low, size), slice(H - low, H)
        return slice(0, high), slice(H + size, H + size + high)

    fields = ((u_ref, ue, H, H - 1), (b_ref, be, H - 2, H - 3))

    def halo_cut(off, k):
        ref, ext, low, high = fields[k]
        sx, tx = cut(off[0], bx, low, high)
        sy, ty = cut(off[1], by, H, H)
        return ref, ext, sx, tx, sy, ty

    def zero(ref, *at):
        ref[at] = jnp.zeros_like(ref[at])

    def halo_copy(n, k):
        ref, ext, sx, tx, sy, ty = halo_cut(xy_offs[n], k)
        to = xy_step(xy_offs[n])[0] + (iz,)
        return remote(ref.at[sx, sy], ext.at[tx, ty], xysend.at[n, k], xyrecv.at[n, k], to)

    yh0 = by + 2 * H
    zh, hb = H // 2, bz // 2
    own_lo, own_n = H // lv0.group, bx // lv0.group
    edge_n = H // lv0.group
    spots = [(a, c) for a in near for c in side]

    def variant(c):
        return 0 if c == 0 else (1 if c > 0 else 2)

    def strip_cut(a):
        if a == 0:
            return slice(0, own_n), slice(own_lo, own_lo + own_n)
        if a > 0:
            return slice(own_n - edge_n, own_n), slice(0, edge_n)
        return slice(0, edge_n), slice(own_lo + own_n, own_lo + own_n + edge_n)

    def strip_copy(n, m):
        a, c = spots[n]
        zs = z_steps[m]
        src, dst = strip_cut(a)
        v, k = variant(c), zs[4]
        to = (shifted(0, a)[0], shifted(1, c)[0], zs[0])
        return remote(
            strip_out.at[k, v, :, src], strip_in.at[k, v, :, dst],
            zsend.at[n, m], zrecv.at[n, m], to,
        )

    def strip_ok(n, m, at):
        a, c = spots[n]
        return both(shifted(0, a)[at], shifted(1, c)[at], z_steps[m][at])

    zero(pad, slice(None), slice(0, H))
    zero(pad, slice(None), slice(H + by, yh0))
    lane_y = lax.broadcasted_iota(jnp.int32, (2 * zh, LANES), 1) % yh0
    load_u.wait()
    load_b.wait()
    for k, ref in enumerate((u_ref, b_ref)):
        for t in range(own_n):
            pad[:, H : H + by] = ref[lv0.group * t : lv0.group * t + lv0.group]
            tmp[...] = pad[...].reshape(LANES, bz).T
            for s, start in ((0, 0), (1, bz - H)):
                v = jnp.concatenate(
                    [tmp[pl.ds(start + par, zh, stride=2)] for par in range(2)], axis=0
                )
                strip_out[s, 0, k, t] = v
                if ny > 1:
                    strip_out[s, 1, k, t] = jnp.where(
                        lane_y < H, pltpu.roll(v, LANES - by, 1), 0.0
                    )
                    strip_out[s, 2, k, t] = jnp.where(
                        lane_y >= H + by, pltpu.roll(v, by, 1), 0.0
                    )

    pl.semaphore_wait(barrier, total)
    for m in range(len(z_steps)):
        for n in sorted(range(len(spots)), key=lambda n: -abs(spots[n][0]) - abs(spots[n][1])):
            when(strip_ok(n, m, 1), lambda: strip_copy(n, m).start())
    far_first = sorted(range(len(xy_offs)), key=lambda n: -abs(xy_offs[n][0] * xy_offs[n][1]))
    for n in far_first:
        when(xy_step(xy_offs[n])[1], lambda: halo_copy(n, 0).start())
    for n in far_first:
        when(xy_step(xy_offs[n])[1], lambda: halo_copy(n, 1).start())

    ue[H : H + bx, H : H + by] = u_ref[...]
    be[H : H + bx, H : H + by] = b_ref[...]
    for _, ext, low, high in fields:
        for at in (slice(0, H - low), slice(H + bx + high, 2 * H + bx)):
            if at.stop > at.start:
                zero(ext, at)
    for off in [(a, c) for a in (-1, 0, 1) for c in (-1, 0, 1) if a or c]:

        def clear():
            for k in range(2):
                _, ext, _, tx, _, ty = halo_cut(off, k)
                zero(ext, tx, ty)

        if off in xy_offs:
            unless(xy_step(off)[2], clear)
        else:
            clear()
    for s, rows in ((0, slice(zq + half_c, 2 * zq + half_c)), (1, slice(0, zq))):
        z_ok = inside(2, iz + (1 - 2 * s)) if nz > 1 else None
        for a in (-1, 0, 1):
            for c in (-1, 0, 1):

                def clear():
                    zero(strip_in, s, variant(c), slice(None), strip_cut(a)[1])

                if (a, c) in spots and nz > 1:
                    unless(both(shifted(0, a)[3], shifted(1, c)[3], z_ok), clear)
                else:
                    clear()

        def clear():
            zero(land, slice(None), slice(None), rows)

        if nz > 1:
            unless(z_ok, clear)
        else:
            clear()
    for st in x_steps:
        unless(st[3], lambda: zero(land, slice(None), st[5]))
    for st in y_steps:
        unless(st[3], lambda: zero(land, st[5]))

    def set_up(lv, level, iv, mk, zm, d, ss, x_first, y_first, z_first, x_at, y_at):
        lane = lax.broadcasted_iota(jnp.int32, (8, LANES), 1)
        row = lax.broadcasted_iota(jnp.int32, (lv.half, LANES), 0)
        xx, yy = x_at(lane), y_at(lane)
        x_even, y_even = xx % 2 == 0, yy % 2 == 0
        n_x, n_y, n_z = (nx * bx) >> level, (ny * by) >> level, (nz * bz) >> level
        gy = y_first + yy
        y_ok = (gy >= 0) & (gy < n_y) & (yy < lv.height)
        mass = lambda e: jnp.where(e, 8.0, 16.0) / 30.0
        stiff = lambda e: jnp.where(e, 14.0, 16.0) / 3.0
        my, ky, mx, kx = mass(y_even), stiff(y_even), mass(x_even), stiff(x_even)
        inv = []
        for kz, mz in ((14.0 / 3.0, 8.0 / 30.0), (16.0 / 3.0, 16.0 / 30.0)):
            inv.append((FIRST / UNIT) / (kx * my * mz + mx * ky * mz + mx * my * kz))

        def one(i):
            gx = x_first + (i - lv.pad) * lv.group + xx
            ok = jnp.where(y_ok & (gx >= 0) & (gx < n_x), 1.0, 0.0).astype(F32)
            mk[i] = ok
            iv[i, 0] = inv[0] * ok
            iv[i, 1] = inv[1] * ok

        loop(lv.tiles + 2 * lv.pad, one, 16)
        for par in range(2):
            gz = z_first + 2 * row + par
            zm[par] = jnp.where((gz >= 0) & (gz < n_z), 1.0, 0.0).astype(F32)
        zero(d, slice(0, lv.pad))
        zero(d, slice(lv.tiles + lv.pad, lv.tiles + 2 * lv.pad))
        ss[:, :, 0:8] = jnp.zeros_like(ss[:, :, 0:8])
        ss[:, :, 8 + lv.half :] = jnp.zeros_like(ss[:, :, 8 + lv.half :])

    gs = LANES // wyp
    set_up(
        lv0, 0, iv0, mk0, zm0, d0, ss0, ix * bx - H, iy * by - H, iz * bz - H,
        lambda n: n // yh0, lambda n: n % yh0,
    )
    set_up(
        lv1, 1, iv1, mk1, zm1, d1, ss1, start_x * cx, start_y * cy, iz * cz - ZR,
        lambda n: (n % gs) // cy, lambda n: (n // gs) * cy + n % cy,
    )
    yh2 = LANES // lv2.group
    set_up(
        lv2, 2, iv2, mk2, zm2, d2, ss2, start_x * (cx // 2), start_y * (cy // 2),
        iz * (cz // 2) - ZR // 2, lambda n: n // yh2, lambda n: n % yh2,
    )
    for ref in (r1, acc1):
        zero(ref, slice(0, lv1.pad))
        zero(ref, slice(lv1.tiles + lv1.pad, lv1.tiles + 2 * lv1.pad))
    xs1[:, 0:8] = jnp.zeros_like(xs1[:, 0:8])
    xs1[:, 8 + lv1.half :] = jnp.zeros_like(xs1[:, 8 + lv1.half :])
    up2[...] = jnp.zeros_like(up2)

    def turn_field(k):
        ext = (ue, be)[k]
        for n, off in enumerate(xy_offs):
            when(xy_step(off)[2], lambda: halo_copy(n, k).wait_recv())
        for t in range(lv0.tiles):
            tmp[...] = ext[lv0.group * t : lv0.group * t + lv0.group].reshape(LANES, bz).T
            for par in range(2):
                val = tmp[pl.ds(par, hb, stride=2)]
                lo = par * lv0.half + zh
                if k == 0:
                    d0[t + 1, lo : lo + hb] = val
                else:
                    r0[t, lo : lo + hb] = UNIT * val - r0[t, lo : lo + hb]

    def fill_strips(k):
        for t in range(lv0.tiles):
            for s in range(2):
                v = (strip_in[s, 0, k, t] + strip_in[s, 1, k, t]) + strip_in[s, 2, k, t]
                for par in range(2):
                    lo = par * lv0.half + (0 if s else zh + hb)
                    rows, part = slice(lo, lo + zh), v[par * zh : par * zh + zh]
                    if k == 0:
                        d0[t + 1, rows] = part
                    else:
                        r0[t, rows] = UNIT * part - r0[t, rows]

    turn_field(0)
    for m in range(len(z_steps)):
        for n in range(len(spots)):
            when(strip_ok(n, m, 3), lambda: strip_copy(n, m).wait_recv())
    fill_strips(0)

    def stage(lv, d, hh, hl, lo, count):
        step = 48 if lv.rows % 48 == 0 else min(lv.rows, 64)
        lane = lax.broadcasted_iota(jnp.int32, (step, LANES), 1)
        if lv is lv1:
            plane = (lane % gs) // cy
        else:
            plane = lane // (LANES // lv.group)
        low = plane < lv.group // 2

        def one(i):
            t = lo + i
            for s in range(0, lv.rows, step):
                rows = slice(s, s + step)
                if lv.paired:
                    v = jnp.where(low, d[t + lv.pad, rows], d[t + lv.pad - 1, rows])
                else:
                    v = d[t + lv.pad - 1, rows]
                hh[t + lv.pad, rows], hl[t + lv.pad, rows] = split(v)

        loop(count + (1 if lv.paired else 2), one)

    def sweep(lv, hh, hl, w, ss, zm, lo, count, use, r_lo=0, r_hi=None):
        r_hi = lv.half if r_hi is None else r_hi
        chunk = next(c for c in (32, 24, 28, 8) if (r_hi - r_lo) % c == 0)
        n_cat = 2 if lv.paired else 3
        size = 2 if count % 2 == 0 else 1

        def group(i):
            t0 = lo + size * i

            def lhs(h):
                return jnp.concatenate(
                    [h[pl.ds(t0 + j + lv.pad, size)].reshape(size * lv.rows, LANES) for j in range(n_cat)],
                    axis=1,
                )

            s = jnp.dot(lhs(hh), w, preferred_element_type=F32) + jnp.dot(
                lhs(hl), w, preferred_element_type=F32
            )
            for k in range(size):
                slot = (i % 2) * 2 + k if isinstance(i, int) else k
                for par in range(2):
                    at = k * lv.rows + par * lv.half
                    for c in range(2):
                        ss[slot, 2 * c + par, 8 : 8 + lv.half] = s[
                            at : at + lv.half, LANES * c : LANES * c + LANES
                        ]
                t = t0 + k
                for at in range(r_lo, r_hi, chunk):

                    def rows_of(n, shift=0):
                        return ss[slot, n, pl.ds(8 + at + shift, chunk)]

                    even = (
                        (-11.0 / 3.0) * rows_of(0) + (-46.0 / 3.0) * rows_of(2)
                    ) + ((rows_of(1) + rows_of(1, -1)) + (rows_of(2, -1) + rows_of(2, 1)))
                    odd = ((-16.0 / 3.0) * rows_of(1) + (-80.0 / 3.0) * rows_of(3)) + (
                        rows_of(0) + rows_of(0, 1)
                    )
                    for par, val in enumerate((even, odd)):
                        edge = None
                        if at < lv.parts or at + chunk > lv.half - lv.parts:
                            edge = zm[par, at : at + chunk]
                        use(t, par, slice(par * lv.half + at, par * lv.half + at + chunk), val, edge)

        loop(count // size, group, 4)

    def wide(v, n):
        return jnp.broadcast_to(v[0:1], (n, LANES))

    def masked(v, edge):
        return v if edge is None else v * edge

    def n_rows(rows):
        return rows.stop - rows.start

    def own(t):
        return own_lo <= t < own_lo + own_n

    def reach(below, above):
        lo = (H - below) // lv0.group
        hi = (H + bx - 1 + above) // lv0.group
        return lo, hi - lo + 1

    def use_product(t, par, rows, av, edge):
        r0[t, rows] = av

    def first_step(t):
        size = 24 if lv0.half % 24 == 0 else 8
        for par in range(2):
            for at in range(0, lv0.half, size):
                rows = slice(par * lv0.half + at, par * lv0.half + at + size)
                d = wide(iv0[t + 1, par], size) * r0[t, rows] * zm0[par, at : at + size]
                if own(t):
                    acc0[t - own_lo, rows] = d0[t + 1, rows] + d
                d0[t + 1, rows] = d

    def use_step(t, par, rows, av, edge):
        r = r0[t, rows] - av
        r0[t, rows] = r
        d = KEEP * d0[t + 1, rows] + masked(
            (RATIO * wide(iv0[t + 1, par], n_rows(rows))) * r, edge
        )
        if own(t):
            acc0[t - own_lo, rows] += d
        d0[t + 1, rows] = d

    def use_down(t, par, rows, av, edge):
        r0[t, rows] = masked((r0[t, rows] - av) * wide(mk0[t + 1], n_rows(rows)), edge)

    lo_a, n_a = reach(6, 5)
    lo_b, n_b = reach(4, 3)
    load_w.wait()
    stage(lv0, d0, hh0, hl0, lo_a, n_a)
    sweep(lv0, hh0, hl0, weights('wa0'), ss0, zm0, lo_a, n_a, use_product)
    turn_field(1)
    fill_strips(1)
    for t in range(lo_a, lo_a + n_a):
        first_step(t)
    stage(lv0, d0, hh0, hl0, lo_b, n_b)
    sweep(lv0, hh0, hl0, weights('wa0'), ss0, zm0, lo_b, n_b, use_step)
    stage(lv0, d0, hh0, hl0, lo_b, n_b)
    sweep(lv0, hh0, hl0, weights('wa0'), ss0, zm0, lo_b, n_b, use_down)

    def restricted(parts, w):
        hi, lo = zip(*[split(p) for p in parts])
        return jnp.dot(
            jnp.concatenate(hi, axis=1), w, preferred_element_type=F32
        ) + jnp.dot(jnp.concatenate(lo, axis=1), w, preferred_element_type=F32)

    x = restricted([r0[lo_b + i] for i in range(n_b)], weights('wr0'))
    xs0[0] = x[: lv0.half]
    xs0[1] = x[lv0.half :]
    def pick(ref, par, start, n):
        return ref[par, pl.ds(start, n, stride=2)]

    def z_restricted(ref, even0, odd0, n):
        even = (
            0.5 * pick(ref, 0, even0, n)
            + 0.1875 * (pick(ref, 1, odd0, n) + pick(ref, 1, odd0 + 1, n))
            - 0.0625 * (pick(ref, 1, odd0 - 1, n) + pick(ref, 1, odd0 + 2, n))
        )
        odd = 0.5 * pick(ref, 0, even0 + 1, n) + 0.375 * (
            pick(ref, 1, odd0 + 1, n) + pick(ref, 1, odd0 + 2, n)
        )
        return even, odd

    even, odd = z_restricted(xs0, zh, zh - 1, half_c)
    lane_c = lax.broadcasted_iota(jnp.int32, (half_c, LANES), 1)
    packed = jnp.where(lane_c < LANES // 2, even, odd)
    blk[...] = packed

    def g_copy(n):
        st = x_steps[n]
        return remote(blk, line.at[st[4]], gsend.at[n], grecv.at[n], (st[0], iy, iz))

    sources = [(None, own_x)] + [(st[3], st[5]) for st in x_steps]

    step_rows = sum(half_c if st[4] is None else zq for st in plane_steps)
    merged = (
        full_x and full_y and nz <= 2 and step_rows > 0 and step_rows % yh0 == 0
        and (step_rows // yh0) * len(sources) <= bx + 2 * H
    )

    def all_of(sem, steps):
        ref = ue.at[0 : steps * step_rows // yh0]
        return pltpu.make_async_copy(ref, ref, sem)

    def p_copy(n, m, jx):
        to, _, _, jy, zs = plane_steps[n]
        if zs is None:
            src, dst = pl.ds(0, half_c), pl.ds(zq, half_c)
        else:
            src, dst = pl.ds(zs[5], zq), pl.ds(zs[6], zq)
        from_ref = blk if m == 0 else line.at[jx]
        return remote(
            from_ref.at[src], land.at[jy, jx, dst],
            psend.at[0, 0] if merged else psend.at[n, m],
            precv.at[0, m] if merged else precv.at[n, m], to,
        )

    for n in reversed(range(len(x_steps))):
        when(x_steps[n][1], lambda: g_copy(n).start())
    for m, (ok, jx) in enumerate(sources):

        def act():
            if m:
                g_copy(m - 1).wait_recv()
            for n in reversed(range(len(plane_steps))):
                when(plane_steps[n][1], lambda: p_copy(n, m, jx).start())
            land[own_y, jx, zq : zq + half_c] = packed if m == 0 else line[jx]

        when(ok, act)
    for n, off in enumerate(xy_offs):
        for k in range(2):
            when(xy_step(off)[1], lambda: halo_copy(n, k).wait_send())
    for m in range(len(z_steps)):
        for n in range(len(spots)):
            when(strip_ok(n, m, 1), lambda: strip_copy(n, m).wait_send())

    per = cx // lv1.group
    lane_h = lax.broadcasted_iota(jnp.int32, (lv1.half, LANES), 1) // gs

    def place_block(jx):
        blocks = [land[jy, jx] for jy in range(wy)]
        for s in range(per):
            t = jx * per + s
            for par in range(2):
                at = par * (LANES // 2) + s * gs
                val = None
                for jy in range(wy):
                    shift = (jy * gs - at) % LANES
                    v = pltpu.roll(blocks[jy], shift, 1) if shift else blocks[jy]
                    if val is None:
                        val = v if wy == wyp else jnp.where(lane_h == jy, v, 0.0)
                    else:
                        val = jnp.where(lane_h == jy, v, val)
                rows = slice(par * lv1.half, par * lv1.half + lv1.half)
                r1[t + lv1.pad, rows] = val
                d = (wide(iv1[t + lv1.pad, par], lv1.half) * zm1[par]) * val
                d1[t + lv1.pad, rows] = d
                acc1[t + lv1.pad, rows] = d

    for m, (ok, jx) in enumerate(sources):

        def act():
            if merged:
                all_of(precv.at[0, m], 1).wait()
                return
            for n, st in enumerate(plane_steps):
                when(st[2], lambda: p_copy(n, m, jx).wait_recv())

        when(ok, act)
        place_block(jx)

    def use_step1(t, par, rows, av, edge):
        r = r1[t + lv1.pad, rows] - av
        r1[t + lv1.pad, rows] = r
        d = KEEP * d1[t + lv1.pad, rows] + masked(
            (RATIO * wide(iv1[t + lv1.pad, par], n_rows(rows))) * r, edge
        )
        d1[t + lv1.pad, rows] = d
        acc1[t + lv1.pad, rows] += d

    def use_down1(t, par, rows, av, edge):
        r1[t + lv1.pad, rows] = masked((r1[t + lv1.pad, rows] - av) * wide(mk1[t + lv1.pad], n_rows(rows)), edge)

    n1 = lv1.tiles
    stage(lv1, d1, hh1, hl1, 0, n1)
    z_cut = ZR // 4
    sweep(lv1, hh1, hl1, weights('wa1'), ss1, zm1, 0, n1, use_step1, z_cut)
    stage(lv1, d1, hh1, hl1, 0, n1)
    sweep(
        lv1, hh1, hl1, weights('wa1'), ss1, zm1, 0, n1, use_down1, z_cut, lv1.half - z_cut
    )

    ratio = 2 * lv2.group // lv1.group
    r_lo = (-3) // lv1.group
    r_hi = (2 * lv2.group + 1) // lv1.group
    wr1 = weights('wr1')
    for t in range(lv2.tiles):
        a, e = max(0, ratio * t + r_lo), min(n1 - 1, ratio * t + r_hi)
        skip = (a - (ratio * t + r_lo)) * LANES
        x = restricted(
            [r1[i + lv1.pad] for i in range(a, e + 1)], wr1[skip : skip + (e + 1 - a) * LANES]
        )
        xs1[0, 8 : 8 + lv1.half] = x[: lv1.half]
        xs1[1, 8 : 8 + lv1.half] = x[lv1.half :]
        for par, val in enumerate(z_restricted(xs1, 8, 7, lv2.half)):
            rows = slice(par * lv2.half, par * lv2.half + lv2.half)
            r2[t, rows] = val
            d2[t + 1, rows] = (wide(iv2[t + 1, par], lv2.half) * zm2[par]) * val

    def use_last(t, par, rows, av, edge):
        r = r2[t, rows] - av
        step = masked((RATIO * wide(iv2[t + 1, par], n_rows(rows))) * r, edge)
        lo = rows.start - par * lv2.half
        up2[t, par, lo : lo + n_rows(rows)] = (1.0 + KEEP) * d2[t + 1, rows] + step

    stage(lv2, d2, hh2, hl2, 0, lv2.tiles)
    sweep(lv2, hh2, hl2, weights('wa2'), ss2, zm2, 0, lv2.tiles, use_last)

    n2 = lv2.half
    wp1 = weights('wp1')
    for t in range(lv2.tiles):
        e2, o2, e3 = up2[t, 0, 0:n2], up2[t, 1, 0:n2], up2[t, 0, 1 : n2 + 1]
        zp1[t, pl.ds(0, n2, stride=2)] = e2
        zp1[t, pl.ds(1, n2, stride=2)] = o2
        zp1[t, pl.ds(lv1.half, n2, stride=2)] = 0.375 * e2 + 0.75 * o2 - 0.125 * e3
        zp1[t, pl.ds(lv1.half + 1, n2, stride=2)] = 0.75 * o2 + 0.375 * e3 - 0.125 * e2
        zh1[t], zl1[t] = split(zp1[t])
    for t in range(lv2.tiles):
        n_in = min(2, lv2.tiles - t)
        w = wp1[: n_in * LANES]
        e = jnp.dot(
            jnp.concatenate([zh1[t + i] for i in range(n_in)], axis=1), w,
            preferred_element_type=F32,
        ) + jnp.dot(
            jnp.concatenate([zl1[t + i] for i in range(n_in)], axis=1), w,
            preferred_element_type=F32,
        )
        for k in range(ratio):
            to = ratio * t + k
            if to < n1:
                for par in range(2):
                    rows = slice(par * lv1.half, par * lv1.half + lv1.half)
                    v = e[rows, LANES * k : LANES * k + LANES] * (
                        wide(mk1[to + lv1.pad], lv1.half) * zm1[par]
                    )
                    d1[to + lv1.pad, rows] = v
                    acc1[to + lv1.pad, rows] += v

    def use_up1(t, par, rows, av, edge):
        r = r1[t + lv1.pad, rows] - av
        r1[t + lv1.pad, rows] = r
        d1[t + lv1.pad, rows] = masked(wide(iv1[t + lv1.pad, par], n_rows(rows)) * r, edge)

    def use_final1(t, par, rows, av, edge):
        r = r1[t + lv1.pad, rows] - av
        c1[t + lv1.pad, rows] = (acc1[t + lv1.pad, rows] + (1.0 + KEEP) * d1[t + lv1.pad, rows]) + masked(
            (RATIO * wide(iv1[t + lv1.pad, par], n_rows(rows))) * r, edge
        )

    base1 = own_x * per

    def around(reach):
        lo, hi = (-reach) // lv1.group, (cx + reach) // lv1.group
        return lo, hi + 1 - lo

    up_lo, up_n = around(4)
    if up_n % 2:
        up_lo, up_n = up_lo - 1, up_n + 1
    fin_lo, fin_n = around(2)
    for lo, n, use in ((up_lo, up_n, use_up1), (fin_lo, fin_n, use_final1)):
        stage(lv1, d1, hh1, hl1, base1 + lo, n)
        sweep(
            lv1, hh1, hl1, weights('wa1'), ss1, zm1, base1 + lo, n, use, z_cut,
            lv1.half - z_cut,
        )

    up = 2 * lv1.group // lv0.group
    tau_lo = (lo_b - own_lo) // up
    tau_hi = (lo_b + n_b - 1 - own_lo) // up
    n_tau = fin_lo + fin_n - tau_lo
    jn = (lv0.half // 2 + 7) // 8 * 8
    lane_j = lax.broadcasted_iota(jnp.int32, (jn, LANES), 1) // gs
    bad = ((lane_j == 0) & (own_y == 0)) | ((lane_j == 2) & (own_y == wy - 1))
    turn = lax.rem(1 - own_y + wyp, wyp) * gs
    first = ZR // 2 - zh // 2
    wp0 = weights('wp0')
    for i in range(n_tau):
        at = base1 + (tau_lo + i + lv1.pad)

        def rows_of(par, start):
            v = pltpu.roll(c1[at, pl.ds(par * lv1.half + start, jn)], turn, 1)
            return jnp.where(bad, 0.0, v)

        e2, o2, e3 = rows_of(0, first), rows_of(1, first), rows_of(0, first + 1)
        zp0[i, pl.ds(0, jn, stride=2)] = e2
        zp0[i, pl.ds(1, jn, stride=2)] = o2
        zp0[i, pl.ds(lv0.half, jn, stride=2)] = 0.375 * e2 + 0.75 * o2 - 0.125 * e3
        zp0[i, pl.ds(lv0.half + 1, jn, stride=2)] = 0.75 * o2 + 0.375 * e3 - 0.125 * e2
        zh0[i], zl0[i] = split(zp0[i, 0 : lv0.rows])
    for i in range(tau_hi + 1 - tau_lo):
        n_in = min(2, n_tau - i)
        w = wp0[: n_in * LANES]
        e = jnp.dot(
            jnp.concatenate([zh0[i + j] for j in range(n_in)], axis=1), w,
            preferred_element_type=F32,
        ) + jnp.dot(
            jnp.concatenate([zl0[i + j] for j in range(n_in)], axis=1), w,
            preferred_element_type=F32,
        )
        for k in range(up):
            t = own_lo + up * (tau_lo + i) + k
            if lo_b <= t < lo_b + n_b:
                for par in range(2):
                    rows = slice(par * lv0.half, par * lv0.half + lv0.half)
                    v = e[rows, LANES * k : LANES * k + LANES] * (
                        wide(mk0[t + 1], lv0.half) * zm0[par]
                    )
                    d0[t + 1, rows] = v
                    if own(t):
                        acc0[t - own_lo, rows] += v

    def use_up(t, par, rows, av, edge):
        r = r0[t, rows] - av
        r0[t, rows] = r
        d0[t + 1, rows] = masked(wide(iv0[t + 1, par], n_rows(rows)) * r, edge)

    def use_final(t, par, rows, av, edge):
        r = r0[t, rows] - av
        acc0[t - own_lo, rows] += (1.0 + KEEP) * d0[t + 1, rows] + (
            RATIO * wide(iv0[t + 1, par], n_rows(rows))
        ) * r

    lo_c, n_c = reach(2, 1)
    stage(lv0, d0, hh0, hl0, lo_c, n_c)
    sweep(lv0, hh0, hl0, weights('wa0'), ss0, zm0, lo_c, n_c, use_up)
    stage(lv0, d0, hh0, hl0, own_lo, own_n)
    sweep(
        lv0, hh0, hl0, weights('wa0'), ss0, zm0, own_lo, own_n, use_final, zh, zh + hb
    )

    for i in range(own_n):
        for par in range(2):
            lo = par * lv0.half + zh
            tmp[pl.ds(par, hb, stride=2)] = acc0[i, lo : lo + hb]
        v = tmp[...].T.reshape(lv0.group, yh0, bz)
        out_ref[lv0.group * i : lv0.group * i + lv0.group] = v[:, H : H + by]

    for n, st in enumerate(x_steps):
        when(st[1], lambda: g_copy(n).wait_send())
    if merged:
        all_of(psend.at[0, 0], len(sources)).wait()
    for m, (ok, jx) in enumerate(sources):

        def act():
            for n, st in enumerate(plane_steps):
                when(st[1], lambda: p_copy(n, m, jx).wait_send())

        if not merged:
            when(ok, act)


def local(mesh_shape, u, b):
    nx, ny, nz = (mesh_shape[a] for a in ("gx", "gy", "gz"))
    bx, by, bz = u.shape
    cx, cy, cz = bx // 2, by // 2, bz // 2
    wx = nx if nx <= 2 * REACH + 1 else 2 * REACH + 1
    wy = ny if ny <= 2 * REACH + 1 else 2 * REACH + 1
    wyp = 4 if wy <= 4 else 8
    gs = LANES // wyp
    yh0 = by + 2 * H
    xg0 = LANES // yh0
    lv0 = Level(
        xg0, (bx + 2 * H) // xg0, yh0, (bz + 2 * H) // 2, lambda x, y: x * yh0 + y, H // 2, 1
    )
    xg1 = gs // cy
    lv1 = Level(
        xg1, cx * wx // xg1, cy * wy, (cz + 2 * ZR) // 2,
        lambda x, y: (y // cy) * gs + x * cy + y % cy, ZR // 2, 4,
    )
    y2 = cy * wy // 2
    yh2 = 16 if y2 <= 16 else 32
    xg2 = LANES // yh2
    lv2 = Level(
        xg2, -(-(cx * wx // 2) // xg2), y2, (cz + 2 * ZR) // 4, lambda x, y: x * yh2 + y,
        ZR // 4, 1,
    )

    own_lo = H // xg0
    lo_b = (H - 4) // xg0
    n_b = (H + bx - 1 + 3) // xg0 - lo_b + 1
    px = []
    for x in range(cx):
        for s, w in restrict_taps(x):
            f = H + 2 * x + s
            px.append(((0, x), f // xg0 - lo_b, f % xg0, w))
    py = [(y, H + 2 * y + s, w) for y in range(cy) for s, w in restrict_taps(y)]
    once = plane_matrix(n_b, 1, px, py, lv0.at, lambda x, y: x * cy + y)
    m_r0 = once + np.roll(once, LANES // 2, axis=1)

    r_lo, r_hi = (-3) // xg1, (2 * xg2 + 1) // xg1
    px = []
    for x in range(xg2):
        for s, w in restrict_taps(x):
            f = 2 * x + s
            px.append(((0, x), f // xg1 - r_lo, f % xg1, w))
    py = [
        (y, 2 * y + s, w) for y in range(y2) for s, w in restrict_taps(y)
        if 0 <= 2 * y + s < cy * wy
    ]
    m_r1 = plane_matrix(r_hi - r_lo + 1, 1, px, py, lv1.at, lv2.at)

    ratio = 2 * xg2 // xg1
    px = []
    for f in range(2 * xg2):
        for c, w in prolong_taps(f):
            px.append(((f // xg1, f % xg1), c // xg2, c % xg2, w))
    py = [
        (f, c, w) for f in range(cy * wy) for c, w in prolong_taps(f) if 0 <= c < y2
    ]
    m_p1 = plane_matrix(2, ratio, px, py, lv2.at, lv1.at)

    up = 2 * xg1 // xg0
    px = []
    for f in range(2 * xg1):
        for c, w in prolong_taps(f):
            px.append(((f // xg0, f % xg0), c // xg1, c % xg1, w))
    py = [
        (f + H, c + cy, w) for f in range(-H, by + H) for c, w in prolong_taps(f)
        if -cy <= c < 2 * cy
    ]
    m_p0 = plane_matrix(2, up, px, py, lv1.at, lv0.at)

    parts, stack, row = {}, [], 0
    for name, m in (
        ("wa0", operator_matrix(lv0)), ("wa1", operator_matrix(lv1)),
        ("wa2", operator_matrix(lv2)), ("wr0", m_r0), ("wr1", m_r1), ("wp1", m_p1),
        ("wp0", m_p0),
    ):
        if m.shape[1] == LANES:
            m = np.pad(m, ((0, m.shape[0] % 2), (0, 0)))
            half = m.shape[0] // 2
            assert half % 16 == 0
            parts[name] = [(row, 0, half, LANES), (row, LANES, half, LANES)]
            stack.append(np.concatenate([m[:half], m[half:]], axis=1))
            row += half
        else:
            parts[name] = []
            for c in range(0, m.shape[1], 256):
                parts[name].append((row, 0, m.shape[0], min(256, m.shape[1] - c)))
                piece = m[:, c : c + 256]
                stack.append(np.pad(piece, ((0, 0), (0, 256 - piece.shape[1]))))
                row += m.shape[0]
    consts = to_bf16(np.concatenate(stack, axis=0))
    vm = lambda *s: pltpu.VMEM(s, F32)
    bm = lambda *s: pltpu.VMEM(s, BF16)
    dma = lambda *s: pltpu.SemaphoreType.DMA(s)

    def per_level(lv):
        t, n, p = lv.tiles, lv.rows, lv.pad
        return (
            vm(t + 2 * p, n, LANES), vm(t + 2 * p, n, LANES), vm(t + 2 * p, n, LANES),
            bm(t + 2 * p + 2, n, LANES), bm(t + 2 * p + 2, n, LANES),
            vm(4, 4, lv.half + 16, LANES), vm(t + 2 * p, 2, 8, LANES),
            vm(t + 2 * p, 8, LANES), vm(2, lv.half, LANES),
        )

    p0, p1, p2 = per_level(lv0), per_level(lv1), per_level(lv2)
    tau_lo = (lo_b - own_lo) // up
    n_tau = (lo_b + n_b - 1 - own_lo) // up + 2 - tau_lo
    jn = (lv0.half // 2 + 7) // 8 * 8
    geo = (nx, ny, nz, bx, by, bz, wx, wy, wyp)
    near, side = (3 if nx > 1 else 1), (3 if ny > 1 else 1)
    n_z = 0 if nz == 1 else 1 if nz == 2 else 2
    n_x = max(1, nx - 1 if wx == nx else 2 * REACH)
    n_y = ny - 1 if wy == ny else 2 * REACH
    n_p = max(1, (n_y + 1) * (n_z + 1) - 1)
    n_xy, n_s = max(1, near * side - 1), near * side
    step_rows = n_y * (cz // 2) + (n_y + 1) * n_z * (ZR // 2)
    merged = (
        wx == nx and wy == ny and nz <= 2 and step_rows > 0 and step_rows % yh0 == 0
        and (step_rows // yh0) * nx <= bx + 2 * H
    )
    sems = (dma(1, 1), dma(1, nx)) if merged else (dma(n_p, n_x + 1), dma(n_p, n_x + 1))
    return pl.pallas_call(
        functools.partial(kernel, geo, lv0, lv1, lv2, parts),
        out_shape=pltpu.VMEM(u.shape, F32),
        in_specs=[pl.BlockSpec(memory_space=pl.ANY)] * 3,
        out_specs=pl.BlockSpec(memory_space=pltpu.VMEM),
        scratch_shapes=[
            bm(*consts.shape), vm(bx, by, bz), vm(bx, by, bz),
            vm(bx + 2 * H, yh0, bz), vm(bx + 2 * H, yh0, bz), vm(bz, LANES),
            vm(xg0, yh0, bz), vm(2, 3, 2, bx // xg0, H, LANES),
            vm(2, 3, 2, lv0.tiles, H, LANES),
            *p0, *p1, vm(lv1.tiles + 8, lv1.rows, LANES), p2[0], p2[1], *p2[3:],
            vm(2, lv0.half, LANES), vm(2, lv1.half + 16, LANES), vm(cz // 2, LANES),
            vm(wx, cz // 2, LANES), vm(wy, wx, lv1.half, LANES),
            vm(lv2.tiles, 2, lv2.half + 8, LANES), vm(lv2.tiles, lv1.rows, LANES),
            vm(n_tau, lv0.half + 2 * jn, LANES),
            bm(lv2.tiles, lv1.rows, LANES), bm(lv2.tiles, lv1.rows, LANES),
            bm(n_tau, lv0.rows, LANES), bm(n_tau, lv0.rows, LANES),
            dma(3), dma(n_xy, 2), dma(n_xy, 2), dma(n_s, max(1, n_z)), dma(n_s, max(1, n_z)),
            dma(n_x), dma(n_x), *sems,
        ],
        compiler_params=pltpu.CompilerParams(
            collective_id=0, has_side_effects=True, vmem_limit_bytes=60 * 1024 * 1024
        ),
    )(u, b, consts)


def solution(mesh):
    placed = P("gx", "gy", "gz")
    return jax.shard_map(
        functools.partial(local, dict(mesh.shape)), mesh=mesh,
        in_specs=(placed, placed), out_specs=placed, check_vma=False,
    )
```
